256 devices in a mesh: gx: 4 (over x), gy: 8 (over z), gz: 8 (over y, core).
Axes of the slice: x: 4, y: 4, z: 8, core: 2. Of those that a mesh axis runs over, the one named last changes fastest.
Arguments:
- right_side: float32 [128, 256, 1024], P('gx', 'gy', 'gz'), may hold values from -1 to 1
- z_faces: float32 [1024], P('gz'), may hold values from 0.5 to 2, as said below
- xy_coupling: float32 [5], replicated, as said below
- block_inverse: float32 [5, 1024, 128], P(None, 'gz'), as said below
Outputs:
- solution: float32 [128, 256, 1024], P('gx', 'gy', 'gz')
- residual: float32 [128, 256, 1024], P('gx', 'gy', 'gz')
The draws below stay inside these ranges and needn't reach their ends.
Inputs may be any that keep to these rules, and one draw needn't show every extreme that they name: z_faces is positive. xy_coupling[l] lies between 2.9 * 4^-l / 128^2 and 5.5 * 4^-l / 128^2. block_inverse[l] holds, block by block, the inverses of the 128 x 128 diagonal blocks of M_l built from z_faces and xy_coupling[l].
All inputs are finite; a program needn't handle non-finite values.
Results may differ from the reference program's by a relative error of at most 0.028.
Values sent between devices are 32-bit elements; how exact they have to be, the bound alone decides.
A program may use at most 128 MiB of HBM per device.

```python
import jax
import jax.numpy as jnp
from jax import lax

CZ = 128
LEVELS = 5
SWEEPS = 2
NX = 128
NY = 256
NZ = 1024


def coefficient_set(key):
    face_key = jax.random.fold_in(key, 101)
    level_key = jax.random.fold_in(key, 202)
    face_values = jnp.exp(jax.random.uniform(face_key, (NZ,), jnp.float32, jnp.log(0.5), jnp.log(2.0)))
    spread = jnp.exp(jax.random.uniform(level_key, (LEVELS,), jnp.float32, -0.3, 0.3))
    lateral = 4.0 / (CZ * CZ) * spread * 0.25 ** jnp.arange(LEVELS).astype(jnp.float32)
    return (face_values, lateral)


def draw_right_side(key, part):
    rough_key = jax.random.fold_in(key, 303)
    amplitude = 0.03 * (256.0 / NZ) ** 1.5
    rough = jnp.clip(jax.random.normal(rough_key, (NX, NY, NZ), jnp.float32), -4.0, 4.0)
    field = amplitude * rough
    return field.astype(jnp.float32)


def draw_z_faces(key, part):
    return coefficient_set(key)[0].astype(jnp.float32)


def draw_xy_coupling(key, part):
    return coefficient_set(key)[1].astype(jnp.float32)


def draw_block_inverse(key, part):
    face_values, lateral = coefficient_set(key)
    blocks_count = NZ // CZ
    up_values = jnp.concatenate([face_values[1:], jnp.ones((1,), jnp.float32)])
    down_rows = face_values.reshape(blocks_count, CZ)
    up_rows = up_values.reshape(blocks_count, CZ)
    identity = jnp.eye(CZ, dtype=jnp.float32)
    upper_shift = jnp.eye(CZ, k=1, dtype=jnp.float32)
    coupling = up_rows[:, :, None] * upper_shift
    base_matrix = (down_rows + up_rows)[:, :, None] * identity - coupling - jnp.swapaxes(coupling, 1, 2)
    matrices = base_matrix[None] + (4.0 * lateral)[:, None, None, None] * identity
    return jnp.linalg.inv(matrices).reshape(LEVELS, NZ, CZ).astype(jnp.float32)


def setup_inputs(seed: int = 0) -> dict:
    streams_of = jax.random.split(jax.random.key(seed), 5)
    right_side = draw_right_side(jax.random.fold_in(streams_of[4], 71), 0)
    z_faces = draw_z_faces(jax.random.fold_in(streams_of[4], 71), 0)
    xy_coupling = draw_xy_coupling(jax.random.fold_in(streams_of[4], 71), 0)
    block_inverse = draw_block_inverse(jax.random.fold_in(streams_of[4], 71), 0)
    return {"right_side": right_side, "z_faces": z_faces, "xy_coupling": xy_coupling, "block_inverse": block_inverse}


damping = 0.8
highest = lax.Precision.HIGHEST

def interface_setup(corner_aa, corner_ab, corner_ba, corner_bb, couplings):
    determinant = corner_aa * corner_bb - corner_ab * corner_ba
    corner_inverse = jnp.stack([jnp.stack([corner_bb, -corner_ab], -1), jnp.stack([-corner_ba, corner_aa], -1)], -2) / determinant[:, None, None]
    blocks_count = corner_aa.shape[0]
    identity = jnp.eye(blocks_count, dtype=corner_inverse.dtype)
    diagonal_part = jnp.einsum('kab,kl->kalb', corner_inverse, identity, precision=highest).reshape(2 * blocks_count, 2 * blocks_count)
    link_values = jnp.zeros((2 * blocks_count - 1,), corner_inverse.dtype).at[1::2].set(-couplings)
    schur_matrix = diagonal_part + jnp.diag(link_values, 1) + jnp.diag(link_values, -1)
    return (corner_inverse, diagonal_part, jnp.linalg.cholesky(schur_matrix))

def level_setup(block_inverse, z_faces, level):
    block_len = block_inverse.shape[2]
    blocks_count = z_faces.shape[0] // block_len
    inverse_blocks = block_inverse[level].reshape(blocks_count, block_len, block_len)
    last_cell = block_len - 1
    couplings = z_faces.reshape(blocks_count, block_len)[1:, 0]
    corner_inverse, diagonal_part, factor = interface_setup(inverse_blocks[:, 0, 0], inverse_blocks[:, 0, last_cell], inverse_blocks[:, last_cell, 0], inverse_blocks[:, last_cell, last_cell], couplings)
    return (inverse_blocks, corner_inverse, factor, couplings)

def line_solve(source, inverse_blocks, corner_inverse, factor, couplings):
    first_extent, second_extent, depth = source.shape
    blocks_count, block_len = (inverse_blocks.shape[0], inverse_blocks.shape[1])
    blocked = source.reshape(first_extent, second_extent, blocks_count, block_len)
    local_part = jnp.einsum('xykj,kij->xyki', blocked, inverse_blocks, precision=highest)
    end_values = jnp.stack([local_part[..., 0], local_part[..., block_len - 1]], -1)
    reduced_source = jnp.einsum('kab,xykb->kaxy', corner_inverse, end_values, precision=highest).reshape(2 * blocks_count, first_extent * second_extent)
    forward = lax.linalg.triangular_solve(factor, reduced_source, left_side=True, lower=True)
    interfaces = lax.linalg.triangular_solve(factor, forward, left_side=True, lower=True, transpose_a=True)
    interfaces = interfaces.reshape(blocks_count, 2, first_extent, second_extent).transpose(2, 3, 0, 1)
    zero_plane = jnp.zeros((first_extent, second_extent, 1), local_part.dtype)
    below_last = jnp.concatenate([zero_plane, interfaces[:, :, :-1, 1]], 2)
    above_first = jnp.concatenate([interfaces[:, :, 1:, 0], zero_plane], 2)
    zero_single = jnp.zeros((1,), couplings.dtype)
    down_coupling = jnp.concatenate([zero_single, couplings])
    up_coupling = jnp.concatenate([couplings, zero_single])
    result = local_part + (down_coupling * below_last)[..., None] * inverse_blocks[:, :, 0] + (up_coupling * above_first)[..., None] * inverse_blocks[:, :, block_len - 1]
    return result.reshape(first_extent, second_extent, depth)

def apply_operator(iterate, lateral_weight, down_faces, up_faces):
    padded = jnp.pad(iterate, 1)
    lateral = padded[:-2, 1:-1, 1:-1] + padded[2:, 1:-1, 1:-1] + padded[1:-1, :-2, 1:-1] + padded[1:-1, 2:, 1:-1]
    return lateral_weight * (4.0 * iterate - lateral) + down_faces * (iterate - padded[1:-1, 1:-1, :-2]) + up_faces * (iterate - padded[1:-1, 1:-1, 2:])

def restrict(field):
    first_extent, second_extent, depth = field.shape
    return field.reshape(first_extent // 2, 2, second_extent // 2, 2, depth).sum(axis=(1, 3)) * 0.25

def prolong(padded):
    first_extent = padded.shape[0] - 2
    second_extent = padded.shape[1] - 2
    depth = padded.shape[2]
    even_rows = 0.75 * padded[1:-1] + 0.25 * padded[:-2]
    odd_rows = 0.75 * padded[1:-1] + 0.25 * padded[2:]
    widened = jnp.stack([even_rows, odd_rows], 1).reshape(2 * first_extent, second_extent + 2, depth)
    even_rows = 0.75 * widened[:, 1:-1] + 0.25 * widened[:, :-2]
    odd_rows = 0.75 * widened[:, 1:-1] + 0.25 * widened[:, 2:]
    return jnp.stack([even_rows, odd_rows], 2).reshape(2 * first_extent, 2 * second_extent, depth)

def reference(right_side, z_faces, xy_coupling, block_inverse):
    up_faces = jnp.concatenate([z_faces[1:], jnp.ones((1,), z_faces.dtype)])
    setups = [level_setup(block_inverse, z_faces, level) for level in range(LEVELS)]

    def operator(iterate, level):
        return apply_operator(iterate, xy_coupling[level], z_faces, up_faces)

    def smooth(source, level):
        return line_solve(source, *setups[level])

    def multigrid_cycle(source, level):
        iterate = damping * smooth(source, level)
        for sweep in range(SWEEPS - 1):
            iterate = iterate + damping * smooth(source - operator(iterate, level), level)
        if level == LEVELS - 1:
            return iterate
        coarse = multigrid_cycle(restrict(source - operator(iterate, level)), level + 1)
        iterate = iterate + prolong(jnp.pad(coarse, ((1, 1), (1, 1), (0, 0))))
        for sweep in range(SWEEPS):
            iterate = iterate + damping * smooth(source - operator(iterate, level), level)
        return iterate
    solution = multigrid_cycle(right_side, 0)
    return (solution, right_side - operator(solution, 0))
```

```python
import jax
import jax.numpy as jnp
from jax import lax
from jax.experimental import pallas as pl
from jax.experimental.pallas import tpu as pltpu
from jax.sharding import PartitionSpec as P

f32 = jnp.float32
bf16 = jnp.bfloat16
HI = lax.Precision.HIGHEST
MESH = pl.DeviceIdType.MESH
DIRS = [(dx, dy) for dx in (-1, 0, 1) for dy in (-1, 0, 1) if (dx, dy) != (0, 0)]

LX = [32, 16, 8, 4, 2]
OX = [4, 3, 3, 4, 4]
OY = [8, 8, 8, 4, 4]
SX = [40, 22, 14, 12, 10]
SY = [48, 32, 24, 16, 16]


def pair_of(p):
    if p < 12:
        return p // 4 + 1, p % 4 + 1
    return (0 if p < 14 else 4), p % 2 + 1


def pid(l, m):
    if l == 0:
        return 11 + m
    if l == 4:
        return 13 + m
    return (l - 1) * 4 + m - 1


def split(x):
    h = x.astype(bf16)
    return h, (x - h.astype(f32)).astype(bf16)


def mm(a, b, trans_b=False):
    dims = (((1,), (1 if trans_b else 0,)), ((), ()))
    return lax.dot_general(a, b, dims, preferred_element_type=f32)


def dot3(a, b, trans_b=False):
    ah, al = split(a)
    bh, bl = split(b)
    return mm(ah, bh, trans_b) + (mm(ah, bl, trans_b) + mm(al, bh, trans_b))


def hdot(a, b):
    return jnp.dot(a, b, precision=HI, preferred_element_type=f32)


def iota(shape, dim):
    return lax.broadcasted_iota(jnp.int32, shape, dim)


def scratch_shapes():
    out = {}
    for l in range(5):
        out[f"S{l}"] = (2, SX[l], SY[l], 128)
        for t in ("TA", "TB", "TC", "AA", "BB", "CC", "MA", "P0", "P1", "P2"):
            out[f"{t}{l}"] = (2, SX[l], SY[l], 128)
        if l:
            for t in ("M", "U", "V"):
                out[f"{t}{l}"] = (2, SX[l], SY[l], 128)
    out["fb3"] = out["mb3"] = (2, 4, 8, 128)
    out["fb4"] = out["mb4"] = (2, 2, 8, 128)
    out["rb3"] = out["qb3"] = (8, 2, 4, 8, 128)
    out["rb4"] = out["qb4"] = (8, 2, 2, 8, 128)
    out["rows"] = (4, 16, 128)
    out["re0"] = (8, 128)
    out["re1"] = (32, 128)
    out["cg"] = (9, 16, 128)
    out["cgl"] = (16, 128)
    out["e0"] = (8, 8, 1920)
    out["e1"] = (8, 32, 256)
    out["el0"] = (8, 1920)
    out["el1"] = (32, 256)
    return out


def kernel(sizes, f_ref, zf_ref, g_ref, e_ref, sol_ref, res_ref, *refs):
    names = list(scratch_shapes())
    r_ = dict(zip(names, refs))
    th, tl, hs, hr, gs, gr = refs[len(names):]
    S0, S1, S2, S3, S4 = [r_[f"S{l}"] for l in range(5)]
    M1, M2, M3, M4 = [r_[f"M{l}"] for l in range(1, 5)]
    fb3, fb4, mb3, mb4 = r_["fb3"], r_["fb4"], r_["mb3"], r_["mb4"]
    rb3, rb4, qb3, qb4 = r_["rb3"], r_["rb4"], r_["qb3"], r_["qb4"]
    rows, re0, re1, cg, cgl = r_["rows"], r_["re0"], r_["re1"], r_["cg"], r_["cgl"]
    e0, e1, el0, el1 = r_["e0"], r_["e1"], r_["el0"], r_["el1"]

    ngx, ngy, ngz = sizes
    ix, iy, k = lax.axis_index("gx"), lax.axis_index("gy"), lax.axis_index("gz")
    S = [S0, S1, S2, S3, S4]
    M = [None, M1, M2, M3, M4]

    def at(name, l):
        return r_[f"{name}{l}"]


    def peer(o):
        return jnp.where(k + o >= ngz, k + o - ngz, k + o)

    def exists(dx, dy):
        x, y = ix + dx, iy + dy
        return (x >= 0) & (x < ngx) & (y >= 0) & (y < ngy)

    def clear(ref):
        def step(i, c):
            ref[i] = jnp.zeros(ref.shape[1:], f32)
            return c
        lax.fori_loop(0, ref.shape[0], step, 0)

    def clear2(ref):
        def step(i, c):
            for h in range(2):
                ref[h, i] = jnp.zeros(ref.shape[2:], f32)
            return c
        lax.fori_loop(0, ref.shape[1], step, 0)

    for r in (S0, S1, S2, S3, S4, M1, M2, M3, M4):
        clear2(r)
    for r in (cg, e0, e1, rb3, rb4, qb3, qb4, fb3, fb4, mb3, mb4, rows):
        clear(r)

    barrier = pltpu.get_barrier_semaphore()
    count = jnp.int32(ngz - 1)
    for dx, dy in DIRS:
        ok = exists(dx, dy)

        @pl.when(ok)
        def _():
            pl.semaphore_signal(
                barrier, inc=1, device_id=(ix + dx, iy + dy, k), device_id_type=MESH
            )

        count = count + jnp.where(ok, 1, 0)
    for o in range(1, ngz):
        pl.semaphore_signal(
            barrier, inc=1, device_id=(ix, iy, peer(o)), device_id_type=MESH
        )

    def exchange(phase, pick):
        def copy(d, dx, dy):
            src, dst = pick(dx, dy)
            return pltpu.make_async_remote_copy(
                src_ref=src, dst_ref=dst, send_sem=hs.at[phase, d], recv_sem=hr.at[phase, d],
                device_id=(ix + dx, iy + dy, k), device_id_type=MESH,
            )

        def start():
            for d, (dx, dy) in enumerate(DIRS):
                @pl.when(exists(dx, dy))
                def _():
                    copy(d, dx, dy).start()

        def wait_recv():
            for d, (dx, dy) in enumerate(DIRS):
                @pl.when(exists(-dx, -dy))
                def _():
                    copy(d, dx, dy).wait_recv()

        def wait_send():
            for d, (dx, dy) in enumerate(DIRS):
                @pl.when(exists(dx, dy))
                def _():
                    copy(d, dx, dy).wait_send()

        return start, wait_recv, wait_send

    def span(d, off, n, h):
        if d == 0:
            return pl.ds(off, n), pl.ds(off, n)
        if d == 1:
            return pl.ds(off + n - h, h), pl.ds(off - h, h)
        return pl.ds(off, h), pl.ds(off + n, h)

    def halo(phase, buf, half, ox, n, hx):
        def pick(dx, dy):
            sx, tx = span(dx, ox, n, hx)
            sy, ty = span(dy, 8, n, 8)
            if half is None:
                return buf.at[:, sx, sy, :], buf.at[:, tx, ty, :]
            return buf.at[half, sx, sy, :], buf.at[half, tx, ty, :]
        return exchange(phase, pick)

    def whole(phase, blk, rbuf):
        def pick(dx, dy):
            return blk, rbuf.at[DIRS.index((dx, dy))]
        return exchange(phase, pick)

    def gather(phase, src, buf):
        def copy(o):
            return pltpu.make_async_remote_copy(
                src_ref=src, dst_ref=buf.at[k], send_sem=gs.at[phase, o],
                recv_sem=gr.at[phase, o], device_id=(ix, iy, peer(o)),
                device_id_type=MESH,
            )

        def start():
            for o in range(1, ngz):
                copy(o).start()

        def wait_recv():
            for o in range(1, ngz):
                copy(o).wait_recv()

        def wait_send():
            for o in range(1, ngz):
                copy(o).wait_send()

        return start, wait_recv, wait_send

    sends = []

    a = [4.0 * e_ref[l] for l in range(5)]
    for l in range(5):
        rows[0, 2 * l : 2 * l + 1, :] = a[l] * g_ref[l, 0:1, :]
        rows[0, 2 * l + 1 : 2 * l + 2, :] = a[l] * g_ref[l, 127:128, :]
    for m in range(1, 4):
        prev = rows[m - 1]
        for l in range(5):
            nxt = a[l] * hdot(prev, g_ref[l])
            rows[m, 2 * l : 2 * l + 2, :] = nxt[2 * l : 2 * l + 2]
    for m in range(4):
        re0[2 * m : 2 * m + 2, :] = rows[m, 0:2, :]
    for p in range(16):
        l, m = pair_of(p)
        re1[2 * p : 2 * p + 2, :] = rows[m - 1, 2 * l : 2 * l + 2, :]
    lane16 = iota((16, 128), 1)
    tile = jnp.where(lane16 == 8, jnp.broadcast_to(zf_ref[0:1, 0:1], (16, 128)), 0.0)
    for n in range(4):
        rn = rows[n]
        tile = jnp.where(lane16 == 2 * n, jnp.broadcast_to(rn[:, 0:1], (16, 128)), tile)
        tile = jnp.where(lane16 == 2 * n + 1, jnp.broadcast_to(rn[:, 127:128], (16, 128)), tile)
    cgl[...] = tile
    cg[k] = tile

    def put_f(i, c):
        S0[0, 4 + i, 8:40, :] = f_ref[i]
        return c
    lax.fori_loop(0, 32, put_f, 0)

    pl.semaphore_wait(barrier, count)

    c_start, c_recv, c_send = gather(0, cgl, cg)
    c_start()

    def pick0(dx, dy):
        sx, tx = span(dx, 4, 32, 4)
        sy, ty = span(dy, 8, 32, 8)
        sx0, _ = span(dx, 0, 32, 4)
        sy0, _ = span(dy, 0, 32, 8)
        return f_ref.at[sx0, sy0, :], S0.at[0, tx, ty, :]

    h_start, h_recv, h_send = exchange(0, pick0)
    h_start()
    sends += [c_send, h_send]

    h_recv()
    r0 = re0[...]
    for i in range(5):
        fx = S0[0, 8 * i : 8 * i + 8].reshape(384, 128)
        el0[:, 384 * i : 384 * i + 384] = dot3(r0, fx, True)
    e0[k] = el0[...]
    g0_start, g0_recv, g0_send = gather(1, el0, e0)
    g0_start()
    sends.append(g0_send)

    c_recv()
    CG = cg[0:8].reshape(128, 128)
    ri, ci = iota((128, 128), 0), iota((128, 128), 1)
    same = (ri >> 1) == (ci >> 1)
    odd = (ci & 1) == 1
    eye = jnp.where(ri == ci, 1.0, 0.0).astype(f32)

    def col(c):
        return jnp.broadcast_to(CG[:, c : c + 1], (128, 128))

    def corner(n):
        return jnp.where(same, jnp.where(odd, col(2 * n + 1), col(2 * n)), 0.0)

    lrow = (ri >> 1) & 7
    inva = jnp.zeros((128, 128), f32)
    for l in range(5):
        inva = jnp.where(lrow == l, 1.0 / a[l], inva)
    face = col(8)
    face_up = jnp.concatenate([face[16:], jnp.zeros((16, 128), f32)], 0)
    K = inva * (
        jnp.where(((ri & 1) == 0) & (ci == ri - 15), face, 0.0)
        + jnp.where(((ri & 1) == 1) & (ci == ri + 15), face_up, 0.0)
    )
    R = corner(0)
    blk = (ri >> 4) + (ri & 1)
    for st in (1, 2, 4):
        link = jnp.where((blk & (2 * st - 1)) == st, K, 0.0)
        d = R * eye
        drow = jnp.sum(d, 1, keepdims=True)
        dcol = jnp.sum(d, 0, keepdims=True)
        off = link / (1.0 - link * link * drow * dcol)
        diag = jnp.sum(off * link * dcol, 1, keepdims=True)
        R = R + hdot(hdot(R, off + eye * diag), R)
    W = eye + hdot(R, K)
    B2, B3, B4 = dot3(corner(1), K), dot3(corner(2), K), dot3(corner(3), K)
    V1 = dot3(W, dot3(B2, W))
    V2 = dot3(W, dot3(B3, W) + dot3(B2, V1))
    V3 = dot3(W, dot3(B4, W) + dot3(B3, V1) + dot3(B2, V2))
    VS = [W, V1, V2, V3]

    def lm_of(p):
        l = jnp.where(p < 12, (p >> 2) + 1, jnp.where(p < 14, 0, 4))
        m = jnp.where(p < 12, (p & 3) + 1, (p & 1) + 1)
        return l, m

    def funct(level):
        width = 64 if level == 0 else 256
        rr, rc = iota((128, 128), 0), iota((128, 128), 1)
        p, side = rr & 15, rr >> 4
        if level == 0:
            l, m = jnp.zeros_like(p), p - 11
            live = (rr < 32) & (p >= 12)
        else:
            l, m = lm_of(p)
            live = rr < 32
        target = jnp.where(side == 0, (k - 1) * 16 + l * 2 + 1, (k + 1) * 16 + l * 2)
        pick_rows = jnp.where(live & (rc == target), 1.0, 0.0).astype(f32)
        er, ec = iota((128, width), 0), iota((128, width), 1)
        if level == 0:
            jc, lc, mc, endc = ec >> 3, jnp.zeros_like(ec), ((ec >> 1) & 3) + 1, ec & 1
        else:
            jc, endc = ec >> 5, ec & 1
            lc, mc = lm_of((ec >> 1) & 15)
        expand = jnp.where(er == jc * 16 + lc * 2 + endc, 1.0, 0.0).astype(f32)
        wr = iota((128, width), 0)
        mrow = ((wr & 15) - 11) if level == 0 else lm_of(wr & 15)[1]
        out = jnp.zeros((128, width), f32)
        for n in range(4):
            x = dot3(dot3(pick_rows, VS[n]), expand)
            out = out + jnp.where(mrow - mc == n, x, 0.0)
        return out

    L0 = funct(0)
    L1 = funct(1)

    side_in, side_out = ri >> 4, ci >> 4
    pi, po = ri & 15, ci & 15
    fl = (ri < 32) & (ci < 32) & (side_in == side_out)
    li, mi = lm_of(pi)
    lo, mo = lm_of(po)
    aout = jnp.zeros((128, 128), f32)
    for l in range(5):
        aout = jnp.where(lo == l, a[l], aout)
    cm = jnp.broadcast_to(zf_ref[0:1, 0:1], (1, 128))
    cp = jnp.broadcast_to(cg[k + 1, 0:1, 8:9], (1, 128))
    for l in range(5):
        gt = g_ref[l].T
        p1 = pid(l, 1)
        ut = jnp.where(ri == p1, jnp.broadcast_to(cm * gt[0:1], (128, 128)), 0.0)
        ut = jnp.where(ri == 16 + p1, jnp.broadcast_to(cp * gt[127:128], (128, 128)), ut)
        if l == 0:
            q = jnp.where(fl & (pi >= 13) & (pi == po + 1), 1.0, 0.0)
        else:
            den = jnp.where(lo == l, 1.0, a[l] - aout)
            amp = a[l] / den
            nb = -aout / den
            p2 = nb * nb
            p3 = p2 * nb
            dm = mo - mi
            pw = jnp.where(dm == 0, 1.0, jnp.where(dm == 1, nb, jnp.where(dm == 2, p2, p3)))
            pm = jnp.where(mo == 1, nb, jnp.where(mo == 2, p2, jnp.where(mo == 3, p3, p2 * p2)))
            q = jnp.where((li == lo) & (dm >= 0), amp * pw, 0.0)
            q = q + jnp.where((li == l) & (mi == 1), pm, 0.0)
            q = jnp.where(lo == l, jnp.where((li == l) & (mi == mo + 1), 1.0, 0.0), q)
            q = jnp.where(fl, q, 0.0)
        for r, v in ((0, a[l] * gt), (128, ut)):
            vh, vl = split(v)
            th[l, r : r + 128, 0:128] = vh
            tl[l, r : r + 128, 0:128] = vl
        qh, ql = split(q.astype(f32))
        zero = jnp.zeros((128, 128), bf16)
        th[l, 0:128, 128:256] = zero
        tl[l, 0:128, 128:256] = zero
        th[l, 128:256, 128:256] = qh
        tl[l, 128:256, 128:256] = ql

    def apply(l, src, dst, step, n, scale=None):
        y = src.shape[2]

        def body(i, c):
            x = pl.ds(i * step, step)
            v = jnp.concatenate(
                [src[0, x].reshape(step * y, 128), src[1, x].reshape(step * y, 128)], 1
            )
            vh, vl = split(v)
            t = mm(vh, th[l]) + (mm(vh, tl[l]) + mm(vl, th[l]))
            if scale is not None:
                t = scale * t
            dst[0, x] = t[:, 0:128].reshape(step, y, 128)
            dst[1, x] = t[:, 128:256].reshape(step, y, 128)
            return c

        lax.fori_loop(0, n, body, 0)

    def stencil(l, src, dst, grow, post, halves=(0, 1)):
        ox, oy, n, y = OX[l], OY[l], LX[l], SY[l]
        gy0 = iota((y, 128), 0) + (iy * n - oy)
        ym = jnp.where((gy0 >= 0) & (gy0 < ngy * n), 0.25, 0.0).astype(f32)

        def body(x, c):
            gx0 = ix * n + x - ox
            s = jnp.where((gx0 >= 0) & (gx0 < ngx * n), 1.0, 0.0).astype(f32)
            m4 = ym * s
            for h in halves:
                v = src[h, x]
                t = (src[h, x - 1] + src[h, x + 1]) + (
                    pltpu.roll(v, 1, 0) + pltpu.roll(v, y - 1, 0)
                )
                dst(h, x, post(h, x, m4 * t))
            return c

        lax.fori_loop(ox - grow, ox + n + grow, body, 0)

    def into(ref):
        def put(h, x, v):
            ref[h, x] = v
        return put

    def solve(l, src, dst, matrix=None, scale=None):
        step, n = (8, 5) if l == 0 else (SX[l], 1)
        apply(l if matrix is None else matrix, src, dst, step, n, scale)

    def residual(l, halves=(0, 1)):
        s, ta, tb = S[l], at("TA", l), at("TB", l)
        aa, bb = at("AA", l), at("BB", l)
        solve(l, s, ta)
        solve(l, ta, tb)
        stencil(l, tb, into(bb), 1, lambda h, x, v: 0.32 * ta[h, x] + 0.64 * v, halves)
        stencil(l, bb, into(aa), 0, lambda h, x, v: 0.04 * s[h, x] + v, halves)

    def smoothed(l):
        w = 1 if l == 0 else 0
        s, ta, tb, tc = S[l], at("TA", l), at("TB", l), at("TC", l)
        bb, cc, ma = at("BB", l), at("CC", l), at("MA", l)
        solve(l, tb, tc)
        stencil(l, tc, into(bb), 2 + w, lambda h, x, v: 0.8192 * tb[h, x] + 0.4096 * v)
        stencil(l, bb, into(cc), 1 + w, lambda h, x, v: 0.9728 * ta[h, x] + v)
        stencil(l, cc, into(ma), w, lambda h, x, v: 0.9984 * s[h, x] + v)

    def restrict(l, put, halves=(0, 1)):
        ox, oy, n = OX[l], OY[l], LX[l] // 2
        aa = at("AA", l)

        def body(i, c):
            x = ox + 2 * i
            for h in halves:
                even, off = pl.ds(oy, n, 2), pl.ds(oy + 1, n, 2)
                v = (aa[h, x, even, :] + aa[h, x, off, :]) + (
                    aa[h, x + 1, even, :] + aa[h, x + 1, off, :]
                )
                put(h, i, 0.25 * v)
            return c

        lax.fori_loop(0, n, body, 0)

    def unpack(dst, blk, rbuf, n):
        for h in range(2):
            for i in range(n):
                dst[h, 4 + i, 4 : 4 + n, :] = blk[h, i, 0:n, :]
                for d, (dx, dy) in enumerate(DIRS):
                    dst[h, 4 - n * dx + i, 4 - n * dy : 4 - n * dy + n, :] = rbuf[d, h, i, 0:n, :]

    def correct(l, store):
        c = l + 1
        w = 1 if l == 0 else 0
        m, u, g2 = M[c], at("U", c), at("V", c)
        kap = a[l] / a[c]
        solve(c, m, u, c, kap)
        solve(c, u, g2, l, 0.64)
        q = 0.04 * (1.0 - a[c] / a[l])
        n, ox, oc = LX[c], OX[l], OX[c]
        y = SY[c]
        ys, cnt = [(4, 24), (4, 16), (0, 12), (2, 8)][l]
        gyc = iota((cnt, 128), 0) + (iy * n + ys - OY[c])
        ym = jnp.where((gyc >= 0) & (gyc < ngy * n), 1.0, 0.0).astype(f32)
        outs = [at("P0", l), at("P1", l), at("P2", l)]

        def fields(h, x):
            uv = u[h, x]
            return (0.04 * m[h, x] + q * uv, 0.32 * uv, g2[h, x])

        def body(j, carry):
            j = j - (1 + w)
            gx = ix * n + j
            s = jnp.where((gx >= 0) & (gx < ngx * n), 1.0, 0.0).astype(f32)
            ms = ym * s
            for h in range(2):
                lower, here, upper = (fields(h, oc + j + i) for i in (-1, 0, 1))
                for o, lo_, he, up_ in zip(outs, lower, here, upper):
                    for i, far in enumerate((lo_, up_)):
                        v = 0.75 * he + 0.25 * far
                        ev = (0.75 * v + 0.25 * pltpu.roll(v, 1, 0))[ys : ys + cnt]
                        od = (0.75 * v + 0.25 * pltpu.roll(v, y - 1, 0))[ys : ys + cnt]
                        o[h, ox + 2 * j + i, pl.ds(0, cnt, 2), :] = ms * ev
                        o[h, ox + 2 * j + i, pl.ds(1, cnt, 2), :] = ms * od
            return carry

        lax.fori_loop(0, n + 2 + 2 * w, body, 0)
        cc, ma = at("CC", l), at("MA", l)
        stencil(l, outs[2], into(cc), 1 + w, lambda h, x, v: outs[1][h, x] + v)
        stencil(l, cc, store, w, lambda h, x, v: (ma[h, x] + outs[0][h, x]) + v)

    g0_recv()
    for i in range(5):
        phi = dot3(L0, e0[:, :, 384 * i : 384 * i + 384].reshape(64, 384))
        S0[1, 8 * i : 8 * i + 8] = phi.T.reshape(8, 48, 128)
    residual(0, (0,))

    def put1(h, i, v):
        S1[h, 3 + i, 8:24, :] = v
    restrict(0, put1, (0,))
    x1_start, x1_recv, x1_send = halo(1, S1, 0, 3, 16, 3)
    x1_start()
    el1[...] = dot3(re1[...], S1[0, 3:19, 8:24, :].reshape(256, 128), True)
    e1[k] = el1[...]
    g1_start, g1_recv, g1_send = gather(2, el1, e1)
    g1_start()
    smoothed(0)

    g1_recv()
    phi = dot3(L1, e1[...].reshape(256, 256))
    S1[1, 3:19, 8:24, :] = phi.T.reshape(16, 16, 128)
    y1_start, y1_recv, y1_send = halo(2, S1, 1, 3, 16, 3)
    y1_start()
    x1_recv()
    y1_recv()
    residual(1)

    def put2(h, i, v):
        S2[h, 3 + i, 8:16, :] = v
    restrict(1, put2)
    x2_start, x2_recv, x2_send = halo(3, S2, None, 3, 8, 3)
    x2_start()
    smoothed(1)

    x2_recv()
    residual(2)

    def put3(h, i, v):
        fb3[h, i, 0:4, :] = v
    restrict(2, put3)
    x3_start, x3_recv, x3_send = whole(4, fb3, rb3)
    x3_start()
    smoothed(2)

    x3_recv()
    unpack(S3, fb3, rb3, 4)
    residual(3)

    def put4(h, i, v):
        fb4[h, i, 0:2, :] = v
    restrict(3, put4)
    x4_start, x4_recv, x4_send = whole(5, fb4, rb4)
    x4_start()
    smoothed(3)

    x4_recv()
    unpack(S4, fb4, rb4, 2)
    ta4 = at("TA", 4)
    solve(4, S4, ta4)

    def putm4(h, x, v):
        mb4[h, x - 4, 0:2, :] = v[4:6]
    stencil(4, ta4, putm4, 0, lambda h, x, v: 0.96 * S4[h, x] + 0.64 * v)
    z4_start, z4_recv, z4_send = whole(6, mb4, qb4)
    z4_start()
    z4_recv()
    unpack(M4, mb4, qb4, 2)

    def putm3(h, x, v):
        mb3[h, x - 4, 0:4, :] = v[4:8]
    correct(3, putm3)
    z3_start, z3_recv, z3_send = whole(7, mb3, qb3)
    z3_start()
    z3_recv()
    unpack(M3, mb3, qb3, 4)

    def putm2(h, x, v):
        M2[h, x, 8:16, :] = v[8:16]
    correct(2, putm2)
    z2_start, z2_recv, z2_send = halo(8, M2, None, 3, 8, 2)
    z2_start()
    z2_recv()

    def putm1(h, x, v):
        M1[h, x, 8:24, :] = v[8:24]
    correct(1, putm1)
    z1_start, z1_recv, z1_send = halo(9, M1, None, 3, 16, 2)
    z1_start()
    z1_recv()

    mo = at("BB", 0)
    correct(0, into(mo))
    tm = at("TB", 0)
    solve(0, mo, tm)
    inv0 = 1.0 / a[0]

    def putout(h, x, v):
        res_ref[x - 4] = v[8:40]
        sol_ref[x - 4] = (inv0 * tm[0, x])[8:40]
    stencil(0, tm, putout, 0, lambda h, x, v: (S0[0, x] - mo[0, x]) + v, (0,))

    for wait in sends + [
        x1_send, g1_send, y1_send, x2_send, x3_send, x4_send, z4_send, z3_send, z2_send, z1_send
    ]:
        wait()


def body(sizes, right_side, z_faces, xy_coupling, block_inverse):
    n = right_side.shape
    vmem = pl.BlockSpec(memory_space=pltpu.VMEM)
    scratch = [pltpu.VMEM(s, f32) for s in scratch_shapes().values()]
    scratch += [pltpu.VMEM((5, 256, 256), bf16), pltpu.VMEM((5, 256, 256), bf16)]
    scratch += [pltpu.SemaphoreType.DMA((10, 8)), pltpu.SemaphoreType.DMA((10, 8))]
    scratch += [pltpu.SemaphoreType.DMA((3, 8)), pltpu.SemaphoreType.DMA((3, 8))]
    return pl.pallas_call(
        lambda *r: kernel(sizes, *r),
        out_shape=(jax.ShapeDtypeStruct(n, f32), jax.ShapeDtypeStruct(n, f32)),
        in_specs=[vmem, vmem, vmem, pl.BlockSpec(memory_space=pltpu.SMEM)],
        out_specs=(vmem, vmem),
        scratch_shapes=scratch,
        compiler_params=pltpu.CompilerParams(
            collective_id=0, has_side_effects=True, vmem_limit_bytes=60 * 2**20
        ),
        name="vcycle",
    )(right_side, z_faces.reshape(1, -1), block_inverse, xy_coupling)


def solution(mesh):
    sizes = tuple(mesh.shape[n] for n in ("gx", "gy", "gz"))
    return jax.shard_map(
        lambda *args: body(sizes, *args),
        mesh=mesh,
        in_specs=(P("gx", "gy", "gz"), P("gz"), P(), P(None, "gz", None)),
        out_specs=(P("gx", "gy", "gz"), P("gx", "gy", "gz")),
        check_vma=False,
    )
```

```python
import jax
import jax.numpy as jnp
from jax import lax
from jax.experimental import pallas as pl
from jax.experimental.pallas import tpu as pltpu
from jax.sharding import PartitionSpec as P

f32 = jnp.float32
bf16 = jnp.bfloat16
HI = lax.Precision.HIGHEST
MESH = pl.DeviceIdType.MESH
DIRS = [(dx, dy) for dx in (-1, 0, 1) for dy in (-1, 0, 1) if (dx, dy) != (0, 0)]

LX = [32, 16, 8, 4, 2]
OX = [4, 3, 3, 4, 4]
OY = [8, 8, 8, 4, 4]
SX = [40, 22, 14, 12, 10]
SY = [48, 32, 24, 16, 16]


def pair_of(p):
    if p < 12:
        return p // 4 + 1, p % 4 + 1
    return (0 if p < 14 else 4), p % 2 + 1


def pid(l, m):
    if l == 0:
        return 11 + m
    if l == 4:
        return 13 + m
    return (l - 1) * 4 + m - 1


def split(x):
    h = x.astype(bf16)
    return h, (x - h.astype(f32)).astype(bf16)


def mm(a, b, trans_b=False):
    dims = (((1,), (1 if trans_b else 0,)), ((), ()))
    return lax.dot_general(a, b, dims, preferred_element_type=f32)


def dot3(a, b, trans_b=False):
    ah, al = split(a)
    bh, bl = split(b)
    return mm(ah, bh, trans_b) + (mm(ah, bl, trans_b) + mm(al, bh, trans_b))


def hdot(a, b):
    return jnp.dot(a, b, precision=HI, preferred_element_type=f32)


def iota(shape, dim):
    return lax.broadcasted_iota(jnp.int32, shape, dim)


MESSAGES = {"f1": 2, "s2": 5, "s3": 3, "s4": 1, "m4": 1, "m3": 3, "m2": 5, "m1": 10}


def scratch_shapes():
    out = {}
    for l in range(5):
        out[f"S{l}"] = (2, SX[l], SY[l], 128)
        for t in ("TA", "TB", "TC", "AA", "BB", "CC", "MA", "P0", "P1", "P2"):
            out[f"{t}{l}"] = (2, SX[l], SY[l], 128)
        if l:
            for t in ("M", "U", "V"):
                out[f"{t}{l}"] = (2, SX[l], SY[l], 128)
    out["C0"] = (4, SX[0], SY[0], 128)
    out["HM"] = out["H2"] = (2, SX[1], SY[1], 128)
    for name, tiles in MESSAGES.items():
        out["out_" + name] = out["in_" + name] = (8, tiles, 8, 128)
    out["rows"] = (4, 16, 128)
    out["re0"] = (8, 128)
    out["re1"] = (32, 128)
    out["cg"] = (9, 16, 128)
    out["cgl"] = (16, 128)
    out["e0"] = (8, 8, 1024)
    out["eh"] = (8, 8, 640)
    out["e1"] = (8, 32, 256)
    out["el0"] = (8, 1024)
    out["elh"] = (8, 640)
    out["el1"] = (32, 256)
    return out


def kernel(sizes, f_ref, zf_ref, ginv_ref, e_ref, sol_ref, res_ref, *refs):
    names = list(scratch_shapes())
    r_ = dict(zip(names, refs))
    g_ref, th, tl, ra, ub, hs, hr, gs, gr, ls = refs[len(names):]
    S0, S1, S2, S3, S4 = [r_[f"S{l}"] for l in range(5)]
    M1, M2, M3, M4 = [r_[f"M{l}"] for l in range(1, 5)]
    rows, re0, re1, cg, cgl = r_["rows"], r_["re0"], r_["re1"], r_["cg"], r_["cgl"]
    e0, e1, el0, el1 = r_["e0"], r_["e1"], r_["el0"], r_["el1"]
    eh, elh, C0, HM, H2 = r_["eh"], r_["elh"], r_["C0"], r_["HM"], r_["H2"]

    ngx, ngy, ngz = sizes
    ix, iy, k = lax.axis_index("gx"), lax.axis_index("gy"), lax.axis_index("gz")
    S = [S0, S1, S2, S3, S4]
    M = [None, M1, M2, M3, M4]

    def at(name, l):
        return r_[f"{name}{l}"]


    def peer(o):
        return jnp.where(k + o >= ngz, k + o - ngz, k + o)

    def exists(dx, dy):
        x, y = ix + dx, iy + dy
        return (x >= 0) & (x < ngx) & (y >= 0) & (y < ngy)

    def clear(ref):
        def step(i, c):
            ref[i] = jnp.zeros(ref.shape[1:], f32)
            return c
        lax.fori_loop(0, ref.shape[0], step, 0)

    def clear2(ref):
        def step(i, c):
            for h in range(2):
                ref[h, i] = jnp.zeros(ref.shape[2:], f32)
            return c
        lax.fori_loop(0, ref.shape[1], step, 0)

    load_f = pltpu.make_async_copy(f_ref, S0.at[0, 4:36, 8:40, :], ls.at[0])
    load_g = pltpu.make_async_copy(ginv_ref, g_ref, ls.at[1])
    load_f.start()
    load_g.start()

    def edge(i, c):
        S0[0, i] = jnp.zeros((48, 128), f32)
        S0[0, 36 + i] = jnp.zeros((48, 128), f32)
        return c
    lax.fori_loop(0, 4, edge, 0)

    def sides(i, c):
        S0[0, 4 + i, 0:8, :] = jnp.zeros((8, 128), f32)
        S0[0, 4 + i, 40:48, :] = jnp.zeros((8, 128), f32)
        return c
    lax.fori_loop(0, 32, sides, 0)
    clear2(S1)
    clear(r_["in_f1"])
    clear(rows)
    if ngz < 8:
        for r in (e0, eh, e1):
            clear(r)
    clear(cg)

    barrier = pltpu.get_barrier_semaphore()
    count = jnp.int32(ngz - 1)
    for dx, dy in DIRS:
        ok = exists(dx, dy)

        @pl.when(ok)
        def _():
            pl.semaphore_signal(
                barrier, inc=1, device_id=(ix + dx, iy + dy, k), device_id_type=MESH
            )

        count = count + jnp.where(ok, 1, 0)
    for o in range(1, ngz):
        pl.semaphore_signal(
            barrier, inc=1, device_id=(ix, iy, peer(o)), device_id_type=MESH
        )

    def exchange(phase, pick):
        def copy(d, dx, dy):
            src, dst = pick(dx, dy)
            return pltpu.make_async_remote_copy(
                src_ref=src, dst_ref=dst, send_sem=hs.at[phase, d], recv_sem=hr.at[phase, d],
                device_id=(ix + dx, iy + dy, k), device_id_type=MESH,
            )

        def start():
            for d, (dx, dy) in enumerate(DIRS):
                @pl.when(exists(dx, dy))
                def _():
                    copy(d, dx, dy).start()

        def wait_recv():
            for d, (dx, dy) in enumerate(DIRS):
                @pl.when(exists(-dx, -dy))
                def _():
                    copy(d, dx, dy).wait_recv()

        def wait_send():
            for d, (dx, dy) in enumerate(DIRS):
                @pl.when(exists(dx, dy))
                def _():
                    copy(d, dx, dy).wait_send()

        return start, wait_recv, wait_send

    def span(d, off, n, h):
        if d == 0:
            return pl.ds(off, n), pl.ds(off, n)
        if d == 1:
            return pl.ds(off + n - h, h), pl.ds(off - h, h)
        return pl.ds(off, h), pl.ds(off + n, h)

    def halo(phase, buf, half, ox, n, hx):
        def pick(dx, dy):
            sx, tx = span(dx, ox, n, hx)
            sy, ty = span(dy, 8, n, 8)
            if half is None:
                return buf.at[:, sx, sy, :], buf.at[:, tx, ty, :]
            return buf.at[half, sx, sy, :], buf.at[half, tx, ty, :]
        return exchange(phase, pick)

    def lanes_of(planes):
        out = planes[0]
        for i, v in enumerate(planes[1:]):
            out = out + pltpu.roll(v, 32 * (i + 1), 1)
        return out

    low_lanes = {r: iota((r, 128), 1) < 32 for r in (8,)}

    def lanes_back(tile, i):
        v = tile if i == 0 else pltpu.roll(tile, 128 - 32 * i, 1)
        return jnp.where(low_lanes[8], v, 0.0)

    def tiles_of(l, dx, dy, both):
        n = LX[l]
        if dx == 0:
            return (n // 2 if both else 0) + (n + 7) // 8
        if dy == 0:
            return (3 * n // 8 if both else 0) + n // 8
        return 2 if both else 1

    def packed(phase, l, name, buf, both=True):
        n, ox, oy = LX[l], OX[l], OY[l]
        ob, ib = r_["out_" + name], r_["in_" + name]

        def pick(dx, dy):
            d, t = DIRS.index((dx, dy)), tiles_of(l, dx, dy, both)
            return ob.at[d, 0:t], ib.at[d, 0:t]

        start0, wait_recv, wait_send = exchange(phase, pick)

        def start():
            for d, (dx, dy) in enumerate(DIRS):
                xs = ox + n - 3 if dx == 1 else ox
                ys = oy + n - 4 if dy == 1 else oy
                yt = oy + n - 8 if dy == 1 else oy
                part = slice(4, 8) if dy == 1 else slice(0, 4)
                if dx == 0:
                    base = n // 2 if both else 0
                    if both:
                        for t in range(n // 2):
                            ob[d, t, 0:4, :] = buf[0, ox + t, ys : ys + 4, :]
                            ob[d, t, 4:8, :] = buf[0, ox + t + n // 2, ys : ys + 4, :]
                    for b in range(n // 4):
                        v = lanes_of([buf[1, ox + 4 * b + i, yt : yt + 8, :] for i in range(4)])
                        r = 4 * (b % 2)
                        ob[d, base + b // 2, r : r + 4, :] = v[part]
                elif dy == 0:
                    m = n // 8
                    base = 3 * m if both else 0
                    for r in range(m):
                        y = slice(oy + 8 * r, oy + 8 * r + 8)
                        if both:
                            for i in range(3):
                                ob[d, i * m + r] = buf[0, xs + i, y, :]
                        ob[d, base + r] = lanes_of([buf[1, xs + i, y, :] for i in range(3)])
                else:
                    if both:
                        ob[d, 0, 0:4, :] = buf[0, xs, ys : ys + 4, :]
                        ob[d, 0, 4:8, :] = buf[0, xs + 1, ys : ys + 4, :]
                        ob[d, 1, 0:4, :] = buf[0, xs + 2, ys : ys + 4, :]
                    v = lanes_of([buf[1, xs + i, yt : yt + 8, :] for i in range(3)])
                    ob[d, 1 if both else 0, 4:8, :] = v[part]
            start0()

        def finish():
            wait_recv()
            for d, (dx, dy) in enumerate(DIRS):
                xd = ox - 3 if dx == 1 else ox + n
                yd = oy - 4 if dy == 1 else oy + n
                if dx == 0:
                    base = n // 2 if both else 0
                    if both:
                        for t in range(n // 2):
                            buf[0, ox + t, yd : yd + 4, :] = ib[d, t, 0:4, :]
                            buf[0, ox + t + n // 2, yd : yd + 4, :] = ib[d, t, 4:8, :]
                    for b in range(n // 4):
                        tile, r = ib[d, base + b // 2], 4 * (b % 2)
                        for i in range(4):
                            v = lanes_back(tile, i)
                            buf[1, ox + 4 * b + i, yd : yd + 4, :] = v[r : r + 4]
                elif dy == 0:
                    m = n // 8
                    base = 3 * m if both else 0
                    for r in range(m):
                        y = slice(oy + 8 * r, oy + 8 * r + 8)
                        for i in range(3):
                            if both:
                                buf[0, xd + i, y, :] = ib[d, i * m + r]
                            buf[1, xd + i, y, :] = lanes_back(ib[d, base + r], i)
                else:
                    if both:
                        buf[0, xd, yd : yd + 4, :] = ib[d, 0, 0:4, :]
                        buf[0, xd + 1, yd : yd + 4, :] = ib[d, 0, 4:8, :]
                        buf[0, xd + 2, yd : yd + 4, :] = ib[d, 1, 0:4, :]
                    tile = ib[d, 1 if both else 0]
                    for i in range(3):
                        buf[1, xd + i, yd : yd + 4, :] = lanes_back(tile, i)[4:8]

        return start, finish, wait_send

    def packed_block(phase, l, name, buf):
        n = LX[l]
        ob, ib = r_["out_" + name], r_["in_" + name]

        def pick(dx, dy):
            return ob.at[0], ib.at[DIRS.index((dx, dy))]

        start0, wait_recv, wait_send = exchange(phase, pick)

        def start():
            phi = lanes_of([buf[1, 4 + i, 0:8, :] for i in range(n)])
            if n == 4:
                for i in range(4):
                    r = 4 * (i // 2)
                    ob[0, i % 2, r : r + 4, :] = buf[0, 4 + i, 4:8, :]
                ob[0, 2] = phi
            else:
                ob[0, 0, 0:2, :] = buf[0, 4, 4:6, :]
                ob[0, 0, 2:4, :] = buf[0, 5, 4:6, :]
                ob[0, 0, 4:8, :] = phi[4:8]
            start0()

        def finish():
            wait_recv()
            for d, (dx, dy) in enumerate(DIRS):
                xd, yd = 4 - n * dx, 4 - n * dy
                tile = ib[d, 2 if n == 4 else 0]
                for i in range(n):
                    v = lanes_back(tile, i)
                    buf[1, xd + i, yd : yd + n, :] = v[4 : 4 + n]
                    if n == 4:
                        r = 4 * (i // 2)
                        buf[0, xd + i, yd : yd + 4, :] = ib[d, i % 2, r : r + 4, :]
                    else:
                        buf[0, xd + i, yd : yd + 2, :] = tile[2 * i : 2 * i + 2]

        return start, finish, wait_send

    def gather(phase, src, buf):
        def copy(o):
            return pltpu.make_async_remote_copy(
                src_ref=src, dst_ref=buf.at[k], send_sem=gs.at[phase, o],
                recv_sem=gr.at[phase, o], device_id=(ix, iy, peer(o)),
                device_id_type=MESH,
            )

        def start():
            for o in range(1, ngz):
                copy(o).start()

        def wait_recv():
            for o in range(1, ngz):
                copy(o).wait_recv()

        def wait_send():
            for o in range(1, ngz):
                copy(o).wait_send()

        return start, wait_recv, wait_send

    sends = []

    def pick0(dx, dy):
        sx, tx = span(dx, 4, 32, 4)
        sy, ty = span(dy, 8, 32, 8)
        return S0.at[0, sx, sy, :], S0.at[0, tx, ty, :]

    load_f.wait()
    pl.semaphore_wait(barrier, count)
    h_start, h_recv, h_send = exchange(0, pick0)
    h_start()

    load_g.wait()
    a = [4.0 * e_ref[l] for l in range(5)]
    for l in range(5):
        rows[0, 2 * l : 2 * l + 1, :] = a[l] * g_ref[l, 0:1, :]
        rows[0, 2 * l + 1 : 2 * l + 2, :] = a[l] * g_ref[l, 127:128, :]
    for m in range(1, 4):
        prev = rows[m - 1]
        for l in range(5):
            nxt = a[l] * hdot(prev, g_ref[l])
            rows[m, 2 * l : 2 * l + 2, :] = nxt[2 * l : 2 * l + 2]
    for m in range(4):
        re0[2 * m : 2 * m + 2, :] = rows[m, 0:2, :]
    for p in range(16):
        l, m = pair_of(p)
        re1[2 * p : 2 * p + 2, :] = rows[m - 1, 2 * l : 2 * l + 2, :]
    lane16 = iota((16, 128), 1)
    tile = jnp.where(lane16 == 8, jnp.broadcast_to(zf_ref[0:1, 0:1], (16, 128)), 0.0)
    for n in range(4):
        rn = rows[n]
        tile = jnp.where(lane16 == 2 * n, jnp.broadcast_to(rn[:, 0:1], (16, 128)), tile)
        tile = jnp.where(lane16 == 2 * n + 1, jnp.broadcast_to(rn[:, 127:128], (16, 128)), tile)
    cgl[...] = tile
    cg[k] = tile

    c_start, c_recv, c_send = gather(0, cgl, cg)
    c_start()
    r0 = re0[...]
    for i in range(4):
        fx = S0[0, 4 + 8 * i : 12 + 8 * i, 8:40, :].reshape(256, 128)
        el0[:, 256 * i : 256 * i + 256] = dot3(r0, fx, True)
    e0[k] = el0[...]
    g0_start, g0_recv, g0_send = gather(1, el0, e0)
    g0_start()
    for l in range(1, 5):
        if l > 1:
            clear2(S[l])
        clear2(M[l])
    for name in MESSAGES:
        if name != "f1":
            clear(r_["in_" + name])

    def side_phi(i, c):
        S0[1, 4 + i, 0:8, :] = jnp.zeros((8, 128), f32)
        S0[1, 4 + i, 40:48, :] = jnp.zeros((8, 128), f32)
        return c
    lax.fori_loop(0, 32, side_phi, 0)

    h_recv()
    elh[:, 0:384] = dot3(
        r0, jnp.concatenate([S0[0, 0:4].reshape(192, 128), S0[0, 36:40].reshape(192, 128)], 0), True
    )
    fx = jnp.concatenate([S0[0, 4:36, 4:8, :], S0[0, 4:36, 40:44, :]], 1).reshape(256, 128)
    elh[:, 384:640] = dot3(r0, fx, True)
    eh[k] = elh[...]
    gh_start, gh_recv, gh_send = gather(3, elh, eh)
    gh_start()
    sends += [h_send, c_send, g0_send, gh_send]

    c_recv()
    CG = cg[0:8].reshape(128, 128)
    ri, ci = iota((128, 128), 0), iota((128, 128), 1)
    same = (ri >> 1) == (ci >> 1)
    odd = (ci & 1) == 1
    eye = jnp.where(ri == ci, 1.0, 0.0).astype(f32)

    def col(c):
        return jnp.broadcast_to(CG[:, c : c + 1], (128, 128))

    def corner(n):
        return jnp.where(same, jnp.where(odd, col(2 * n + 1), col(2 * n)), 0.0)

    lrow = (ri >> 1) & 7
    inva = jnp.zeros((128, 128), f32)
    for l in range(5):
        inva = jnp.where(lrow == l, 1.0 / a[l], inva)
    face = col(8)
    face_up = jnp.concatenate([face[16:], jnp.zeros((16, 128), f32)], 0)
    K = inva * (
        jnp.where(((ri & 1) == 0) & (ci == ri - 15), face, 0.0)
        + jnp.where(((ri & 1) == 1) & (ci == ri + 15), face_up, 0.0)
    )
    R = corner(0)
    blk = (ri >> 4) + (ri & 1)
    for st in (1, 2, 4):
        link = jnp.where((blk & (2 * st - 1)) == st, K, 0.0)
        d = R * eye
        drow = jnp.sum(d, 1, keepdims=True)
        dcol = jnp.sum(d, 0, keepdims=True)
        off = link / (1.0 - link * link * drow * dcol)
        diag = jnp.sum(off * link * dcol, 1, keepdims=True)
        R = R + hdot(hdot(R, off + eye * diag), R)
    W = eye + hdot(R, K)
    B2, B3, B4 = dot3(corner(1), K), dot3(corner(2), K), dot3(corner(3), K)
    V1 = dot3(W, dot3(B2, W))
    V2 = dot3(W, dot3(B3, W) + dot3(B2, V1))
    V3 = dot3(W, dot3(B4, W) + dot3(B3, V1) + dot3(B2, V2))
    VS = [W, V1, V2, V3]

    def lm_of(p):
        l = jnp.where(p < 12, (p >> 2) + 1, jnp.where(p < 14, 0, 4))
        m = jnp.where(p < 12, (p & 3) + 1, (p & 1) + 1)
        return l, m

    def funct(level):
        width = 64 if level == 0 else 256
        rr, rc = iota((128, 128), 0), iota((128, 128), 1)
        p, side = rr & 15, rr >> 4
        if level == 0:
            l, m = jnp.zeros_like(p), p - 11
            live = (rr < 32) & (p >= 12)
        else:
            l, m = lm_of(p)
            live = rr < 32
        target = jnp.where(side == 0, (k - 1) * 16 + l * 2 + 1, (k + 1) * 16 + l * 2)
        pick_rows = jnp.where(live & (rc == target), 1.0, 0.0).astype(f32)
        er, ec = iota((128, width), 0), iota((128, width), 1)
        if level == 0:
            jc, lc, mc, endc = ec >> 3, jnp.zeros_like(ec), ((ec >> 1) & 3) + 1, ec & 1
        else:
            jc, endc = ec >> 5, ec & 1
            lc, mc = lm_of((ec >> 1) & 15)
        expand = jnp.where(er == jc * 16 + lc * 2 + endc, 1.0, 0.0).astype(f32)
        wr = iota((128, width), 0)
        mrow = ((wr & 15) - 11) if level == 0 else lm_of(wr & 15)[1]
        out = jnp.zeros((128, width), f32)
        for n in range(4):
            x = dot3(dot3(pick_rows, VS[n]), expand)
            out = out + jnp.where(mrow - mc == n, x, 0.0)
        return out

    L0 = funct(0)
    L1 = funct(1)

    side_in, side_out = ri >> 4, ci >> 4
    pi, po = ri & 15, ci & 15
    fl = (ri < 32) & (ci < 32) & (side_in == side_out)
    li, mi = lm_of(pi)
    lo, mo = lm_of(po)
    aout = jnp.zeros((128, 128), f32)
    for l in range(5):
        aout = jnp.where(lo == l, a[l], aout)
    cm = jnp.broadcast_to(zf_ref[0:1, 0:1], (1, 128))
    cp = jnp.broadcast_to(cg[k + 1, 0:1, 8:9], (1, 128))
    for l in range(5):
        gt = g_ref[l].T
        p1 = pid(l, 1)
        ut = jnp.where(ri == p1, jnp.broadcast_to(cm * gt[0:1], (128, 128)), 0.0)
        ut = jnp.where(ri == 16 + p1, jnp.broadcast_to(cp * gt[127:128], (128, 128)), ut)
        if l == 0:
            q = jnp.where(fl & (pi >= 13) & (pi == po + 1), 1.0, 0.0)
        else:
            den = jnp.where(lo == l, 1.0, a[l] - aout)
            amp = a[l] / den
            nb = -aout / den
            p2 = nb * nb
            p3 = p2 * nb
            dm = mo - mi
            pw = jnp.where(dm == 0, 1.0, jnp.where(dm == 1, nb, jnp.where(dm == 2, p2, p3)))
            pm = jnp.where(mo == 1, nb, jnp.where(mo == 2, p2, jnp.where(mo == 3, p3, p2 * p2)))
            q = jnp.where((li == lo) & (dm >= 0), amp * pw, 0.0)
            q = q + jnp.where((li == l) & (mi == 1), pm, 0.0)
            q = jnp.where(lo == l, jnp.where((li == l) & (mi == mo + 1), 1.0, 0.0), q)
            q = jnp.where(fl, q, 0.0)
        for r, v in ((0, a[l] * gt), (128, ut)):
            vh, vl = split(v)
            th[l, r : r + 128, 0:128] = vh
            tl[l, r : r + 128, 0:128] = vl
        qh, ql = split(q.astype(f32))
        zero = jnp.zeros((128, 128), bf16)
        th[l, 0:128, 128:256] = zero
        tl[l, 0:128, 128:256] = zero
        th[l, 128:256, 128:256] = qh
        tl[l, 128:256, 128:256] = ql

    gt = a[0] * g_ref[0].T
    gh, gl = split(gt)
    ra[0:128, 0:128] = gh
    ra[128:256, 0:128] = gh
    ra[0:128, 128:256] = gl
    ra[128:256, 128:256] = jnp.zeros((128, 128), bf16)
    gt = g_ref[0].T
    for i in range(4):
        row = ri & 31
        u = jnp.where(row == 12 + i, jnp.broadcast_to(cm * gt[0:1], (128, 128)), 0.0)
        u = jnp.where(row == 28 + i, jnp.broadcast_to(cp * gt[127:128], (128, 128)), u)
        uh, ul = split(u)
        u = jnp.where(ri < 64, uh.astype(f32), jnp.where(ri < 96, ul.astype(f32), 0.0))
        ub[:, 128 * i : 128 * i + 128] = u.astype(bf16)

    def apply(l, src, dst, step, n, scale=None):
        y = src.shape[2]

        def body(i, c):
            x = pl.ds(i * step, step)
            v = jnp.concatenate(
                [src[0, x].reshape(step * y, 128), src[1, x].reshape(step * y, 128)], 1
            )
            vh, vl = split(v)
            t = mm(vh, th[l]) + (mm(vh, tl[l]) + mm(vl, th[l]))
            if scale is not None:
                t = scale * t
            dst[0, x] = t[:, 0:128].reshape(step, y, 128)
            dst[1, x] = t[:, 128:256].reshape(step, y, 128)
            return c

        lax.fori_loop(0, n, body, 0)

    def stencil(l, src, dst, grow, post, halves=(0, 1)):
        ox, oy, n, y = OX[l], OY[l], LX[l], SY[l]
        gy0 = iota((y, 128), 0) + (iy * n - oy)
        ym = jnp.where((gy0 >= 0) & (gy0 < ngy * n), 0.25, 0.0).astype(f32)

        def body(x, c):
            gx0 = ix * n + x - ox
            s = jnp.where((gx0 >= 0) & (gx0 < ngx * n), 1.0, 0.0).astype(f32)
            m4 = ym * s
            for h in halves:
                v = src[h, x]
                t = (src[h, x - 1] + src[h, x + 1]) + (
                    pltpu.roll(v, 1, 0) + pltpu.roll(v, y - 1, 0)
                )
                dst(h, x, post(h, x, m4 * t))
            return c

        lax.fori_loop(ox - grow, ox + n + grow, body, 0)

    def into(ref):
        def put(h, x, v):
            ref[h, x] = v
        return put

    def solve(l, src, dst, matrix=None, scale=None):
        step, n = SX[l], 1
        apply(l if matrix is None else matrix, src, dst, step, n, scale)

    def residual(l, halves=(0, 1)):
        s, ta, tb = S[l], at("TA", l), at("TB", l)
        aa, bb = at("AA", l), at("BB", l)
        solve(l, s, ta)
        solve(l, ta, tb)
        stencil(l, tb, into(bb), 1, lambda h, x, v: 0.32 * ta[h, x] + 0.64 * v, halves)
        stencil(l, bb, into(aa), 0, lambda h, x, v: 0.04 * s[h, x] + v, halves)

    def smoothed(l):
        w = 0
        s, ta, tb, tc = S[l], at("TA", l), at("TB", l), at("TC", l)
        bb, cc, ma = at("BB", l), at("CC", l), at("MA", l)
        solve(l, tb, tc)
        stencil(l, tc, into(bb), 2 + w, lambda h, x, v: 0.8192 * tb[h, x] + 0.4096 * v)
        stencil(l, bb, into(cc), 1 + w, lambda h, x, v: 0.9728 * ta[h, x] + v)
        stencil(l, cc, into(ma), w, lambda h, x, v: 0.9984 * s[h, x] + v)

    def restrict(l, put, halves=(0, 1)):
        ox, oy, n = OX[l], OY[l], LX[l] // 2
        aa = at("AA", l)

        def body(i, c):
            x = ox + 2 * i
            for h in halves:
                even, off = pl.ds(oy, n, 2), pl.ds(oy + 1, n, 2)
                v = (aa[h, x, even, :] + aa[h, x, off, :]) + (
                    aa[h, x + 1, even, :] + aa[h, x + 1, off, :]
                )
                put(h, i, 0.25 * v)
            return c

        lax.fori_loop(0, n, body, 0)

    def prolong(l, fields, outs, halves):
        c = l + 1
        w = 1 if l == 0 else 0
        n, ox, oc, y = LX[c], OX[l], OX[c], SY[c]
        ys, cnt = [(4, 24), (4, 16), (0, 12), (2, 8)][l]
        gyc = iota((cnt, 128), 0) + (iy * n + ys - OY[c])
        ym = jnp.where((gyc >= 0) & (gyc < ngy * n), 1.0, 0.0).astype(f32)

        def body(j, carry):
            j = j - (1 + w)
            gx = ix * n + j
            s = jnp.where((gx >= 0) & (gx < ngx * n), 1.0, 0.0).astype(f32)
            ms = ym * s
            for h in halves:
                lower, here, upper = (fields(h, oc + j + i) for i in (-1, 0, 1))
                for (o, oh), lo_, he, up_ in zip(outs, lower, here, upper):
                    oh = h if oh is None else oh
                    for i, far in enumerate((lo_, up_)):
                        v = 0.75 * he + 0.25 * far
                        ev = (0.75 * v + 0.25 * pltpu.roll(v, 1, 0))[ys : ys + cnt]
                        od = (0.75 * v + 0.25 * pltpu.roll(v, y - 1, 0))[ys : ys + cnt]
                        o[oh, ox + 2 * j + i, pl.ds(0, cnt, 2), :] = ms * ev
                        o[oh, ox + 2 * j + i, pl.ds(1, cnt, 2), :] = ms * od
            return carry

        lax.fori_loop(0, n + 2 + 2 * w, body, 0)

    def correct(l, store):
        c = l + 1
        m, u, g2 = M[c], at("U", c), at("V", c)
        kap = a[l] / a[c]
        solve(c, m, u, c, kap)
        solve(c, u, g2, l, 0.64)
        q = 0.04 * (1.0 - a[c] / a[l])
        outs = [at("P0", l), at("P1", l), at("P2", l)]

        def fields(h, x):
            uv = u[h, x]
            return (0.04 * m[h, x] + q * uv, 0.32 * uv, g2[h, x])

        prolong(l, fields, [(o, None) for o in outs], (0, 1))
        cc, ma = at("CC", l), at("MA", l)
        stencil(l, outs[2], into(cc), 1, lambda h, x, v: outs[1][h, x] + v)
        stencil(l, cc, store, 0, lambda h, x, v: (ma[h, x] + outs[0][h, x]) + v)

    def parts(et):
        phi = dot3(L0, et).T
        h, lo_ = split(phi)
        h, lo_ = h.astype(f32), lo_.astype(f32)
        return h + pltpu.roll(lo_, 32, 1) + pltpu.roll(h, 64, 1)

    def outside(first):
        def chunk(i, c):
            x = pl.ds(i * 8, 8)
            w = S0[1, x].reshape(384, 128).astype(bf16)
            t = mm(w, ub[:, 128 * first : 128 * first + 256])
            C0[first, x] = t[:, 0:128].reshape(8, 48, 128)
            C0[first + 1, x] = t[:, 128:256].reshape(8, 48, 128)
            return c
        lax.fori_loop(0, 5, chunk, 0)

    def power(i, src, dst):
        def chunk(j, c):
            x = pl.ds(j * 8, 8)
            vh, vl = split(src[0, x].reshape(384, 128))
            t = mm(jnp.concatenate([vh, vl], 1), ra[...])
            dst[0, x] = (t[:, 0:128] + t[:, 128:256]).reshape(8, 48, 128) + C0[i, x]
            return c
        lax.fori_loop(0, 5, chunk, 0)

    g0_recv()
    for i in range(4):
        w = parts(e0[:, :, 256 * i : 256 * i + 256].reshape(64, 256))
        S0[1, 4 + 8 * i : 12 + 8 * i, 8:40, :] = w.reshape(8, 32, 128)
    gh_recv()
    w = parts(eh[:, :, 0:384].reshape(64, 384))
    S0[1, 0:4] = w[0:192].reshape(4, 48, 128)
    S0[1, 36:40] = w[192:384].reshape(4, 48, 128)
    w = parts(eh[:, :, 384:640].reshape(64, 256)).reshape(32, 8, 128)
    S0[1, 4:36, 4:8, :] = w[:, 0:4]
    S0[1, 4:36, 40:44, :] = w[:, 4:8]

    t1, t2, t3, t4 = at("TA", 0), at("TB", 0), at("TC", 0), at("P0", 0)
    aa0, bb0, cc0, ma0 = at("AA", 0), at("BB", 0), at("CC", 0), at("MA", 0)
    outside(0)
    power(0, S0, t1)
    power(1, t1, t2)
    stencil(0, t2, into(bb0), 1, lambda h, x, v: 0.32 * t1[h, x] + 0.64 * v, (0,))
    stencil(0, bb0, into(aa0), 0, lambda h, x, v: 0.04 * S0[h, x] + v, (0,))

    def put1(h, i, v):
        S1[h, 3 + i, 8:24, :] = v
    restrict(0, put1, (0,))
    x1_start, x1_recv, x1_send = halo(1, S1, 0, 3, 16, 3)
    x1_start()
    el1[...] = dot3(re1[...], S1[0, 3:19, 8:24, :].reshape(256, 128), True)
    e1[k] = el1[...]
    g1_start, g1_recv, g1_send = gather(2, el1, e1)
    g1_start()

    outside(2)
    power(2, t2, t3)
    power(3, t3, t4)

    def both0(h, x, v):
        bb0[0, x] = 0.8192 * t3[0, x] + 0.4096 * v
        bb0[1, x] = 0.4096 * (t3[0, x] + v)
    stencil(0, t4, both0, 3, lambda h, x, v: v, (0,))
    stencil(0, bb0, into(cc0), 2, lambda h, x, v: (0.1536 if h else 0.9728) * t2[0, x] + v)
    stencil(0, cc0, into(aa0), 1, lambda h, x, v: (0.0256 if h else 0.9984) * t1[0, x] + v)
    stencil(0, aa0, into(ma0), 0, lambda h, x, v: 0.0016 * S0[0, x] + v, (1,))

    g1_recv()
    phi = dot3(L1, e1[...].reshape(256, 256))
    S1[1, 3:19, 8:24, :] = phi.T.reshape(16, 16, 128)
    y1_start, y1_finish, y1_send = packed(2, 1, "f1", S1, False)
    y1_start()
    x1_recv()
    y1_finish()
    residual(1)

    def put2(h, i, v):
        S2[h, 3 + i, 8:16, :] = v
    restrict(1, put2)
    x2_start, x2_finish, x2_send = packed(3, 2, "s2", S2)
    x2_start()
    smoothed(1)

    x2_finish()
    residual(2)

    def put3(h, i, v):
        S3[h, 4 + i, 4:8, :] = v
    restrict(2, put3)
    x3_start, x3_finish, x3_send = packed_block(4, 3, "s3", S3)
    x3_start()
    smoothed(2)

    x3_finish()
    residual(3)

    def put4(h, i, v):
        S4[h, 4 + i, 4:6, :] = v
    restrict(3, put4)
    x4_start, x4_finish, x4_send = packed_block(5, 4, "s4", S4)
    x4_start()
    smoothed(3)

    x4_finish()
    ta4 = at("TA", 4)
    solve(4, S4, ta4)

    def putm4(h, x, v):
        M4[h, x, 4:6, :] = v[4:6]
    stencil(4, ta4, putm4, 0, lambda h, x, v: 0.96 * S4[h, x] + 0.64 * v)
    z4_start, z4_finish, z4_send = packed_block(6, 4, "m4", M4)
    z4_start()
    z4_finish()

    def putm3(h, x, v):
        M3[h, x, 4:8, :] = v[4:8]
    correct(3, putm3)
    z3_start, z3_finish, z3_send = packed_block(7, 3, "m3", M3)
    z3_start()
    z3_finish()

    def putm2(h, x, v):
        M2[h, x, 8:16, :] = v[8:16]
    correct(2, putm2)
    z2_start, z2_finish, z2_send = packed(8, 2, "m2", M2)
    z2_start()
    z2_finish()

    def putm1(h, x, v):
        M1[h, x, 8:24, :] = v[8:24]
    correct(1, putm1)
    z1_start, z1_finish, z1_send = packed(9, 1, "m1", M1)
    z1_start()
    z1_finish()

    u, g2 = at("U", 1), at("V", 1)
    kap = a[0] / a[1]
    solve(1, M1, u, 1, kap)
    solve(1, u, g2, 0, 0.64)
    solve(1, M1, HM, 0)
    solve(1, g2, H2, 0)
    q = 0.04 * (1.0 - a[1] / a[0])

    def fields0(h, x):
        uv, gv = u[0, x], g2[0, x]
        h0 = 0.04 * HM[0, x] + (q / 0.64) * gv
        return (0.04 * M1[0, x] + q * uv, h0 - 0.32 * uv, 0.5 * gv, H2[0, x], h0)

    P0, P1, P2 = at("P0", 0), at("P1", 0), at("P2", 0)
    prolong(0, fields0, [(P0, 0), (P0, 1), (P1, 0), (P1, 1), (P2, 0)], (0,))

    def pair(h, x, v):
        bb0[0, x] = v - P1[0, x]
        bb0[1, x] = v + P1[0, x]
    stencil(0, P1, pair, 2, lambda h, x, v: v, (1,))
    stencil(0, bb0, into(cc0), 1, lambda h, x, v: P0[1, x] + v, (0,))
    inv0 = 1.0 / a[0]

    def put_sol(h, x, v):
        sol_ref[x - 4] = v[8:40]

    def put_res(h, x, v):
        res_ref[x - 4] = v[8:40]
    stencil(0, bb0, put_sol, 0, lambda h, x, v: inv0 * ((aa0[0, x] + P2[0, x]) + v), (1,))
    stencil(0, cc0, put_res, 0, lambda h, x, v: (ma0[1, x] - P0[0, x]) + v, (0,))

    for wait in sends + [
        x1_send, g1_send, y1_send, x2_send, x3_send, x4_send, z4_send, z3_send, z2_send, z1_send
    ]:
        wait()


def body(sizes, right_side, z_faces, xy_coupling, block_inverse):
    n = right_side.shape
    vmem = pl.BlockSpec(memory_space=pltpu.VMEM)
    hbm = pl.BlockSpec(memory_space=pl.ANY)
    scratch = [pltpu.VMEM(s, f32) for s in scratch_shapes().values()]
    scratch += [pltpu.VMEM((5, 128, 128), f32)]
    scratch += [pltpu.VMEM((5, 256, 256), bf16), pltpu.VMEM((5, 256, 256), bf16)]
    scratch += [pltpu.VMEM((256, 256), bf16), pltpu.VMEM((128, 512), bf16)]
    scratch += [pltpu.SemaphoreType.DMA((10, 8)), pltpu.SemaphoreType.DMA((10, 8))]
    scratch += [pltpu.SemaphoreType.DMA((4, 8)), pltpu.SemaphoreType.DMA((4, 8))]
    scratch += [pltpu.SemaphoreType.DMA((2,))]
    return pl.pallas_call(
        lambda *r: kernel(sizes, *r),
        out_shape=(pltpu.VMEM(n, f32), pltpu.VMEM(n, f32)),
        in_specs=[hbm, vmem, hbm, pl.BlockSpec(memory_space=pltpu.SMEM)],
        out_specs=(vmem, vmem),
        scratch_shapes=scratch,
        compiler_params=pltpu.CompilerParams(
            collective_id=0, has_side_effects=True, vmem_limit_bytes=60 * 2**20
        ),
        name="vcycle",
    )(right_side, z_faces.reshape(1, -1), block_inverse, xy_coupling)


def solution(mesh):
    sizes = tuple(mesh.shape[n] for n in ("gx", "gy", "gz"))
    return jax.shard_map(
        lambda *args: body(sizes, *args),
        mesh=mesh,
        in_specs=(P("gx", "gy", "gz"), P("gz"), P(), P(None, "gz", None)),
        out_specs=(P("gx", "gy", "gz"), P("gx", "gy", "gz")),
        check_vma=False,
    )
```

```python
import jax
import jax.numpy as jnp
from jax import lax
from jax.experimental import pallas as pl
from jax.experimental.pallas import tpu as pltpu
from jax.sharding import PartitionSpec as P

f32 = jnp.float32
bf16 = jnp.bfloat16
HI = lax.Precision.HIGHEST
MESH = pl.DeviceIdType.MESH
FAR = [(dx, dy) for dx in (-2, -1, 0, 1, 2) for dy in (-2, -1, 0, 1, 2) if 0 < abs(dx) + abs(dy) < 4]
DIRS = [(dx, dy) for dx in (-1, 0, 1) for dy in (-1, 0, 1) if (dx, dy) != (0, 0)]

LX = [32, 16, 8, 4, 2]
OX = [4, 3, 3, 4, 4]
OY = [8, 4, 4, 4, 4]
SX = [40, 22, 14, 12, 10]
SY = [48, 24, 16, 16, 16]


def pair_of(p):
    if p < 12:
        return p // 4 + 1, p % 4 + 1
    return (0 if p < 14 else 4), p % 2 + 1


def pid(l, m):
    if l == 0:
        return 11 + m
    if l == 4:
        return 13 + m
    return (l - 1) * 4 + m - 1


def split(x):
    h = x.astype(bf16)
    return h, (x - h.astype(f32)).astype(bf16)


def mm(a, b, trans_b=False):
    dims = (((1,), (1 if trans_b else 0,)), ((), ()))
    return lax.dot_general(a, b, dims, preferred_element_type=f32)


def dot3(a, b, trans_b=False):
    ah, al = split(a)
    bh, bl = split(b)
    return mm(ah, bh, trans_b) + (mm(ah, bl, trans_b) + mm(al, bh, trans_b))


def hdot(a, b):
    return jnp.dot(a, b, precision=HI, preferred_element_type=f32)


def iota(shape, dim):
    return lax.broadcasted_iota(jnp.int32, shape, dim)


MESSAGES = {"f0": 16, "g1": 8, "f1": 2, "s2": 5, "s3": 3, "s4": 1, "m3": 3, "m2": 5, "m1": 10}


def scratch_shapes():
    out = {}
    for l in range(5):
        out[f"S{l}"] = (2, SX[l], SY[l], 128)
        for t in ("TA", "TB", "TC", "AA", "BB", "CC", "MA", "P0", "P1", "P2"):
            out[f"{t}{l}"] = (2, SX[l], SY[l], 128)
        if l:
            for t in ("M", "U", "V"):
                out[f"{t}{l}"] = (2, SX[l], SY[l], 128)
    out["HM"] = out["H2"] = (2, SX[1], SY[1], 128)
    for name, tiles in MESSAGES.items():
        out["out_" + name] = out["in_" + name] = (len(FAR) if name == "s4" else 8, tiles, 8, 128)
    out["rows"] = (4, 16, 128)
    out["re0"] = (8, 128)
    out["re1"] = (32, 128)
    out["cg"] = (9, 16, 128)
    out["cgl"] = out["cgl2"] = (16, 128)
    out["cg2"] = (8, 16, 128)
    out["e0"] = (8, 8, 1024)
    out["eh"] = (8, 8, 640)
    out["e1"] = (8, 32, 256)
    out["el0"] = (8, 1024)
    out["elh"] = (8, 640)
    out["el1"] = (32, 256)
    return out


def kernel(sizes, f_ref, zf_ref, ginv_ref, e_ref, sol_ref, res_ref, *refs):
    names = list(scratch_shapes())
    r_ = dict(zip(names, refs))
    g_ref, th, tl, ra, ub, hs, hr, gs, gr, ls = refs[len(names):]
    S0, S1, S2, S3, S4 = [r_[f"S{l}"] for l in range(5)]
    M1, M2, M3, M4 = [r_[f"M{l}"] for l in range(1, 5)]
    rows, re0, re1, cg, cgl = r_["rows"], r_["re0"], r_["re1"], r_["cg"], r_["cgl"]
    e0, e1, el0, el1 = r_["e0"], r_["e1"], r_["el0"], r_["el1"]
    eh, elh, HM, H2 = r_["eh"], r_["elh"], r_["HM"], r_["H2"]
    cg2, cgl2 = r_["cg2"], r_["cgl2"]

    ngx, ngy, ngz = sizes
    ix, iy, k = lax.axis_index("gx"), lax.axis_index("gy"), lax.axis_index("gz")
    S = [S0, S1, S2, S3, S4]
    M = [None, M1, M2, M3, M4]

    def at(name, l):
        return r_[f"{name}{l}"]


    def peer(o):
        return jnp.where(k + o >= ngz, k + o - ngz, k + o)

    def exists(dx, dy):
        x, y = ix + dx, iy + dy
        return (x >= 0) & (x < ngx) & (y >= 0) & (y < ngy)

    def clear(ref):
        def step(i, c):
            ref[i] = jnp.zeros(ref.shape[1:], f32)
            return c
        lax.fori_loop(0, ref.shape[0], step, 0)

    def clear2(ref):
        def step(i, c):
            for h in range(2):
                ref[h, i] = jnp.zeros(ref.shape[2:], f32)
            return c
        lax.fori_loop(0, ref.shape[1], step, 0)

    load_f = pltpu.make_async_copy(f_ref, S0.at[0, 4:36, 8:40, :], ls.at[0])
    load_g = pltpu.make_async_copy(ginv_ref, g_ref, ls.at[1])
    load_f.start()
    load_g.start()

    def edge(i, c):
        S0[0, i] = jnp.zeros((48, 128), f32)
        S0[0, 36 + i] = jnp.zeros((48, 128), f32)
        return c
    lax.fori_loop(0, 4, edge, 0)

    def sides(i, c):
        S0[0, 4 + i, 0:8, :] = jnp.zeros((8, 128), f32)
        S0[0, 4 + i, 40:48, :] = jnp.zeros((8, 128), f32)
        return c
    lax.fori_loop(0, 32, sides, 0)
    for name in ("f0", "g1", "f1"):
        clear(r_["in_" + name])
    clear(rows)
    if ngz < 8:
        for r in (e0, eh, e1, cg2):
            clear(r)
    clear(cg)

    barrier = pltpu.get_barrier_semaphore()
    count = jnp.int32(ngz - 1)
    for dx, dy in FAR:
        ok = exists(dx, dy)

        @pl.when(ok)
        def _():
            pl.semaphore_signal(
                barrier, inc=1, device_id=(ix + dx, iy + dy, k), device_id_type=MESH
            )

        count = count + jnp.where(ok, 1, 0)
    for o in range(1, ngz):
        pl.semaphore_signal(
            barrier, inc=1, device_id=(ix, iy, peer(o)), device_id_type=MESH
        )

    def exchange(phase, pick, dirs=DIRS):
        def copy(d, dx, dy):
            src, dst = pick(dx, dy)
            return pltpu.make_async_remote_copy(
                src_ref=src, dst_ref=dst, send_sem=hs.at[phase, d], recv_sem=hr.at[phase, d],
                device_id=(ix + dx, iy + dy, k), device_id_type=MESH,
            )

        def start():
            for d, (dx, dy) in enumerate(dirs):
                @pl.when(exists(dx, dy))
                def _():
                    copy(d, dx, dy).start()

        def wait_recv():
            for d, (dx, dy) in enumerate(dirs):
                @pl.when(exists(-dx, -dy))
                def _():
                    copy(d, dx, dy).wait_recv()

        def wait_send():
            for d, (dx, dy) in enumerate(dirs):
                @pl.when(exists(dx, dy))
                def _():
                    copy(d, dx, dy).wait_send()

        return start, wait_recv, wait_send

    def span(d, off, n, h):
        if d == 0:
            return pl.ds(off, n), pl.ds(off, n)
        if d == 1:
            return pl.ds(off + n - h, h), pl.ds(off - h, h)
        return pl.ds(off, h), pl.ds(off + n, h)

    def lanes_of(planes):
        out = planes[0]
        for i, v in enumerate(planes[1:]):
            out = out + pltpu.roll(v, 32 * (i + 1), 1)
        return out

    low_lanes = {r: iota((r, 128), 1) < 32 for r in (8,)}

    def lanes_back(tile, i):
        v = tile if i == 0 else pltpu.roll(tile, 128 - 32 * i, 1)
        return jnp.where(low_lanes[8], v, 0.0)

    def tiles_of(l, dx, dy, wf, wp):
        n = LX[l]
        if dx == 0:
            return (n // 2 if wf else 0) + ((n + 7) // 8 if wp else 0)
        if dy == 0:
            return (3 * n // 8 if wf else 0) + (n // 8 if wp else 0)
        return 2 if wf else 1

    def packed(phase, l, name, buf, wf=True, wp=True):
        n, ox, oy = LX[l], OX[l], OY[l]
        ob, ib = r_["out_" + name], r_["in_" + name]

        def pick(dx, dy):
            d, t = DIRS.index((dx, dy)), tiles_of(l, dx, dy, wf, wp)
            return ob.at[d, 0:t], ib.at[d, 0:t]

        start0, wait_recv, wait_send = exchange(phase, pick)

        def start():
            for d, (dx, dy) in enumerate(DIRS):
                xs = ox + n - 3 if dx == 1 else ox
                ys = oy + n - 4 if dy == 1 else oy
                yt = ys // 8 * 8
                part = slice(ys - yt, ys - yt + 4)
                if dx == 0:
                    base = n // 2 if wf else 0
                    if wf:
                        for t in range(n // 2):
                            ob[d, t, 0:4, :] = buf[0, ox + t, ys : ys + 4, :]
                            ob[d, t, 4:8, :] = buf[0, ox + t + n // 2, ys : ys + 4, :]
                    if wp:
                        for b in range(n // 4):
                            v = lanes_of([buf[1, ox + 4 * b + i, yt : yt + 8, :] for i in range(4)])
                            r = 4 * (b % 2)
                            ob[d, base + b // 2, r : r + 4, :] = v[part]
                elif dy == 0:
                    m = n // 8
                    base = 3 * m if wf else 0
                    for r in range(m):
                        y = slice(oy + 8 * r, oy + 8 * r + 8)
                        if wf:
                            for i in range(3):
                                ob[d, i * m + r] = buf[0, xs + i, y, :]
                        if wp:
                            ob[d, base + r] = lanes_of([buf[1, xs + i, y, :] for i in range(3)])
                else:
                    if wf:
                        ob[d, 0, 0:4, :] = buf[0, xs, ys : ys + 4, :]
                        ob[d, 0, 4:8, :] = buf[0, xs + 1, ys : ys + 4, :]
                        ob[d, 1, 0:4, :] = buf[0, xs + 2, ys : ys + 4, :]
                    if wp:
                        v = lanes_of([buf[1, xs + i, yt : yt + 8, :] for i in range(3)])
                        ob[d, 1 if wf else 0, 4:8, :] = v[part]
            start0()

        def finish():
            wait_recv()
            for d, (dx, dy) in enumerate(DIRS):
                xd = ox - 3 if dx == 1 else ox + n
                yd = oy - 4 if dy == 1 else oy + n
                if dx == 0:
                    base = n // 2 if wf else 0
                    if wf:
                        for t in range(n // 2):
                            buf[0, ox + t, yd : yd + 4, :] = ib[d, t, 0:4, :]
                            buf[0, ox + t + n // 2, yd : yd + 4, :] = ib[d, t, 4:8, :]
                    if wp:
                        for b in range(n // 4):
                            tile, r = ib[d, base + b // 2], 4 * (b % 2)
                            for i in range(4):
                                v = lanes_back(tile, i)
                                buf[1, ox + 4 * b + i, yd : yd + 4, :] = v[r : r + 4]
                elif dy == 0:
                    m = n // 8
                    base = 3 * m if wf else 0
                    for r in range(m):
                        y = slice(oy + 8 * r, oy + 8 * r + 8)
                        for i in range(3):
                            if wf:
                                buf[0, xd + i, y, :] = ib[d, i * m + r]
                            if wp:
                                buf[1, xd + i, y, :] = lanes_back(ib[d, base + r], i)
                else:
                    if wf:
                        buf[0, xd, yd : yd + 4, :] = ib[d, 0, 0:4, :]
                        buf[0, xd + 1, yd : yd + 4, :] = ib[d, 0, 4:8, :]
                        buf[0, xd + 2, yd : yd + 4, :] = ib[d, 1, 0:4, :]
                    if wp:
                        tile = ib[d, 1 if wf else 0]
                        for i in range(3):
                            buf[1, xd + i, yd : yd + 4, :] = lanes_back(tile, i)[4:8]

        return start, finish, wait_send

    def packed_block(phase, l, name, buf, dirs=DIRS):
        n = LX[l]
        ob, ib = r_["out_" + name], r_["in_" + name]

        def pick(dx, dy):
            return ob.at[0], ib.at[dirs.index((dx, dy))]

        start0, wait_recv, wait_send = exchange(phase, pick, dirs)

        def start():
            phi = lanes_of([buf[1, 4 + i, 0:8, :] for i in range(n)])
            if n == 4:
                for i in range(4):
                    r = 4 * (i // 2)
                    ob[0, i % 2, r : r + 4, :] = buf[0, 4 + i, 4:8, :]
                ob[0, 2] = phi
            else:
                ob[0, 0, 0:2, :] = buf[0, 4, 4:6, :]
                ob[0, 0, 2:4, :] = buf[0, 5, 4:6, :]
                ob[0, 0, 4:8, :] = phi[4:8]
            start0()

        def finish():
            wait_recv()
            for d, (dx, dy) in enumerate(dirs):
                xd, yd = 4 - n * dx, 4 - n * dy
                tile = ib[d, 2 if n == 4 else 0]
                for i in range(n):
                    v = lanes_back(tile, i)
                    buf[1, xd + i, yd : yd + n, :] = v[4 : 4 + n]
                    if n == 4:
                        r = 4 * (i // 2)
                        buf[0, xd + i, yd : yd + 4, :] = ib[d, i % 2, r : r + 4, :]
                    else:
                        buf[0, xd + i, yd : yd + 2, :] = tile[2 * i : 2 * i + 2]

        return start, finish, wait_send

    def gather(phase, src, buf):
        def copy(o):
            return pltpu.make_async_remote_copy(
                src_ref=src, dst_ref=buf.at[k], send_sem=gs.at[phase, o],
                recv_sem=gr.at[phase, o], device_id=(ix, iy, peer(o)),
                device_id_type=MESH,
            )

        def start():
            for o in range(1, ngz):
                copy(o).start()

        def wait_recv():
            for o in range(1, ngz):
                copy(o).wait_recv()

        def wait_send():
            for o in range(1, ngz):
                copy(o).wait_send()

        return start, wait_recv, wait_send

    sends = []
    ob0, ib0 = r_["out_f0"], r_["in_f0"]

    def pick0(dx, dy):
        d = DIRS.index((dx, dy))
        if dy == 0:
            sx, tx = span(dx, 4, 32, 4)
            return S0.at[0, sx, 8:40, :], S0.at[0, tx, 8:40, :]
        t = 16 if dx == 0 else 2
        return ob0.at[d, 0:t], ib0.at[d, 0:t]

    def ends0(dx):
        return 32 if dx == 1 else 4

    a = [4.0 * e_ref[l] for l in range(5)]
    lane16 = iota((16, 128), 1)

    def corner_tile(first, last, tile):
        for n in range(first, last):
            rn = rows[n]
            tile = jnp.where(lane16 == 2 * n, jnp.broadcast_to(rn[:, 0:1], (16, 128)), tile)
            tile = jnp.where(lane16 == 2 * n + 1, jnp.broadcast_to(rn[:, 127:128], (16, 128)), tile)
        return tile

    load_g.wait()
    for l in range(5):
        rows[0, 2 * l : 2 * l + 1, :] = a[l] * g_ref[l, 0:1, :]
        rows[0, 2 * l + 1 : 2 * l + 2, :] = a[l] * g_ref[l, 127:128, :]
    tile = corner_tile(
        0, 1, jnp.where(lane16 == 8, jnp.broadcast_to(zf_ref[0:1, 0:1], (16, 128)), 0.0)
    )
    cgl[...] = tile
    cg[k] = tile
    load_f.wait()
    for d, (dx, dy) in enumerate(DIRS):
        ys = 36 if dy == 1 else 8
        if dy != 0 and dx == 0:
            for t in range(16):
                ob0[d, t, 0:4, :] = S0[0, 4 + t, ys : ys + 4, :]
                ob0[d, t, 4:8, :] = S0[0, 20 + t, ys : ys + 4, :]
        elif dy != 0:
            for t in range(4):
                r = 4 * (t % 2)
                ob0[d, t // 2, r : r + 4, :] = S0[0, ends0(dx) + t, ys : ys + 4, :]

    pl.semaphore_wait(barrier, count)
    h_start, h_recv, h_send = exchange(0, pick0)
    h_start()
    c_start, c_recv, c_send = gather(0, cgl, cg)
    c_start()

    for m in range(4):
        if m > 0:
            prev = rows[m - 1]
            for l in range(5):
                nxt = a[l] * hdot(prev, g_ref[l])
                rows[m, 2 * l : 2 * l + 2, :] = nxt[2 * l : 2 * l + 2]
        re0[2 * m : 2 * m + 2, :] = rows[m, 0:2, :]
    r0 = re0[...]
    for i in range(4):
        fx = S0[0, 4 + 8 * i : 12 + 8 * i, 8:40, :].reshape(256, 128)
        el0[:, 256 * i : 256 * i + 256] = dot3(r0, fx, True)
    e0[k] = el0[...]
    g0_start, g0_recv, g0_send = gather(1, el0, e0)
    g0_start()
    tile = corner_tile(1, 4, jnp.zeros((16, 128), f32))
    cgl2[...] = tile
    cg2[k] = tile
    c2_start, c2_recv, c2_send = gather(4, cgl2, cg2)
    c2_start()

    for p in range(16):
        l, m = pair_of(p)
        re1[2 * p : 2 * p + 2, :] = rows[m - 1, 2 * l : 2 * l + 2, :]
    for l in range(1, 5):
        clear2(S[l])
        clear2(M[l])
    for name in MESSAGES:
        if name not in ("f0", "g1", "f1"):
            clear(r_["in_" + name])

    def side_phi(i, c):
        S0[1, 4 + i, 0:8, :] = jnp.zeros((8, 128), f32)
        S0[1, 4 + i, 40:48, :] = jnp.zeros((8, 128), f32)
        return c
    lax.fori_loop(0, 32, side_phi, 0)

    h_recv()
    for d, (dx, dy) in enumerate(DIRS):
        yd = 4 if dy == 1 else 40
        if dy != 0 and dx == 0:
            for t in range(16):
                S0[0, 4 + t, yd : yd + 4, :] = ib0[d, t, 0:4, :]
                S0[0, 20 + t, yd : yd + 4, :] = ib0[d, t, 4:8, :]
        elif dy != 0:
            for t in range(4):
                r = 4 * (t % 2)
                S0[0, (0 if dx == 1 else 36) + t, yd : yd + 4, :] = ib0[d, t // 2, r : r + 4, :]
    elh[:, 0:384] = dot3(
        r0, jnp.concatenate([S0[0, 0:4].reshape(192, 128), S0[0, 36:40].reshape(192, 128)], 0), True
    )
    fx = jnp.concatenate([S0[0, 4:36, 4:8, :], S0[0, 4:36, 40:44, :]], 1).reshape(256, 128)
    elh[:, 384:640] = dot3(r0, fx, True)
    eh[k] = elh[...]
    gh_start, gh_recv, gh_send = gather(3, elh, eh)
    gh_start()
    sends += [h_send, c_send, c2_send, g0_send, gh_send]

    c_recv()
    CG = cg[0:8].reshape(128, 128)
    CG2 = [None]
    ri, ci = iota((128, 128), 0), iota((128, 128), 1)
    same = (ri >> 1) == (ci >> 1)
    odd = (ci & 1) == 1
    eye = jnp.where(ri == ci, 1.0, 0.0).astype(f32)

    def col(c):
        src = CG2[0] if 2 <= c < 8 else CG
        return jnp.broadcast_to(src[:, c : c + 1], (128, 128))

    def corner(n):
        return jnp.where(same, jnp.where(odd, col(2 * n + 1), col(2 * n)), 0.0)

    lrow = (ri >> 1) & 7
    inva = jnp.zeros((128, 128), f32)
    for l in range(5):
        inva = jnp.where(lrow == l, 1.0 / a[l], inva)
    face = col(8)
    face_up = jnp.concatenate([face[16:], jnp.zeros((16, 128), f32)], 0)
    K = inva * (
        jnp.where(((ri & 1) == 0) & (ci == ri - 15), face, 0.0)
        + jnp.where(((ri & 1) == 1) & (ci == ri + 15), face_up, 0.0)
    )
    R = corner(0)
    blk = (ri >> 4) + (ri & 1)
    for st in (1, 2, 4):
        link = jnp.where((blk & (2 * st - 1)) == st, K, 0.0)
        d = R * eye
        drow = jnp.sum(d, 1, keepdims=True)
        dcol = jnp.sum(d, 0, keepdims=True)
        off = link / (1.0 - link * link * drow * dcol)
        diag = jnp.sum(off * link * dcol, 1, keepdims=True)
        R = R + hdot(hdot(R, off + eye * diag), R)
    W = eye + hdot(R, K)
    c2_recv()
    CG2[0] = cg2[...].reshape(128, 128)
    B2, B3, B4 = dot3(corner(1), K), dot3(corner(2), K), dot3(corner(3), K)
    V1 = dot3(W, dot3(B2, W))
    V2 = dot3(W, dot3(B3, W) + dot3(B2, V1))
    V3 = dot3(W, dot3(B4, W) + dot3(B3, V1) + dot3(B2, V2))
    VS = [W, V1, V2, V3]

    def lm_of(p):
        l = jnp.where(p < 12, (p >> 2) + 1, jnp.where(p < 14, 0, 4))
        m = jnp.where(p < 12, (p & 3) + 1, (p & 1) + 1)
        return l, m

    def funct(level):
        width = 64 if level == 0 else 256
        rr, rc = iota((128, 128), 0), iota((128, 128), 1)
        p, side = rr & 15, rr >> 4
        if level == 0:
            l, m = jnp.zeros_like(p), p - 11
            live = (rr < 32) & (p >= 12)
        else:
            l, m = lm_of(p)
            live = rr < 32
        target = jnp.where(side == 0, (k - 1) * 16 + l * 2 + 1, (k + 1) * 16 + l * 2)
        pick_rows = jnp.where(live & (rc == target), 1.0, 0.0).astype(f32)
        er, ec = iota((128, width), 0), iota((128, width), 1)
        if level == 0:
            jc, lc, mc, endc = ec >> 3, jnp.zeros_like(ec), ((ec >> 1) & 3) + 1, ec & 1
        else:
            jc, endc = ec >> 5, ec & 1
            lc, mc = lm_of((ec >> 1) & 15)
        expand = jnp.where(er == jc * 16 + lc * 2 + endc, 1.0, 0.0).astype(f32)
        wr = iota((128, width), 0)
        mrow = ((wr & 15) - 11) if level == 0 else lm_of(wr & 15)[1]
        out = jnp.zeros((128, width), f32)
        for n in range(4):
            x = dot3(dot3(pick_rows, VS[n]), expand)
            out = out + jnp.where(mrow - mc == n, x, 0.0)
        return out

    L0 = funct(0)

    side_in, side_out = ri >> 4, ci >> 4
    pi, po = ri & 15, ci & 15
    fl = (ri < 32) & (ci < 32) & (side_in == side_out)
    li, mi = lm_of(pi)
    lo, mo = lm_of(po)
    aout = jnp.zeros((128, 128), f32)
    for l in range(5):
        aout = jnp.where(lo == l, a[l], aout)
    cm = jnp.broadcast_to(zf_ref[0:1, 0:1], (1, 128))
    cp = jnp.broadcast_to(cg[k + 1, 0:1, 8:9], (1, 128))

    def matrices():
        for l in range(5):
            gt = g_ref[l].T
            p1 = pid(l, 1)
            ut = jnp.where(ri == p1, jnp.broadcast_to(cm * gt[0:1], (128, 128)), 0.0)
            ut = jnp.where(ri == 16 + p1, jnp.broadcast_to(cp * gt[127:128], (128, 128)), ut)
            if l == 0:
                q = jnp.where(fl & (pi >= 13) & (pi == po + 1), 1.0, 0.0)
            else:
                den = jnp.where(lo == l, 1.0, a[l] - aout)
                amp = a[l] / den
                nb = -aout / den
                p2 = nb * nb
                p3 = p2 * nb
                dm = mo - mi
                pw = jnp.where(dm == 0, 1.0, jnp.where(dm == 1, nb, jnp.where(dm == 2, p2, p3)))
                pm = jnp.where(mo == 1, nb, jnp.where(mo == 2, p2, jnp.where(mo == 3, p3, p2 * p2)))
                q = jnp.where((li == lo) & (dm >= 0), amp * pw, 0.0)
                q = q + jnp.where((li == l) & (mi == 1), pm, 0.0)
                q = jnp.where(lo == l, jnp.where((li == l) & (mi == mo + 1), 1.0, 0.0), q)
                q = jnp.where(fl, q, 0.0)
            for r, v in ((0, a[l] * gt), (128, ut)):
                vh, vl = split(v)
                th[l, r : r + 128, 0:128] = vh
                tl[l, r : r + 128, 0:128] = vl
            qh, ql = split(q.astype(f32))
            zero = jnp.zeros((128, 128), bf16)
            th[l, 0:128, 128:256] = zero
            tl[l, 0:128, 128:256] = zero
            th[l, 128:256, 128:256] = qh
            tl[l, 128:256, 128:256] = ql

    gt = a[0] * g_ref[0].T
    gh, gl = split(gt)
    ra[0:128, 0:128] = gh
    ra[128:256, 0:128] = gh
    ra[0:128, 128:256] = gl
    ra[128:256, 128:256] = jnp.zeros((128, 128), bf16)
    gt = g_ref[0].T
    for i in range(4):
        row = ri & 31
        u = jnp.where(row == 12 + i, jnp.broadcast_to(cm * gt[0:1], (128, 128)), 0.0)
        u = jnp.where(row == 28 + i, jnp.broadcast_to(cp * gt[127:128], (128, 128)), u)
        uh, ul = split(u)
        u = jnp.where(ri < 64, uh.astype(f32), jnp.where(ri < 96, ul.astype(f32), 0.0))
        ub[:, 128 * i : 128 * i + 128] = u.astype(bf16)

    def apply(l, src, dst, step, n, scale=None):
        y = src.shape[2]

        def body(i, c):
            x = pl.ds(i * step, step)
            v = jnp.concatenate(
                [src[0, x].reshape(step * y, 128), src[1, x].reshape(step * y, 128)], 1
            )
            vh, vl = split(v)
            t = mm(vh, th[l]) + (mm(vh, tl[l]) + mm(vl, th[l]))
            if scale is not None:
                t = scale * t
            dst[0, x] = t[:, 0:128].reshape(step, y, 128)
            dst[1, x] = t[:, 128:256].reshape(step, y, 128)
            return c

        lax.fori_loop(0, n, body, 0)

    def solve_block(src, dst):
        n, y = src.shape[1], src.shape[2]
        v = jnp.concatenate([src[0].reshape(n * y, 128), src[1].reshape(n * y, 128)], 1)
        vh, vl = split(v)
        t = mm(vh, jnp.concatenate([th[0, :, 0:128], tl[0, :, 0:128]], 1))
        t = t[:, 0:128] + (t[:, 128:256] + mm(vl, th[0, :, 0:128]))
        dst[0] = t.reshape(n, y, 128)

    def stencil(l, src, dst, grow, post, halves=(0, 1)):
        ox, oy, n, y = OX[l], OY[l], LX[l], SY[l]
        gy0 = iota((y, 128), 0) + (iy * n - oy)
        ym = jnp.where((gy0 >= 0) & (gy0 < ngy * n), 0.25, 0.0).astype(f32)

        def body(x, c):
            gx0 = ix * n + x - ox
            s = jnp.where((gx0 >= 0) & (gx0 < ngx * n), 1.0, 0.0).astype(f32)
            m4 = ym * s
            for h in halves:
                v = src[h, x]
                t = (src[h, x - 1] + src[h, x + 1]) + (
                    pltpu.roll(v, 1, 0) + pltpu.roll(v, y - 1, 0)
                )
                dst(h, x, post(h, x, m4 * t))
            return c

        lax.fori_loop(ox - grow, ox + n + grow, body, 0)

    def into(ref):
        def put(h, x, v):
            ref[h, x] = v
        return put

    def solve(l, src, dst, matrix=None, scale=None):
        step, n = SX[l], 1
        apply(l if matrix is None else matrix, src, dst, step, n, scale)

    def residual(l, halves=(0, 1)):
        s, ta, tb = S[l], at("TA", l), at("TB", l)
        aa, bb = at("AA", l), at("BB", l)
        solve(l, s, ta)
        solve(l, ta, tb)
        stencil(l, tb, into(bb), 1, lambda h, x, v: 0.32 * ta[h, x] + 0.64 * v, halves)
        stencil(l, bb, into(aa), 0, lambda h, x, v: 0.04 * s[h, x] + v, halves)

    def smoothed(l):
        w = 0
        s, ta, tb, tc = S[l], at("TA", l), at("TB", l), at("TC", l)
        bb, cc, ma = at("BB", l), at("CC", l), at("MA", l)
        solve(l, tb, tc)
        stencil(l, tc, into(bb), 2 + w, lambda h, x, v: 0.8192 * tb[h, x] + 0.4096 * v)
        stencil(l, bb, into(cc), 1 + w, lambda h, x, v: 0.9728 * ta[h, x] + v)
        stencil(l, cc, into(ma), w, lambda h, x, v: 0.9984 * s[h, x] + v)

    def restrict(l, put, halves=(0, 1)):
        ox, oy, n = OX[l], OY[l], LX[l] // 2
        aa = at("AA", l)

        def body(i, c):
            x = ox + 2 * i
            for h in halves:
                even, off = pl.ds(oy, n, 2), pl.ds(oy + 1, n, 2)
                v = (aa[h, x, even, :] + aa[h, x, off, :]) + (
                    aa[h, x + 1, even, :] + aa[h, x + 1, off, :]
                )
                put(h, i, 0.25 * v)
            return c

        lax.fori_loop(0, n, body, 0)

    def prolong(l, fields, outs, halves):
        c = l + 1
        w = 1 if l == 0 else 0
        n, ox, oc, y = LX[c], OX[l], OX[c], SY[c]
        ys, cnt = [(0, 24), (2, 12), (2, 8), (2, 8)][l]
        gyc = iota((cnt, 128), 0) + (iy * n + ys - OY[c])
        ym = jnp.where((gyc >= 0) & (gyc < ngy * n), 1.0, 0.0).astype(f32)

        def body(j, carry):
            j = j - (1 + w)
            gx = ix * n + j
            s = jnp.where((gx >= 0) & (gx < ngx * n), 1.0, 0.0).astype(f32)
            ms = ym * s
            for h in halves:
                lower, here, upper = (fields(h, oc + j + i) for i in (-1, 0, 1))
                for (o, oh), lo_, he, up_ in zip(outs, lower, here, upper):
                    oh = h if oh is None else oh
                    for i, far in enumerate((lo_, up_)):
                        v = 0.75 * he + 0.25 * far
                        ev = (0.75 * v + 0.25 * pltpu.roll(v, 1, 0))[ys : ys + cnt]
                        od = (0.75 * v + 0.25 * pltpu.roll(v, y - 1, 0))[ys : ys + cnt]
                        o[oh, ox + 2 * j + i, pl.ds(0, cnt, 2), :] = ms * ev
                        o[oh, ox + 2 * j + i, pl.ds(1, cnt, 2), :] = ms * od
            return carry

        lax.fori_loop(0, n + 2 + 2 * w, body, 0)

    def correct(l, store):
        c = l + 1
        m, u, g2 = M[c], at("U", c), at("V", c)
        kap = a[l] / a[c]
        solve(c, m, u, c, kap)
        solve(c, u, g2, l, 0.64)
        q = 0.04 * (1.0 - a[c] / a[l])
        outs = [at("P0", l), at("P1", l), at("P2", l)]

        def fields(h, x):
            uv = u[h, x]
            return (0.04 * m[h, x] + q * uv, 0.32 * uv, g2[h, x])

        prolong(l, fields, [(o, None) for o in outs], (0, 1))
        cc, ma = at("CC", l), at("MA", l)
        stencil(l, outs[2], into(cc), 1, lambda h, x, v: outs[1][h, x] + v)
        stencil(l, cc, store, 0, lambda h, x, v: (ma[h, x] + outs[0][h, x]) + v)

    def parts(et):
        phi = dot3(L0, et).T
        h, lo_ = split(phi)
        h, lo_ = h.astype(f32), lo_.astype(f32)
        return h + pltpu.roll(lo_, 32, 1) + pltpu.roll(h, 64, 1)

    def powers(first, src, d1, d2):
        for i in range(5):
            x = slice(8 * i, 8 * i + 8)
            w = S0[1, x].reshape(384, 128).astype(bf16)
            c = mm(w, ub[:, 128 * first : 128 * first + 256])
            vh, vl = split(src[0, x].reshape(384, 128))
            t = mm(jnp.concatenate([vh, vl], 1), ra[...])
            t = (t[:, 0:128] + t[:, 128:256]) + c[:, 0:128]
            d1[0, x] = t.reshape(8, 48, 128)
            vh, vl = split(t)
            t = mm(jnp.concatenate([vh, vl], 1), ra[...])
            t = (t[:, 0:128] + t[:, 128:256]) + c[:, 128:256]
            d2[0, x] = t.reshape(8, 48, 128)

    g0_recv()
    for i in range(4):
        w = parts(e0[:, :, 256 * i : 256 * i + 256].reshape(64, 256))
        S0[1, 4 + 8 * i : 12 + 8 * i, 8:40, :] = w.reshape(8, 32, 128)
    gh_recv()
    w = parts(eh[:, :, 0:384].reshape(64, 384))
    S0[1, 0:4] = w[0:192].reshape(4, 48, 128)
    S0[1, 36:40] = w[192:384].reshape(4, 48, 128)
    w = parts(eh[:, :, 384:640].reshape(64, 256)).reshape(32, 8, 128)
    S0[1, 4:36, 4:8, :] = w[:, 0:4]
    S0[1, 4:36, 40:44, :] = w[:, 4:8]

    t1, t2, t3, t4 = at("TA", 0), at("TB", 0), at("TC", 0), at("P0", 0)
    aa0, bb0, cc0, ma0 = at("AA", 0), at("BB", 0), at("CC", 0), at("MA", 0)
    powers(0, S0, t1, t2)
    stencil(0, t2, into(bb0), 1, lambda h, x, v: 0.32 * t1[h, x] + 0.64 * v, (0,))
    stencil(0, bb0, into(aa0), 0, lambda h, x, v: 0.04 * S0[h, x] + v, (0,))

    def put1(h, i, v):
        S1[h, 3 + i, 4:20, :] = v
    restrict(0, put1, (0,))
    el1[...] = dot3(re1[...], S1[0, 3:19, 4:20, :].reshape(256, 128), True)
    e1[k] = el1[...]
    g1_start, g1_recv, g1_send = gather(2, el1, e1)
    g1_start()
    x1_start, x1_finish, x1_send = packed(1, 1, "g1", S1, True, False)
    x1_start()

    L1 = funct(1)
    matrices()
    powers(2, t2, t3, t4)

    def both0(h, x, v):
        bb0[0, x] = 0.8192 * t3[0, x] + 0.4096 * v
        bb0[1, x] = 0.4096 * (t3[0, x] + v)

    g1_recv()
    phi = dot3(L1, e1[...].reshape(256, 256))
    S1[1, 3:19, 4:20, :] = phi.T.reshape(16, 16, 128)
    y1_start, y1_finish, y1_send = packed(2, 1, "f1", S1, False, True)
    y1_start()
    stencil(0, t4, both0, 3, lambda h, x, v: v, (0,))
    stencil(0, bb0, into(cc0), 2, lambda h, x, v: (0.1536 if h else 0.9728) * t2[0, x] + v)
    x1_finish()
    y1_finish()
    residual(1)

    def put2(h, i, v):
        S2[h, 3 + i, 4:12, :] = v
    restrict(1, put2)
    x2_start, x2_finish, x2_send = packed(3, 2, "s2", S2)
    x2_start()
    smoothed(1)
    stencil(0, cc0, into(aa0), 1, lambda h, x, v: (0.0256 if h else 0.9984) * t1[0, x] + v)

    x2_finish()
    residual(2)

    def put3(h, i, v):
        S3[h, 4 + i, 4:8, :] = v
    restrict(2, put3)
    x3_start, x3_finish, x3_send = packed_block(4, 3, "s3", S3)
    x3_start()
    smoothed(2)
    stencil(0, aa0, into(ma0), 0, lambda h, x, v: 0.0016 * S0[0, x] + v, (1,))

    x3_finish()
    residual(3)

    def put4(h, i, v):
        S4[h, 4 + i, 4:6, :] = v
    restrict(3, put4)
    x4_start, x4_finish, x4_send = packed_block(5, 4, "s4", S4, FAR)
    x4_start()
    smoothed(3)

    x4_finish()
    ta4 = at("TA", 4)
    solve(4, S4, ta4)

    stencil(4, ta4, into(M4), 2, lambda h, x, v: 0.96 * S4[h, x] + 0.64 * v)

    def putm3(h, x, v):
        M3[h, x, 4:8, :] = v[4:8]
    correct(3, putm3)
    z3_start, z3_finish, z3_send = packed_block(7, 3, "m3", M3)
    z3_start()
    z3_finish()

    def putm2(h, x, v):
        M2[h, x, 4:12, :] = v[4:12]
    correct(2, putm2)
    z2_start, z2_finish, z2_send = packed(8, 2, "m2", M2)
    z2_start()
    z2_finish()

    def putm1(h, x, v):
        M1[h, x, 4:20, :] = v[4:20]
    correct(1, putm1)
    z1_start, z1_finish, z1_send = packed(9, 1, "m1", M1)
    z1_start()
    z1_finish()

    u, g2 = at("U", 1), at("V", 1)
    kap = a[0] / a[1]
    solve(1, M1, u, 1, kap)
    solve(1, u, g2, 0, 0.64)
    solve_block(M1, HM)
    solve_block(g2, H2)
    q = 0.04 * (1.0 - a[1] / a[0])

    def fields0(h, x):
        uv, gv = u[0, x], g2[0, x]
        h0 = 0.04 * HM[0, x] + (q / 0.64) * gv
        return (0.04 * M1[0, x] + q * uv, h0 - 0.32 * uv, 0.5 * gv, H2[0, x], h0)

    P0, P1, P2 = at("P0", 0), at("P1", 0), at("P2", 0)
    prolong(0, fields0, [(P0, 0), (P0, 1), (P1, 0), (P1, 1), (P2, 0)], (0,))

    def pair(h, x, v):
        bb0[0, x] = v - P1[0, x]
        bb0[1, x] = v + P1[0, x]
    stencil(0, P1, pair, 2, lambda h, x, v: v, (1,))
    stencil(0, bb0, into(cc0), 1, lambda h, x, v: P0[1, x] + v, (0,))
    inv0 = 1.0 / a[0]

    def put_sol(h, x, v):
        sol_ref[x - 4] = v[8:40]

    def put_res(h, x, v):
        res_ref[x - 4] = v[8:40]
    stencil(0, bb0, put_sol, 0, lambda h, x, v: inv0 * ((aa0[0, x] + P2[0, x]) + v), (1,))
    stencil(0, cc0, put_res, 0, lambda h, x, v: (ma0[1, x] - P0[0, x]) + v, (0,))

    for wait in sends + [
        x1_send, g1_send, y1_send, x2_send, x3_send, x4_send, z3_send, z2_send, z1_send
    ]:
        wait()


def body(sizes, right_side, z_faces, xy_coupling, block_inverse):
    n = right_side.shape
    vmem = pl.BlockSpec(memory_space=pltpu.VMEM)
    hbm = pl.BlockSpec(memory_space=pl.ANY)
    scratch = [pltpu.VMEM(s, f32) for s in scratch_shapes().values()]
    scratch += [pltpu.VMEM((5, 128, 128), f32)]
    scratch += [pltpu.VMEM((5, 256, 256), bf16), pltpu.VMEM((5, 256, 256), bf16)]
    scratch += [pltpu.VMEM((256, 256), bf16), pltpu.VMEM((128, 512), bf16)]
    scratch += [pltpu.SemaphoreType.DMA((10, 20)), pltpu.SemaphoreType.DMA((10, 20))]
    scratch += [pltpu.SemaphoreType.DMA((5, 8)), pltpu.SemaphoreType.DMA((5, 8))]
    scratch += [pltpu.SemaphoreType.DMA((2,))]
    return pl.pallas_call(
        lambda *r: kernel(sizes, *r),
        out_shape=(pltpu.VMEM(n, f32), pltpu.VMEM(n, f32)),
        in_specs=[hbm, vmem, hbm, pl.BlockSpec(memory_space=pltpu.SMEM)],
        out_specs=(vmem, vmem),
        scratch_shapes=scratch,
        compiler_params=pltpu.CompilerParams(
            collective_id=0, has_side_effects=True, vmem_limit_bytes=60 * 2**20
        ),
        name="vcycle",
    )(right_side, z_faces.reshape(1, -1), block_inverse, xy_coupling)


def solution(mesh):
    sizes = tuple(mesh.shape[n] for n in ("gx", "gy", "gz"))
    return jax.shard_map(
        lambda *args: body(sizes, *args),
        mesh=mesh,
        in_specs=(P("gx", "gy", "gz"), P("gz"), P(), P(None, "gz", None)),
        out_specs=(P("gx", "gy", "gz"), P("gx", "gy", "gz")),
        check_vma=False,
    )
```

```python
import jax
import jax.numpy as jnp
from jax import lax
from jax.experimental import pallas as pl
from jax.experimental.pallas import tpu as pltpu
from jax.sharding import PartitionSpec as P

f32 = jnp.float32
bf16 = jnp.bfloat16
HI = lax.Precision.HIGHEST
MESH = pl.DeviceIdType.MESH
FAR = [(dx, dy) for dx in (-2, -1, 0, 1, 2) for dy in (-2, -1, 0, 1, 2) if 0 < abs(dx) + abs(dy) < 4]
DIRS = [(dx, dy) for dx in (-1, 0, 1) for dy in (-1, 0, 1) if (dx, dy) != (0, 0)]

LX = [32, 16, 8, 4, 2]
OX = [4, 3, 3, 4, 4]
OY = [8, 4, 4, 4, 4]
SX = [40, 22, 14, 12, 10]
SY = [48, 24, 16, 16, 16]


def pair_of(p):
    if p < 12:
        return p // 4 + 1, p % 4 + 1
    return (0 if p < 14 else 4), p % 2 + 1


def pid(l, m):
    if l == 0:
        return 11 + m
    if l == 4:
        return 13 + m
    return (l - 1) * 4 + m - 1


def split(x):
    h = x.astype(bf16)
    return h, (x - h.astype(f32)).astype(bf16)


def mm(a, b, trans_b=False):
    dims = (((1,), (1 if trans_b else 0,)), ((), ()))
    return lax.dot_general(a, b, dims, preferred_element_type=f32)


def dot3(a, b, trans_b=False):
    ah, al = split(a)
    bh, bl = split(b)
    return mm(ah, bh, trans_b) + (mm(ah, bl, trans_b) + mm(al, bh, trans_b))


def hdot(a, b):
    return jnp.dot(a, b, precision=HI, preferred_element_type=f32)


def iota(shape, dim):
    return lax.broadcasted_iota(jnp.int32, shape, dim)


MESSAGES = {"f0": 16, "g1": 8, "f1": 2, "s2": 5, "s3": 3, "s4": 1, "m3": 3, "m2": 5, "m1": 10}


def scratch_shapes():
    out = {}
    for l in range(5):
        out[f"S{l}"] = (2, SX[l], SY[l], 128)
        for t in ("TA", "TB", "TC", "AA", "BB", "CC", "MA", "P0", "P1", "P2"):
            out[f"{t}{l}"] = (2, SX[l], SY[l], 128)
        if l:
            for t in ("M", "U", "V"):
                out[f"{t}{l}"] = (2, SX[l], SY[l], 128)
    out["HM"] = out["H2"] = (2, SX[1], SY[1], 128)
    for name, tiles in MESSAGES.items():
        out["out_" + name] = out["in_" + name] = (len(FAR) if name == "s4" else 8, tiles, 8, 128)
    out["rows"] = (4, 16, 128)
    out["re0"] = (8, 128)
    out["re1"] = (32, 128)
    out["cg"] = (9, 16, 128)
    out["cgl"] = out["cgl2"] = (16, 128)
    out["cg2"] = (8, 16, 128)
    out["e0"] = (8, 8, 1024)
    out["eh"] = (8, 8, 640)
    out["e1"] = (8, 32, 256)
    out["el0"] = (8, 1024)
    out["elh"] = (8, 640)
    out["el1"] = (32, 256)
    return out


def kernel(sizes, f_ref, zf_in, ginv_ref, e_in, sol_ref, res_ref, *refs):
    names = list(scratch_shapes())
    r_ = dict(zip(names, refs))
    g_ref, th, tl, ra, ub, hs, hr, gs, gr, ls, zf_ref, e_ref = refs[len(names):]
    S0, S1, S2, S3, S4 = [r_[f"S{l}"] for l in range(5)]
    M1, M2, M3, M4 = [r_[f"M{l}"] for l in range(1, 5)]
    rows, re0, re1, cg, cgl = r_["rows"], r_["re0"], r_["re1"], r_["cg"], r_["cgl"]
    e0, e1, el0, el1 = r_["e0"], r_["e1"], r_["el0"], r_["el1"]
    eh, elh, HM, H2 = r_["eh"], r_["elh"], r_["HM"], r_["H2"]
    cg2, cgl2 = r_["cg2"], r_["cgl2"]

    ngx, ngy, ngz = sizes
    ix, iy, k = lax.axis_index("gx"), lax.axis_index("gy"), lax.axis_index("gz")
    S = [S0, S1, S2, S3, S4]
    M = [None, M1, M2, M3, M4]

    def at(name, l):
        return r_[f"{name}{l}"]


    def peer(o):
        return jnp.where(k + o >= ngz, k + o - ngz, k + o)

    def exists(dx, dy):
        x, y = ix + dx, iy + dy
        return (x >= 0) & (x < ngx) & (y >= 0) & (y < ngy)

    def clear(ref):
        def step(i, c):
            ref[i] = jnp.zeros(ref.shape[1:], f32)
            return c
        lax.fori_loop(0, ref.shape[0], step, 0)

    def clear2(ref):
        def step(i, c):
            for h in range(2):
                ref[h, i] = jnp.zeros(ref.shape[2:], f32)
            return c
        lax.fori_loop(0, ref.shape[1], step, 0)

    load_f = pltpu.make_async_copy(f_ref, S0.at[0, 4:36, 8:40, :], ls.at[0])
    load_g = pltpu.make_async_copy(ginv_ref, g_ref, ls.at[1])
    load_z = pltpu.make_async_copy(zf_in, zf_ref, ls.at[2])
    load_e = pltpu.make_async_copy(e_in, e_ref, ls.at[3])
    for load in (load_e, load_z, load_g, load_f):
        load.start()

    barrier = pltpu.get_barrier_semaphore()
    count = jnp.int32(ngz - 1)
    for dx, dy in FAR:
        ok = exists(dx, dy)

        @pl.when(ok)
        def _():
            pl.semaphore_signal(
                barrier, inc=1, device_id=(ix + dx, iy + dy, k), device_id_type=MESH
            )

        count = count + jnp.where(ok, 1, 0)
    for o in range(1, ngz):
        pl.semaphore_signal(
            barrier, inc=1, device_id=(ix, iy, peer(o)), device_id_type=MESH
        )

    for d, (dx, dy) in enumerate(DIRS):
        @pl.when(jnp.logical_not(exists(-dx, -dy)))
        def _():
            for name in ("f0", "g1", "f1"):
                r = r_["in_" + name]
                for t in range(MESSAGES[name]):
                    r[d, t] = jnp.zeros((8, 128), f32)
            if dy == 0:
                for i in range(4):
                    S0[0, (0 if dx == 1 else 36) + i, 8:40, :] = jnp.zeros((32, 128), f32)

    def sides(i, c):
        S0[0, i, 0:8, :] = jnp.zeros((8, 128), f32)
        S0[0, i, 40:48, :] = jnp.zeros((8, 128), f32)
        return c
    lax.fori_loop(0, 40, sides, 0)
    clear(rows)
    if ngz < 8:
        for r in (e0, eh, e1, cg2):
            clear(r)
    cg[8] = jnp.zeros((16, 128), f32)

    def exchange(phase, pick, dirs=DIRS):
        def copy(d, dx, dy):
            src, dst = pick(dx, dy)
            return pltpu.make_async_remote_copy(
                src_ref=src, dst_ref=dst, send_sem=hs.at[phase, d], recv_sem=hr.at[phase, d],
                device_id=(ix + dx, iy + dy, k), device_id_type=MESH,
            )

        def start():
            for d, (dx, dy) in enumerate(dirs):
                @pl.when(exists(dx, dy))
                def _():
                    copy(d, dx, dy).start()

        def wait_recv():
            for d, (dx, dy) in enumerate(dirs):
                @pl.when(exists(-dx, -dy))
                def _():
                    copy(d, dx, dy).wait_recv()

        def wait_send():
            for d, (dx, dy) in enumerate(dirs):
                @pl.when(exists(dx, dy))
                def _():
                    copy(d, dx, dy).wait_send()

        return start, wait_recv, wait_send

    def span(d, off, n, h):
        if d == 0:
            return pl.ds(off, n), pl.ds(off, n)
        if d == 1:
            return pl.ds(off + n - h, h), pl.ds(off - h, h)
        return pl.ds(off, h), pl.ds(off + n, h)

    def lanes_of(planes):
        out = planes[0]
        for i, v in enumerate(planes[1:]):
            out = out + pltpu.roll(v, 32 * (i + 1), 1)
        return out

    low_lanes = {r: iota((r, 128), 1) < 32 for r in (8,)}

    def lanes_back(tile, i):
        v = tile if i == 0 else pltpu.roll(tile, 128 - 32 * i, 1)
        return jnp.where(low_lanes[8], v, 0.0)

    def tiles_of(l, dx, dy, wf, wp):
        n = LX[l]
        if dx == 0:
            return (n // 2 if wf else 0) + ((n + 7) // 8 if wp else 0)
        if dy == 0:
            return (3 * n // 8 if wf else 0) + (n // 8 if wp else 0)
        return 2 if wf else 1

    def packed(phase, l, name, buf, wf=True, wp=True):
        n, ox, oy = LX[l], OX[l], OY[l]
        ob, ib = r_["out_" + name], r_["in_" + name]

        def pick(dx, dy):
            d, t = DIRS.index((dx, dy)), tiles_of(l, dx, dy, wf, wp)
            return ob.at[d, 0:t], ib.at[d, 0:t]

        start0, wait_recv, wait_send = exchange(phase, pick)

        def start():
            for d, (dx, dy) in enumerate(DIRS):
                xs = ox + n - 3 if dx == 1 else ox
                ys = oy + n - 4 if dy == 1 else oy
                yt = ys // 8 * 8
                part = slice(ys - yt, ys - yt + 4)
                if dx == 0:
                    base = n // 2 if wf else 0
                    if wf:
                        for t in range(n // 2):
                            ob[d, t, 0:4, :] = buf[0, ox + t, ys : ys + 4, :]
                            ob[d, t, 4:8, :] = buf[0, ox + t + n // 2, ys : ys + 4, :]
                    if wp:
                        for b in range(n // 4):
                            v = lanes_of([buf[1, ox + 4 * b + i, yt : yt + 8, :] for i in range(4)])
                            r = 4 * (b % 2)
                            ob[d, base + b // 2, r : r + 4, :] = v[part]
                elif dy == 0:
                    m = n // 8
                    base = 3 * m if wf else 0
                    for r in range(m):
                        y = slice(oy + 8 * r, oy + 8 * r + 8)
                        if wf:
                            for i in range(3):
                                ob[d, i * m + r] = buf[0, xs + i, y, :]
                        if wp:
                            ob[d, base + r] = lanes_of([buf[1, xs + i, y, :] for i in range(3)])
                else:
                    if wf:
                        ob[d, 0, 0:4, :] = buf[0, xs, ys : ys + 4, :]
                        ob[d, 0, 4:8, :] = buf[0, xs + 1, ys : ys + 4, :]
                        ob[d, 1, 0:4, :] = buf[0, xs + 2, ys : ys + 4, :]
                    if wp:
                        v = lanes_of([buf[1, xs + i, yt : yt + 8, :] for i in range(3)])
                        ob[d, 1 if wf else 0, 4:8, :] = v[part]
            start0()

        def finish():
            wait_recv()
            for d, (dx, dy) in enumerate(DIRS):
                xd = ox - 3 if dx == 1 else ox + n
                yd = oy - 4 if dy == 1 else oy + n
                if dx == 0:
                    base = n // 2 if wf else 0
                    if wf:
                        for t in range(n // 2):
                            buf[0, ox + t, yd : yd + 4, :] = ib[d, t, 0:4, :]
                            buf[0, ox + t + n // 2, yd : yd + 4, :] = ib[d, t, 4:8, :]
                    if wp:
                        for b in range(n // 4):
                            tile, r = ib[d, base + b // 2], 4 * (b % 2)
                            for i in range(4):
                                v = lanes_back(tile, i)
                                buf[1, ox + 4 * b + i, yd : yd + 4, :] = v[r : r + 4]
                elif dy == 0:
                    m = n // 8
                    base = 3 * m if wf else 0
                    for r in range(m):
                        y = slice(oy + 8 * r, oy + 8 * r + 8)
                        for i in range(3):
                            if wf:
                                buf[0, xd + i, y, :] = ib[d, i * m + r]
                            if wp:
                                buf[1, xd + i, y, :] = lanes_back(ib[d, base + r], i)
                else:
                    if wf:
                        buf[0, xd, yd : yd + 4, :] = ib[d, 0, 0:4, :]
                        buf[0, xd + 1, yd : yd + 4, :] = ib[d, 0, 4:8, :]
                        buf[0, xd + 2, yd : yd + 4, :] = ib[d, 1, 0:4, :]
                    if wp:
                        tile = ib[d, 1 if wf else 0]
                        for i in range(3):
                            buf[1, xd + i, yd : yd + 4, :] = lanes_back(tile, i)[4:8]

        return start, finish, wait_send

    def packed_block(phase, l, name, buf, dirs=DIRS):
        n = LX[l]
        ob, ib = r_["out_" + name], r_["in_" + name]

        def pick(dx, dy):
            return ob.at[0], ib.at[dirs.index((dx, dy))]

        start0, wait_recv, wait_send = exchange(phase, pick, dirs)

        def start():
            phi = lanes_of([buf[1, 4 + i, 0:8, :] for i in range(n)])
            if n == 4:
                for i in range(4):
                    r = 4 * (i // 2)
                    ob[0, i % 2, r : r + 4, :] = buf[0, 4 + i, 4:8, :]
                ob[0, 2] = phi
            else:
                ob[0, 0, 0:2, :] = buf[0, 4, 4:6, :]
                ob[0, 0, 2:4, :] = buf[0, 5, 4:6, :]
                ob[0, 0, 4:8, :] = phi[4:8]
            start0()

        def finish():
            wait_recv()
            for d, (dx, dy) in enumerate(dirs):
                xd, yd = 4 - n * dx, 4 - n * dy
                tile = ib[d, 2 if n == 4 else 0]
                for i in range(n):
                    v = lanes_back(tile, i)
                    buf[1, xd + i, yd : yd + n, :] = v[4 : 4 + n]
                    if n == 4:
                        r = 4 * (i // 2)
                        buf[0, xd + i, yd : yd + 4, :] = ib[d, i % 2, r : r + 4, :]
                    else:
                        buf[0, xd + i, yd : yd + 2, :] = tile[2 * i : 2 * i + 2]

        return start, finish, wait_send

    def gather(phase, src, buf):
        def copy(o):
            return pltpu.make_async_remote_copy(
                src_ref=src, dst_ref=buf.at[k], send_sem=gs.at[phase, o],
                recv_sem=gr.at[phase, o], device_id=(ix, iy, peer(o)),
                device_id_type=MESH,
            )

        def start():
            for o in range(1, ngz):
                copy(o).start()

        def wait_recv():
            for o in range(1, ngz):
                copy(o).wait_recv()

        def wait_send():
            for o in range(1, ngz):
                copy(o).wait_send()

        return start, wait_recv, wait_send

    sends = []
    ob0, ib0 = r_["out_f0"], r_["in_f0"]

    def pick0(dx, dy):
        d = DIRS.index((dx, dy))
        if dy == 0:
            sx, tx = span(dx, 4, 32, 4)
            return S0.at[0, sx, 8:40, :], S0.at[0, tx, 8:40, :]
        t = 16 if dx == 0 else 2
        return ob0.at[d, 0:t], ib0.at[d, 0:t]

    def ends0(dx):
        return 32 if dx == 1 else 4

    load_e.wait()
    a = [4.0 * e_ref[l] for l in range(5)]
    lane16 = iota((16, 128), 1)

    def corner_tile(first, last, tile):
        for n in range(first, last):
            rn = rows[n]
            tile = jnp.where(lane16 == 2 * n, jnp.broadcast_to(rn[:, 0:1], (16, 128)), tile)
            tile = jnp.where(lane16 == 2 * n + 1, jnp.broadcast_to(rn[:, 127:128], (16, 128)), tile)
        return tile

    load_z.wait()
    load_g.wait()
    for l in range(5):
        rows[0, 2 * l : 2 * l + 1, :] = a[l] * g_ref[l, 0:1, :]
        rows[0, 2 * l + 1 : 2 * l + 2, :] = a[l] * g_ref[l, 127:128, :]
    tile = corner_tile(
        0, 1, jnp.where(lane16 == 8, jnp.broadcast_to(zf_ref[0:1, 0:1], (16, 128)), 0.0)
    )
    cgl[...] = tile
    cg[k] = tile
    load_f.wait()
    for d, (dx, dy) in enumerate(DIRS):
        ys = 36 if dy == 1 else 8
        if dy != 0 and dx == 0:
            for t in range(16):
                ob0[d, t, 0:4, :] = S0[0, 4 + t, ys : ys + 4, :]
                ob0[d, t, 4:8, :] = S0[0, 20 + t, ys : ys + 4, :]
        elif dy != 0:
            for t in range(4):
                r = 4 * (t % 2)
                ob0[d, t // 2, r : r + 4, :] = S0[0, ends0(dx) + t, ys : ys + 4, :]

    pl.semaphore_wait(barrier, count)
    h_start, h_recv, h_send = exchange(0, pick0)
    h_start()
    c_start, c_recv, c_send = gather(0, cgl, cg)
    c_start()

    for m in range(4):
        if m > 0:
            prev = rows[m - 1]
            for l in range(5):
                nxt = a[l] * hdot(prev, g_ref[l])
                rows[m, 2 * l : 2 * l + 2, :] = nxt[2 * l : 2 * l + 2]
        re0[2 * m : 2 * m + 2, :] = rows[m, 0:2, :]
    tile = corner_tile(1, 4, jnp.zeros((16, 128), f32))
    cgl2[...] = tile
    cg2[k] = tile
    c2_start, c2_recv, c2_send = gather(4, cgl2, cg2)
    c2_start()

    r0 = re0[...]
    for i in range(4):
        fx = S0[0, 4 + 8 * i : 12 + 8 * i, 8:40, :].reshape(256, 128)
        el0[:, 256 * i : 256 * i + 256] = dot3(r0, fx, True)
    e0[k] = el0[...]
    g0_start, g0_recv, g0_send = gather(1, el0, e0)
    g0_start()
    for p in range(16):
        l, m = pair_of(p)
        re1[2 * p : 2 * p + 2, :] = rows[m - 1, 2 * l : 2 * l + 2, :]
    for l in range(1, 5):
        clear2(S[l])
        clear2(M[l])
    for name in MESSAGES:
        if name not in ("f0", "g1", "f1"):
            clear(r_["in_" + name])

    def side_phi(i, c):
        S0[1, 4 + i, 0:8, :] = jnp.zeros((8, 128), f32)
        S0[1, 4 + i, 40:48, :] = jnp.zeros((8, 128), f32)
        return c
    lax.fori_loop(0, 32, side_phi, 0)

    h_recv()
    for d, (dx, dy) in enumerate(DIRS):
        yd = 4 if dy == 1 else 40
        if dy != 0 and dx == 0:
            for t in range(16):
                S0[0, 4 + t, yd : yd + 4, :] = ib0[d, t, 0:4, :]
                S0[0, 20 + t, yd : yd + 4, :] = ib0[d, t, 4:8, :]
        elif dy != 0:
            for t in range(4):
                r = 4 * (t % 2)
                S0[0, (0 if dx == 1 else 36) + t, yd : yd + 4, :] = ib0[d, t // 2, r : r + 4, :]
    elh[:, 0:384] = dot3(
        r0, jnp.concatenate([S0[0, 0:4].reshape(192, 128), S0[0, 36:40].reshape(192, 128)], 0), True
    )
    fx = jnp.concatenate([S0[0, 4:36, 4:8, :], S0[0, 4:36, 40:44, :]], 1).reshape(256, 128)
    elh[:, 384:640] = dot3(r0, fx, True)
    eh[k] = elh[...]
    gh_start, gh_recv, gh_send = gather(3, elh, eh)
    gh_start()
    sends += [h_send, c_send, c2_send, g0_send, gh_send]

    c_recv()
    CG = cg[0:8].reshape(128, 128)
    CG2 = [None]
    ri, ci = iota((128, 128), 0), iota((128, 128), 1)
    same = (ri >> 1) == (ci >> 1)
    odd = (ci & 1) == 1
    eye = jnp.where(ri == ci, 1.0, 0.0).astype(f32)

    def col(c):
        src = CG2[0] if 2 <= c < 8 else CG
        return jnp.broadcast_to(src[:, c : c + 1], (128, 128))

    def corner(n):
        return jnp.where(same, jnp.where(odd, col(2 * n + 1), col(2 * n)), 0.0)

    lrow = (ri >> 1) & 7
    inva = jnp.zeros((128, 128), f32)
    for l in range(5):
        inva = jnp.where(lrow == l, 1.0 / a[l], inva)
    face = col(8)
    face_up = jnp.concatenate([face[16:], jnp.zeros((16, 128), f32)], 0)
    K = inva * (
        jnp.where(((ri & 1) == 0) & (ci == ri - 15), face, 0.0)
        + jnp.where(((ri & 1) == 1) & (ci == ri + 15), face_up, 0.0)
    )
    R = corner(0)
    blk = (ri >> 4) + (ri & 1)
    for st in (1, 2, 4):
        link = jnp.where((blk & (2 * st - 1)) == st, K, 0.0)
        d = R * eye
        drow = jnp.sum(d, 1, keepdims=True)
        dcol = jnp.sum(d, 0, keepdims=True)
        off = link / (1.0 - link * link * drow * dcol)
        diag = jnp.sum(off * link * dcol, 1, keepdims=True)
        R = R + hdot(hdot(R, off + eye * diag), R)
    W = eye + hdot(R, K)
    c2_recv()
    CG2[0] = cg2[...].reshape(128, 128)
    B2, B3, B4 = dot3(corner(1), K), dot3(corner(2), K), dot3(corner(3), K)
    V1 = dot3(W, dot3(B2, W))
    V2 = dot3(W, dot3(B3, W) + dot3(B2, V1))
    V3 = dot3(W, dot3(B4, W) + dot3(B3, V1) + dot3(B2, V2))
    VS = [W, V1, V2, V3]

    def lm_of(p):
        l = jnp.where(p < 12, (p >> 2) + 1, jnp.where(p < 14, 0, 4))
        m = jnp.where(p < 12, (p & 3) + 1, (p & 1) + 1)
        return l, m

    def funct(level):
        width = 64 if level == 0 else 256
        rr, rc = iota((128, 128), 0), iota((128, 128), 1)
        p, side = rr & 15, rr >> 4
        if level == 0:
            l, m = jnp.zeros_like(p), p - 11
            live = (rr < 32) & (p >= 12)
        else:
            l, m = lm_of(p)
            live = rr < 32
        target = jnp.where(side == 0, (k - 1) * 16 + l * 2 + 1, (k + 1) * 16 + l * 2)
        pick_rows = jnp.where(live & (rc == target), 1.0, 0.0).astype(f32)
        er, ec = iota((128, width), 0), iota((128, width), 1)
        if level == 0:
            jc, lc, mc, endc = ec >> 3, jnp.zeros_like(ec), ((ec >> 1) & 3) + 1, ec & 1
        else:
            jc, endc = ec >> 5, ec & 1
            lc, mc = lm_of((ec >> 1) & 15)
        expand = jnp.where(er == jc * 16 + lc * 2 + endc, 1.0, 0.0).astype(f32)
        wr = iota((128, width), 0)
        mrow = ((wr & 15) - 11) if level == 0 else lm_of(wr & 15)[1]
        out = jnp.zeros((128, width), f32)
        for n in range(4):
            x = dot3(dot3(pick_rows, VS[n]), expand)
            out = out + jnp.where(mrow - mc == n, x, 0.0)
        return out

    L0 = funct(0)

    side_in, side_out = ri >> 4, ci >> 4
    pi, po = ri & 15, ci & 15
    fl = (ri < 32) & (ci < 32) & (side_in == side_out)
    li, mi = lm_of(pi)
    lo, mo = lm_of(po)
    aout = jnp.zeros((128, 128), f32)
    for l in range(5):
        aout = jnp.where(lo == l, a[l], aout)
    cm = jnp.broadcast_to(zf_ref[0:1, 0:1], (1, 128))
    cp = jnp.broadcast_to(cg[k + 1, 0:1, 8:9], (1, 128))

    def matrices():
        for l in range(5):
            gt = g_ref[l].T
            p1 = pid(l, 1)
            ut = jnp.where(ri == p1, jnp.broadcast_to(cm * gt[0:1], (128, 128)), 0.0)
            ut = jnp.where(ri == 16 + p1, jnp.broadcast_to(cp * gt[127:128], (128, 128)), ut)
            if l == 0:
                q = jnp.where(fl & (pi >= 13) & (pi == po + 1), 1.0, 0.0)
            else:
                den = jnp.where(lo == l, 1.0, a[l] - aout)
                amp = a[l] / den
                nb = -aout / den
                p2 = nb * nb
                p3 = p2 * nb
                dm = mo - mi
                pw = jnp.where(dm == 0, 1.0, jnp.where(dm == 1, nb, jnp.where(dm == 2, p2, p3)))
                pm = jnp.where(mo == 1, nb, jnp.where(mo == 2, p2, jnp.where(mo == 3, p3, p2 * p2)))
                q = jnp.where((li == lo) & (dm >= 0), amp * pw, 0.0)
                q = q + jnp.where((li == l) & (mi == 1), pm, 0.0)
                q = jnp.where(lo == l, jnp.where((li == l) & (mi == mo + 1), 1.0, 0.0), q)
                q = jnp.where(fl, q, 0.0)
            for r, v in ((0, a[l] * gt), (128, ut)):
                vh, vl = split(v)
                th[l, r : r + 128, 0:128] = vh
                tl[l, r : r + 128, 0:128] = vl
            qh, ql = split(q.astype(f32))
            zero = jnp.zeros((128, 128), bf16)
            th[l, 0:128, 128:256] = zero
            tl[l, 0:128, 128:256] = zero
            th[l, 128:256, 128:256] = qh
            tl[l, 128:256, 128:256] = ql

    gt = a[0] * g_ref[0].T
    gh, gl = split(gt)
    ra[0:128, 0:128] = gh
    ra[128:256, 0:128] = gh
    ra[0:128, 128:256] = gl
    ra[128:256, 128:256] = jnp.zeros((128, 128), bf16)
    gt = g_ref[0].T
    for i in range(4):
        row = ri & 31
        u = jnp.where(row == 12 + i, jnp.broadcast_to(cm * gt[0:1], (128, 128)), 0.0)
        u = jnp.where(row == 28 + i, jnp.broadcast_to(cp * gt[127:128], (128, 128)), u)
        uh, ul = split(u)
        u = jnp.where(ri < 64, uh.astype(f32), jnp.where(ri < 96, ul.astype(f32), 0.0))
        ub[:, 128 * i : 128 * i + 128] = u.astype(bf16)

    def apply(l, src, dst, step, n, scale=None):
        y = src.shape[2]

        def body(i, c):
            x = pl.ds(i * step, step)
            v = jnp.concatenate(
                [src[0, x].reshape(step * y, 128), src[1, x].reshape(step * y, 128)], 1
            )
            vh, vl = split(v)
            t = mm(vh, th[l]) + (mm(vh, tl[l]) + mm(vl, th[l]))
            if scale is not None:
                t = scale * t
            dst[0, x] = t[:, 0:128].reshape(step, y, 128)
            dst[1, x] = t[:, 128:256].reshape(step, y, 128)
            return c

        lax.fori_loop(0, n, body, 0)

    def solve_block(src, dst):
        n, y = src.shape[1], src.shape[2]
        v = jnp.concatenate([src[0].reshape(n * y, 128), src[1].reshape(n * y, 128)], 1)
        vh, vl = split(v)
        t = mm(vh, jnp.concatenate([th[0, :, 0:128], tl[0, :, 0:128]], 1))
        t = t[:, 0:128] + (t[:, 128:256] + mm(vl, th[0, :, 0:128]))
        dst[0] = t.reshape(n, y, 128)

    def solves(src, dsts):
        n, y = src.shape[1], src.shape[2]
        v = jnp.concatenate([src[0].reshape(n * y, 128), src[1].reshape(n * y, 128)], 1)
        vh, vl = split(v)
        for dst, i, scale in dsts:
            t = mm(vh, th[i]) + (mm(vh, tl[i]) + mm(vl, th[i]))
            if scale is not None:
                t = scale * t
            dst[0] = t[:, 0:128].reshape(n, y, 128)
            dst[1] = t[:, 128:256].reshape(n, y, 128)

    def product(i, l1, l2):
        t = mm(th[l1], th[l2]) + (mm(th[l1], tl[l2]) + mm(tl[l1], th[l2]))
        h, lo_ = split(t)
        th[i] = h
        tl[i] = lo_

    def square(l):
        product(4 + l, l, l)

    def both(l):
        product(8 + l, l + 1, l)

    def stencil(l, src, dst, grow, post, halves=(0, 1)):
        ox, oy, n, y = OX[l], OY[l], LX[l], SY[l]
        gy0 = iota((y, 128), 0) + (iy * n - oy)
        ym = jnp.where((gy0 >= 0) & (gy0 < ngy * n), 0.25, 0.0).astype(f32)
        total = n + 2 * grow
        step = next(u for u in (4, 3, 2, 1) if total % u == 0)

        def body(i, c):
            x0 = ox - grow + i * step
            outs = []
            for h in halves:
                r = [src[h, x0 - 1 + j] for j in range(step + 2)]
                for j in range(step):
                    gx0 = ix * n + (x0 + j - ox)
                    s = jnp.where((gx0 >= 0) & (gx0 < ngx * n), 1.0, 0.0).astype(f32)
                    t = (r[j] + r[j + 2]) + (
                        pltpu.roll(r[j + 1], 1, 0) + pltpu.roll(r[j + 1], y - 1, 0)
                    )
                    outs.append((h, x0 + j, post(h, x0 + j, (ym * s) * t)))
            for o in outs:
                dst(*o)
            return c

        lax.fori_loop(0, total // step, body, 0)

    def into(ref):
        def put(h, x, v):
            ref[h, x] = v
        return put

    def solve(l, src, dst, matrix=None, scale=None):
        step, n = SX[l], 1
        apply(l if matrix is None else matrix, src, dst, step, n, scale)

    def residual(l, halves=(0, 1)):
        s, ta, tb = S[l], at("TA", l), at("TB", l)
        aa, bb = at("AA", l), at("BB", l)
        solves(s, [(ta, l, None), (tb, 4 + l, None)])
        stencil(l, tb, into(bb), 1, lambda h, x, v: 0.32 * ta[h, x] + 0.64 * v, halves)
        stencil(l, bb, into(aa), 0, lambda h, x, v: 0.04 * s[h, x] + v, halves)

    def smoothed(l):
        w = 0
        s, ta, tb, tc = S[l], at("TA", l), at("TB", l), at("TC", l)
        bb, cc, ma = at("BB", l), at("CC", l), at("MA", l)
        solve(l, tb, tc)
        stencil(l, tc, into(bb), 2 + w, lambda h, x, v: 0.8192 * tb[h, x] + 0.4096 * v)
        stencil(l, bb, into(cc), 1 + w, lambda h, x, v: 0.9728 * ta[h, x] + v)
        stencil(l, cc, into(ma), w, lambda h, x, v: 0.9984 * s[h, x] + v)

    def restrict(l, put, halves=(0, 1)):
        ox, oy, n = OX[l], OY[l], LX[l] // 2
        aa = at("AA", l)

        def body(i, c):
            x = ox + 2 * i
            for h in halves:
                even, off = pl.ds(oy, n, 2), pl.ds(oy + 1, n, 2)
                v = (aa[h, x, even, :] + aa[h, x, off, :]) + (
                    aa[h, x + 1, even, :] + aa[h, x + 1, off, :]
                )
                put(h, i, 0.25 * v)
            return c

        lax.fori_loop(0, n, body, 0)

    def prolong(l, fields, outs, halves):
        c = l + 1
        w = 1 if l == 0 else 0
        n, ox, oc, y = LX[c], OX[l], OX[c], SY[c]
        ys, cnt = [(0, 24), (2, 12), (2, 8), (2, 8)][l]
        gyc = iota((cnt, 128), 0) + (iy * n + ys - OY[c])
        ym = jnp.where((gyc >= 0) & (gyc < ngy * n), 1.0, 0.0).astype(f32)

        def body(j, carry):
            j = j - (1 + w)
            gx = ix * n + j
            s = jnp.where((gx >= 0) & (gx < ngx * n), 1.0, 0.0).astype(f32)
            ms = ym * s
            for h in halves:
                lower, here, upper = (fields(h, oc + j + i) for i in (-1, 0, 1))
                for (o, oh), lo_, he, up_ in zip(outs, lower, here, upper):
                    oh = h if oh is None else oh
                    for i, far in enumerate((lo_, up_)):
                        v = 0.75 * he + 0.25 * far
                        ev = (0.75 * v + 0.25 * pltpu.roll(v, 1, 0))[ys : ys + cnt]
                        od = (0.75 * v + 0.25 * pltpu.roll(v, y - 1, 0))[ys : ys + cnt]
                        o[oh, ox + 2 * j + i, pl.ds(0, cnt, 2), :] = ms * ev
                        o[oh, ox + 2 * j + i, pl.ds(1, cnt, 2), :] = ms * od
            return carry

        lax.fori_loop(0, n + 2 + 2 * w, body, 0)

    def correct(l, store):
        c = l + 1
        m, u, g2 = M[c], at("U", c), at("V", c)
        kap = a[l] / a[c]
        solves(m, [(u, c, kap), (g2, 8 + l, 0.64 * kap)])
        q = 0.04 * (1.0 - a[c] / a[l])
        outs = [at("P0", l), at("P1", l), at("P2", l)]

        def fields(h, x):
            uv = u[h, x]
            return (0.04 * m[h, x] + q * uv, 0.32 * uv, g2[h, x])

        prolong(l, fields, [(o, None) for o in outs], (0, 1))
        cc, ma = at("CC", l), at("MA", l)
        stencil(l, outs[2], into(cc), 1, lambda h, x, v: outs[1][h, x] + v)
        stencil(l, cc, store, 0, lambda h, x, v: (ma[h, x] + outs[0][h, x]) + v)

    def parts(et):
        phi = dot3(L0, et).T
        h, lo_ = split(phi)
        h, lo_ = h.astype(f32), lo_.astype(f32)
        return h + pltpu.roll(lo_, 32, 1) + pltpu.roll(h, 64, 1)

    def powers(first, src, d1, d2):
        for i in range(5):
            x = slice(8 * i, 8 * i + 8)
            w = S0[1, x].reshape(384, 128).astype(bf16)
            c = mm(w, ub[:, 128 * first : 128 * first + 256])
            vh, vl = split(src[0, x].reshape(384, 128))
            t = mm(jnp.concatenate([vh, vl], 1), ra[...])
            t = (t[:, 0:128] + t[:, 128:256]) + c[:, 0:128]
            d1[0, x] = t.reshape(8, 48, 128)
            vh, vl = split(t)
            t = mm(jnp.concatenate([vh, vl], 1), ra[...])
            t = (t[:, 0:128] + t[:, 128:256]) + c[:, 128:256]
            d2[0, x] = t.reshape(8, 48, 128)

    g0_recv()
    for i in range(4):
        w = parts(e0[:, :, 256 * i : 256 * i + 256].reshape(64, 256))
        S0[1, 4 + 8 * i : 12 + 8 * i, 8:40, :] = w.reshape(8, 32, 128)
    gh_recv()
    w = parts(eh[:, :, 0:384].reshape(64, 384))
    S0[1, 0:4] = w[0:192].reshape(4, 48, 128)
    S0[1, 36:40] = w[192:384].reshape(4, 48, 128)
    w = parts(eh[:, :, 384:640].reshape(64, 256)).reshape(32, 8, 128)
    S0[1, 4:36, 4:8, :] = w[:, 0:4]
    S0[1, 4:36, 40:44, :] = w[:, 4:8]

    t1, t2, t3, t4 = at("TA", 0), at("TB", 0), at("TC", 0), at("P0", 0)
    aa0, bb0, cc0, ma0 = at("AA", 0), at("BB", 0), at("CC", 0), at("MA", 0)
    powers(0, S0, t1, t2)
    stencil(0, t2, into(bb0), 1, lambda h, x, v: 0.32 * t1[h, x] + 0.64 * v, (0,))
    stencil(0, bb0, into(aa0), 0, lambda h, x, v: 0.04 * S0[h, x] + v, (0,))

    def put1(h, i, v):
        S1[h, 3 + i, 4:20, :] = v
    restrict(0, put1, (0,))
    el1[...] = dot3(re1[...], S1[0, 3:19, 4:20, :].reshape(256, 128), True)
    e1[k] = el1[...]
    g1_start, g1_recv, g1_send = gather(2, el1, e1)
    g1_start()
    x1_start, x1_finish, x1_send = packed(1, 1, "g1", S1, True, False)
    x1_start()

    L1 = funct(1)
    matrices()
    powers(2, t2, t3, t4)
    for l in (1, 2, 3):
        square(l)

    def both0(h, x, v):
        bb0[0, x] = 0.8192 * t3[0, x] + 0.4096 * v
        bb0[1, x] = 0.4096 * (t3[0, x] + v)

    g1_recv()
    phi = dot3(L1, e1[...].reshape(256, 256))
    S1[1, 3:19, 4:20, :] = phi.T.reshape(16, 16, 128)
    y1_start, y1_finish, y1_send = packed(2, 1, "f1", S1, False, True)
    y1_start()
    stencil(0, t4, both0, 3, lambda h, x, v: v, (0,))
    stencil(0, bb0, into(cc0), 2, lambda h, x, v: (0.1536 if h else 0.9728) * t2[0, x] + v)
    x1_finish()
    y1_finish()
    residual(1)

    def put2(h, i, v):
        S2[h, 3 + i, 4:12, :] = v
    restrict(1, put2)
    x2_start, x2_finish, x2_send = packed(3, 2, "s2", S2)
    x2_start()
    smoothed(1)
    stencil(0, cc0, into(aa0), 1, lambda h, x, v: (0.0256 if h else 0.9984) * t1[0, x] + v)

    x2_finish()
    residual(2)

    def put3(h, i, v):
        S3[h, 4 + i, 4:8, :] = v
    restrict(2, put3)
    x3_start, x3_finish, x3_send = packed_block(4, 3, "s3", S3)
    x3_start()
    smoothed(2)
    stencil(0, aa0, into(ma0), 0, lambda h, x, v: 0.0016 * S0[0, x] + v, (1,))

    x3_finish()
    residual(3)

    def put4(h, i, v):
        S4[h, 4 + i, 4:6, :] = v
    restrict(3, put4)
    x4_start, x4_finish, x4_send = packed_block(5, 4, "s4", S4, FAR)
    x4_start()
    smoothed(3)
    for l in (3, 2, 1, 0):
        both(l)

    x4_finish()
    ta4 = at("TA", 4)
    solve(4, S4, ta4)

    stencil(4, ta4, into(M4), 2, lambda h, x, v: 0.96 * S4[h, x] + 0.64 * v)

    def putm3(h, x, v):
        M3[h, x, 4:8, :] = v[4:8]
    correct(3, putm3)
    z3_start, z3_finish, z3_send = packed_block(7, 3, "m3", M3)
    z3_start()
    z3_finish()

    def putm2(h, x, v):
        M2[h, x, 4:12, :] = v[4:12]
    correct(2, putm2)
    z2_start, z2_finish, z2_send = packed(8, 2, "m2", M2)
    z2_start()
    z2_finish()

    def putm1(h, x, v):
        M1[h, x, 4:20, :] = v[4:20]
    correct(1, putm1)
    z1_start, z1_finish, z1_send = packed(9, 1, "m1", M1)
    z1_start()
    z1_finish()

    u, g2 = at("U", 1), at("V", 1)
    kap = a[0] / a[1]
    solves(M1, [(u, 1, kap), (g2, 8, 0.64 * kap)])
    solve_block(M1, HM)
    solve_block(g2, H2)
    q = 0.04 * (1.0 - a[1] / a[0])

    def fields0(h, x):
        uv, gv = u[0, x], g2[0, x]
        h0 = 0.04 * HM[0, x] + (q / 0.64) * gv
        return (0.04 * M1[0, x] + q * uv, h0 - 0.32 * uv, 0.5 * gv, H2[0, x], h0)

    P0, P1, P2 = at("P0", 0), at("P1", 0), at("P2", 0)
    prolong(0, fields0, [(P0, 0), (P0, 1), (P1, 0), (P1, 1), (P2, 0)], (0,))

    def pair(h, x, v):
        bb0[0, x] = v - P1[0, x]
        bb0[1, x] = v + P1[0, x]
    stencil(0, P1, pair, 2, lambda h, x, v: v, (1,))
    stencil(0, bb0, into(cc0), 1, lambda h, x, v: P0[1, x] + v, (0,))
    inv0 = 1.0 / a[0]

    def put_sol(h, x, v):
        sol_ref[x - 4] = v[8:40]

    def put_res(h, x, v):
        res_ref[x - 4] = v[8:40]
    stencil(0, bb0, put_sol, 0, lambda h, x, v: inv0 * ((aa0[0, x] + P2[0, x]) + v), (1,))
    stencil(0, cc0, put_res, 0, lambda h, x, v: (ma0[1, x] - P0[0, x]) + v, (0,))

    for wait in sends + [
        x1_send, g1_send, y1_send, x2_send, x3_send, x4_send, z3_send, z2_send, z1_send
    ]:
        wait()


def body(sizes, right_side, z_faces, xy_coupling, block_inverse):
    n = right_side.shape
    vmem = pl.BlockSpec(memory_space=pltpu.VMEM)
    hbm = pl.BlockSpec(memory_space=pl.ANY)
    scratch = [pltpu.VMEM(s, f32) for s in scratch_shapes().values()]
    scratch += [pltpu.VMEM((5, 128, 128), f32)]
    scratch += [pltpu.VMEM((12, 256, 256), bf16), pltpu.VMEM((12, 256, 256), bf16)]
    scratch += [pltpu.VMEM((256, 256), bf16), pltpu.VMEM((128, 512), bf16)]
    scratch += [pltpu.SemaphoreType.DMA((10, 20)), pltpu.SemaphoreType.DMA((10, 20))]
    scratch += [pltpu.SemaphoreType.DMA((5, 8)), pltpu.SemaphoreType.DMA((5, 8))]
    scratch += [pltpu.SemaphoreType.DMA((4,)), pltpu.VMEM((1, 128), f32), pltpu.SMEM((5,), f32)]
    return pl.pallas_call(
        lambda *r: kernel(sizes, *r),
        out_shape=(pltpu.VMEM(n, f32), pltpu.VMEM(n, f32)),
        in_specs=[hbm, hbm, hbm, hbm],
        out_specs=(vmem, vmem),
        scratch_shapes=scratch,
        compiler_params=pltpu.CompilerParams(
            collective_id=0, has_side_effects=True, vmem_limit_bytes=60 * 2**20
        ),
        name="vcycle",
    )(right_side, z_faces.reshape(1, -1), block_inverse, xy_coupling)


def solution(mesh):
    sizes = tuple(mesh.shape[n] for n in ("gx", "gy", "gz"))
    return jax.shard_map(
        lambda *args: body(sizes, *args),
        mesh=mesh,
        in_specs=(P("gx", "gy", "gz"), P("gz"), P(), P(None, "gz", None)),
        out_specs=(P("gx", "gy", "gz"), P("gx", "gy", "gz")),
        check_vma=False,
    )
```

```python
import jax
import jax.numpy as jnp
from jax import lax
from jax.experimental import pallas as pl
from jax.experimental.pallas import tpu as pltpu
from jax.sharding import PartitionSpec as P

f32 = jnp.float32
bf16 = jnp.bfloat16
HI = lax.Precision.HIGHEST
MESH = pl.DeviceIdType.MESH
FAR = [(dx, dy) for dx in (-2, -1, 0, 1, 2) for dy in (-2, -1, 0, 1, 2) if 0 < abs(dx) + abs(dy) < 4]
DIRS = [(dx, dy) for dx in (-1, 0, 1) for dy in (-1, 0, 1) if (dx, dy) != (0, 0)]

LX = [32, 16, 8, 4, 2]
OX = [4, 3, 3, 4, 4]
OY = [8, 4, 4, 4, 4]
SX = [40, 22, 14, 12, 10]
SY = [48, 24, 16, 16, 16]


def pair_of(p):
    if p < 12:
        return p // 4 + 1, p % 4 + 1
    return (0 if p < 14 else 4), p % 2 + 1


def pid(l, m):
    if l == 0:
        return 11 + m
    if l == 4:
        return 13 + m
    return (l - 1) * 4 + m - 1


def split(x):
    h = x.astype(bf16)
    return h, (x - h.astype(f32)).astype(bf16)


def mm(a, b, trans_b=False):
    dims = (((1,), (1 if trans_b else 0,)), ((), ()))
    return lax.dot_general(a, b, dims, preferred_element_type=f32)


def dot3(a, b, trans_b=False):
    ah, al = split(a)
    bh, bl = split(b)
    return mm(ah, bh, trans_b) + (mm(ah, bl, trans_b) + mm(al, bh, trans_b))


def hdot(a, b):
    return jnp.dot(a, b, precision=HI, preferred_element_type=f32)


def iota(shape, dim):
    return lax.broadcasted_iota(jnp.int32, shape, dim)


MESSAGES = {"f0": 16, "g1": 8, "f1": 2, "s2": 5, "s3": 3, "s4": 1, "m3": 3, "m2": 5, "m1": 10}


def scratch_shapes():
    out = {}
    for l in range(5):
        out[f"S{l}"] = (2, SX[l], SY[l], 128)
        for t in ("TA", "TB", "TC", "AA", "BB", "CC", "MA", "P0", "P1", "P2"):
            out[f"{t}{l}"] = (2, SX[l], SY[l], 128)
        if l:
            for t in ("M", "U", "V"):
                out[f"{t}{l}"] = (2, SX[l], SY[l], 128)
    out["HM"] = out["H2"] = (2, SX[1], SY[1], 128)
    for name, tiles in MESSAGES.items():
        out["out_" + name] = out["in_" + name] = (len(FAR) if name == "s4" else 8, tiles, 8, 128)
    out["rows"] = (4, 16, 128)
    out["re0"] = (8, 128)
    out["re1"] = (32, 128)
    out["cg"] = (9, 16, 128)
    out["cgl"] = out["cgl2"] = (16, 128)
    out["cg2"] = (8, 16, 128)
    out["e0"] = (8, 8, 1024)
    out["eh"] = (8, 8, 640)
    out["e1"] = (8, 32, 256)
    out["el0"] = (8, 1024)
    out["elh"] = (8, 640)
    out["el1"] = (32, 256)
    return out


def kernel(sizes, f_ref, zf_in, ginv_ref, e_in, sol_ref, res_ref, *refs):
    names = list(scratch_shapes())
    r_ = dict(zip(names, refs))
    g_ref, th, tl, ra, ub, hs, hr, gs, gr, ls, zf_ref, e_ref = refs[len(names):]
    S0, S1, S2, S3, S4 = [r_[f"S{l}"] for l in range(5)]
    M1, M2, M3, M4 = [r_[f"M{l}"] for l in range(1, 5)]
    rows, re0, re1, cg, cgl = r_["rows"], r_["re0"], r_["re1"], r_["cg"], r_["cgl"]
    e0, e1, el0, el1 = r_["e0"], r_["e1"], r_["el0"], r_["el1"]
    eh, elh, HM, H2 = r_["eh"], r_["elh"], r_["HM"], r_["H2"]
    cg2, cgl2 = r_["cg2"], r_["cgl2"]

    ngx, ngy, ngz = sizes
    ix, iy, k = lax.axis_index("gx"), lax.axis_index("gy"), lax.axis_index("gz")
    S = [S0, S1, S2, S3, S4]
    M = [None, M1, M2, M3, M4]

    def at(name, l):
        return r_[f"{name}{l}"]


    def peer(o):
        return jnp.where(k + o >= ngz, k + o - ngz, k + o)

    def exists(dx, dy):
        x, y = ix + dx, iy + dy
        return (x >= 0) & (x < ngx) & (y >= 0) & (y < ngy)

    def clear(ref):
        def step(i, c):
            ref[i] = jnp.zeros(ref.shape[1:], f32)
            return c
        lax.fori_loop(0, ref.shape[0], step, 0)

    def clear2(ref):
        def step(i, c):
            for h in range(2):
                ref[h, i] = jnp.zeros(ref.shape[2:], f32)
            return c
        lax.fori_loop(0, ref.shape[1], step, 0)

    load_f = pltpu.make_async_copy(f_ref, S0.at[0, 4:36, 8:40, :], ls.at[0])
    load_g = pltpu.make_async_copy(ginv_ref, g_ref, ls.at[1])
    load_z = pltpu.make_async_copy(zf_in, zf_ref, ls.at[2])
    load_e = pltpu.make_async_copy(e_in, e_ref, ls.at[3])
    for load in (load_e, load_z, load_g, load_f):
        load.start()

    barrier = pltpu.get_barrier_semaphore()
    count = jnp.int32(ngz - 1)
    for dx, dy in FAR:
        ok = exists(dx, dy)

        @pl.when(ok)
        def _():
            pl.semaphore_signal(
                barrier, inc=1, device_id=(ix + dx, iy + dy, k), device_id_type=MESH
            )

        count = count + jnp.where(ok, 1, 0)
    for o in range(1, ngz):
        pl.semaphore_signal(
            barrier, inc=1, device_id=(ix, iy, peer(o)), device_id_type=MESH
        )

    for d, (dx, dy) in enumerate(DIRS):
        @pl.when(jnp.logical_not(exists(-dx, -dy)))
        def _():
            for name in ("f0", "g1", "f1"):
                r = r_["in_" + name]
                for t in range(MESSAGES[name]):
                    r[d, t] = jnp.zeros((8, 128), f32)
            if dy == 0:
                for i in range(4):
                    S0[0, (0 if dx == 1 else 36) + i, 8:40, :] = jnp.zeros((32, 128), f32)

    def sides(i, c):
        S0[0, i, 0:8, :] = jnp.zeros((8, 128), f32)
        S0[0, i, 40:48, :] = jnp.zeros((8, 128), f32)
        return c
    lax.fori_loop(0, 40, sides, 0)
    clear(rows)
    if ngz < 8:
        for r in (e0, eh, e1, cg2):
            clear(r)
    cg[8] = jnp.zeros((16, 128), f32)

    def exchange(phase, pick, dirs=DIRS):
        def copy(d, dx, dy):
            src, dst = pick(dx, dy)
            return pltpu.make_async_remote_copy(
                src_ref=src, dst_ref=dst, send_sem=hs.at[phase, d], recv_sem=hr.at[phase, d],
                device_id=(ix + dx, iy + dy, k), device_id_type=MESH,
            )

        def start():
            for d, (dx, dy) in sorted(enumerate(dirs), key=lambda i: -abs(i[1][0]) - abs(i[1][1])):
                @pl.when(exists(dx, dy))
                def _():
                    copy(d, dx, dy).start()

        def wait_recv():
            for d, (dx, dy) in enumerate(dirs):
                @pl.when(exists(-dx, -dy))
                def _():
                    copy(d, dx, dy).wait_recv()

        def wait_send():
            for d, (dx, dy) in enumerate(dirs):
                @pl.when(exists(dx, dy))
                def _():
                    copy(d, dx, dy).wait_send()

        return start, wait_recv, wait_send

    def span(d, off, n, h):
        if d == 0:
            return pl.ds(off, n), pl.ds(off, n)
        if d == 1:
            return pl.ds(off + n - h, h), pl.ds(off - h, h)
        return pl.ds(off, h), pl.ds(off + n, h)

    def lanes_of(planes):
        out = planes[0]
        for i, v in enumerate(planes[1:]):
            out = out + pltpu.roll(v, 32 * (i + 1), 1)
        return out

    low_lanes = {r: iota((r, 128), 1) < 32 for r in (8,)}

    def lanes_back(tile, i):
        v = tile if i == 0 else pltpu.roll(tile, 128 - 32 * i, 1)
        return jnp.where(low_lanes[8], v, 0.0)

    def tiles_of(l, dx, dy, wf, wp):
        n = LX[l]
        if dx == 0:
            return (n // 2 if wf else 0) + ((n + 7) // 8 if wp else 0)
        if dy == 0:
            return (3 * n // 8 if wf else 0) + (n // 8 if wp else 0)
        return 2 if wf else 1

    def packed(phase, l, name, buf, wf=True, wp=True):
        n, ox, oy = LX[l], OX[l], OY[l]
        ob, ib = r_["out_" + name], r_["in_" + name]

        def pick(dx, dy):
            d, t = DIRS.index((dx, dy)), tiles_of(l, dx, dy, wf, wp)
            return ob.at[d, 0:t], ib.at[d, 0:t]

        start0, wait_recv, wait_send = exchange(phase, pick)

        def start():
            for d, (dx, dy) in enumerate(DIRS):
                xs = ox + n - 3 if dx == 1 else ox
                ys = oy + n - 4 if dy == 1 else oy
                yt = ys // 8 * 8
                part = slice(ys - yt, ys - yt + 4)
                if dx == 0:
                    base = n // 2 if wf else 0
                    if wf:
                        for t in range(n // 2):
                            ob[d, t, 0:4, :] = buf[0, ox + t, ys : ys + 4, :]
                            ob[d, t, 4:8, :] = buf[0, ox + t + n // 2, ys : ys + 4, :]
                    if wp:
                        for b in range(n // 4):
                            v = lanes_of([buf[1, ox + 4 * b + i, yt : yt + 8, :] for i in range(4)])
                            r = 4 * (b % 2)
                            ob[d, base + b // 2, r : r + 4, :] = v[part]
                elif dy == 0:
                    m = n // 8
                    base = 3 * m if wf else 0
                    for r in range(m):
                        y = slice(oy + 8 * r, oy + 8 * r + 8)
                        if wf:
                            for i in range(3):
                                ob[d, i * m + r] = buf[0, xs + i, y, :]
                        if wp:
                            ob[d, base + r] = lanes_of([buf[1, xs + i, y, :] for i in range(3)])
                else:
                    if wf:
                        ob[d, 0, 0:4, :] = buf[0, xs, ys : ys + 4, :]
                        ob[d, 0, 4:8, :] = buf[0, xs + 1, ys : ys + 4, :]
                        ob[d, 1, 0:4, :] = buf[0, xs + 2, ys : ys + 4, :]
                    if wp:
                        v = lanes_of([buf[1, xs + i, yt : yt + 8, :] for i in range(3)])
                        ob[d, 1 if wf else 0, 4:8, :] = v[part]
            start0()

        def finish():
            wait_recv()
            for d, (dx, dy) in enumerate(DIRS):
                xd = ox - 3 if dx == 1 else ox + n
                yd = oy - 4 if dy == 1 else oy + n
                if dx == 0:
                    base = n // 2 if wf else 0
                    if wf:
                        for t in range(n // 2):
                            buf[0, ox + t, yd : yd + 4, :] = ib[d, t, 0:4, :]
                            buf[0, ox + t + n // 2, yd : yd + 4, :] = ib[d, t, 4:8, :]
                    if wp:
                        for b in range(n // 4):
                            tile, r = ib[d, base + b // 2], 4 * (b % 2)
                            for i in range(4):
                                v = lanes_back(tile, i)
                                buf[1, ox + 4 * b + i, yd : yd + 4, :] = v[r : r + 4]
                elif dy == 0:
                    m = n // 8
                    base = 3 * m if wf else 0
                    for r in range(m):
                        y = slice(oy + 8 * r, oy + 8 * r + 8)
                        for i in range(3):
                            if wf:
                                buf[0, xd + i, y, :] = ib[d, i * m + r]
                            if wp:
                                buf[1, xd + i, y, :] = lanes_back(ib[d, base + r], i)
                else:
                    if wf:
                        buf[0, xd, yd : yd + 4, :] = ib[d, 0, 0:4, :]
                        buf[0, xd + 1, yd : yd + 4, :] = ib[d, 0, 4:8, :]
                        buf[0, xd + 2, yd : yd + 4, :] = ib[d, 1, 0:4, :]
                    if wp:
                        tile = ib[d, 1 if wf else 0]
                        for i in range(3):
                            buf[1, xd + i, yd : yd + 4, :] = lanes_back(tile, i)[4:8]

        return start, finish, wait_send

    def packed_block(phase, l, name, buf, dirs=DIRS):
        n = LX[l]
        ob, ib = r_["out_" + name], r_["in_" + name]

        def pick(dx, dy):
            return ob.at[0], ib.at[dirs.index((dx, dy))]

        start0, wait_recv, wait_send = exchange(phase, pick, dirs)

        def start():
            phi = lanes_of([buf[1, 4 + i, 0:8, :] for i in range(n)])
            if n == 4:
                for i in range(4):
                    r = 4 * (i // 2)
                    ob[0, i % 2, r : r + 4, :] = buf[0, 4 + i, 4:8, :]
                ob[0, 2] = phi
            else:
                ob[0, 0, 0:2, :] = buf[0, 4, 4:6, :]
                ob[0, 0, 2:4, :] = buf[0, 5, 4:6, :]
                ob[0, 0, 4:8, :] = phi[4:8]
            start0()

        def finish():
            wait_recv()
            for d, (dx, dy) in enumerate(dirs):
                xd, yd = 4 - n * dx, 4 - n * dy
                tile = ib[d, 2 if n == 4 else 0]
                for i in range(n):
                    v = lanes_back(tile, i)
                    buf[1, xd + i, yd : yd + n, :] = v[4 : 4 + n]
                    if n == 4:
                        r = 4 * (i // 2)
                        buf[0, xd + i, yd : yd + 4, :] = ib[d, i % 2, r : r + 4, :]
                    else:
                        buf[0, xd + i, yd : yd + 2, :] = tile[2 * i : 2 * i + 2]

        return start, finish, wait_send

    def gather(phase, src, buf):
        def copy(o):
            return pltpu.make_async_remote_copy(
                src_ref=src, dst_ref=buf.at[k], send_sem=gs.at[phase, o],
                recv_sem=gr.at[phase, o], device_id=(ix, iy, peer(o)),
                device_id_type=MESH,
            )

        def start():
            for o in range(1, ngz):
                copy(o).start()

        def wait_recv():
            for o in range(1, ngz):
                copy(o).wait_recv()

        def wait_send():
            for o in range(1, ngz):
                copy(o).wait_send()

        return start, wait_recv, wait_send

    sends = []
    ob0, ib0 = r_["out_f0"], r_["in_f0"]

    def pick0(dx, dy):
        d = DIRS.index((dx, dy))
        if dy == 0:
            sx, tx = span(dx, 4, 32, 4)
            return S0.at[0, sx, 8:40, :], S0.at[0, tx, 8:40, :]
        t = 16 if dx == 0 else 2
        return ob0.at[d, 0:t], ib0.at[d, 0:t]

    def ends0(dx):
        return 32 if dx == 1 else 4

    load_e.wait()
    a = [4.0 * e_ref[l] for l in range(5)]
    lane16 = iota((16, 128), 1)

    def corner_tile(first, last, tile):
        for n in range(first, last):
            rn = rows[n]
            tile = jnp.where(lane16 == 2 * n, jnp.broadcast_to(rn[:, 0:1], (16, 128)), tile)
            tile = jnp.where(lane16 == 2 * n + 1, jnp.broadcast_to(rn[:, 127:128], (16, 128)), tile)
        return tile

    load_z.wait()
    load_g.wait()
    for l in range(5):
        rows[0, 2 * l : 2 * l + 1, :] = a[l] * g_ref[l, 0:1, :]
        rows[0, 2 * l + 1 : 2 * l + 2, :] = a[l] * g_ref[l, 127:128, :]
    tile = corner_tile(
        0, 1, jnp.where(lane16 == 8, jnp.broadcast_to(zf_ref[0:1, 0:1], (16, 128)), 0.0)
    )
    cgl[...] = tile
    cg[k] = tile
    load_f.wait()
    for d, (dx, dy) in enumerate(DIRS):
        ys = 36 if dy == 1 else 8
        if dy != 0 and dx == 0:
            for t in range(16):
                ob0[d, t, 0:4, :] = S0[0, 4 + t, ys : ys + 4, :]
                ob0[d, t, 4:8, :] = S0[0, 20 + t, ys : ys + 4, :]
        elif dy != 0:
            for t in range(4):
                r = 4 * (t % 2)
                ob0[d, t // 2, r : r + 4, :] = S0[0, ends0(dx) + t, ys : ys + 4, :]

    pl.semaphore_wait(barrier, count)
    h_start, h_recv, h_send = exchange(0, pick0)
    h_start()
    c_start, c_recv, c_send = gather(0, cgl, cg)
    c_start()

    for m in range(4):
        if m > 0:
            prev = rows[m - 1]
            for l in range(5):
                nxt = a[l] * hdot(prev, g_ref[l])
                rows[m, 2 * l : 2 * l + 2, :] = nxt[2 * l : 2 * l + 2]
        re0[2 * m : 2 * m + 2, :] = rows[m, 0:2, :]
    tile = corner_tile(1, 4, jnp.zeros((16, 128), f32))
    cgl2[...] = tile
    cg2[k] = tile
    c2_start, c2_recv, c2_send = gather(4, cgl2, cg2)
    c2_start()

    r0 = re0[...]
    for i in range(4):
        fx = S0[0, 4 + 8 * i : 12 + 8 * i, 8:40, :].reshape(256, 128)
        el0[:, 256 * i : 256 * i + 256] = dot3(r0, fx, True)
    e0[k] = el0[...]
    g0_start, g0_recv, g0_send = gather(1, el0, e0)
    g0_start()
    for p in range(16):
        l, m = pair_of(p)
        re1[2 * p : 2 * p + 2, :] = rows[m - 1, 2 * l : 2 * l + 2, :]
    def side_phi(i, c):
        S0[1, 4 + i, 0:8, :] = jnp.zeros((8, 128), f32)
        S0[1, 4 + i, 40:48, :] = jnp.zeros((8, 128), f32)
        return c
    lax.fori_loop(0, 32, side_phi, 0)

    h_recv()
    for d, (dx, dy) in enumerate(DIRS):
        yd = 4 if dy == 1 else 40
        if dy != 0 and dx == 0:
            for t in range(16):
                S0[0, 4 + t, yd : yd + 4, :] = ib0[d, t, 0:4, :]
                S0[0, 20 + t, yd : yd + 4, :] = ib0[d, t, 4:8, :]
        elif dy != 0:
            for t in range(4):
                r = 4 * (t % 2)
                S0[0, (0 if dx == 1 else 36) + t, yd : yd + 4, :] = ib0[d, t // 2, r : r + 4, :]
    elh[:, 0:384] = dot3(
        r0, jnp.concatenate([S0[0, 0:4].reshape(192, 128), S0[0, 36:40].reshape(192, 128)], 0), True
    )
    fx = jnp.concatenate([S0[0, 4:36, 4:8, :], S0[0, 4:36, 40:44, :]], 1).reshape(256, 128)
    elh[:, 384:640] = dot3(r0, fx, True)
    eh[k] = elh[...]
    gh_start, gh_recv, gh_send = gather(3, elh, eh)
    gh_start()
    sends += [h_send, c_send, c2_send, g0_send, gh_send]

    c_recv()
    CG = cg[0:8].reshape(128, 128)
    CG2 = [None]
    ri, ci = iota((128, 128), 0), iota((128, 128), 1)
    same = (ri >> 1) == (ci >> 1)
    odd = (ci & 1) == 1
    eye = jnp.where(ri == ci, 1.0, 0.0).astype(f32)

    def col(c):
        src = CG2[0] if 2 <= c < 8 else CG
        return jnp.broadcast_to(src[:, c : c + 1], (128, 128))

    def corner(n):
        return jnp.where(same, jnp.where(odd, col(2 * n + 1), col(2 * n)), 0.0)

    lrow = (ri >> 1) & 7
    inva = jnp.zeros((128, 128), f32)
    for l in range(5):
        inva = jnp.where(lrow == l, 1.0 / a[l], inva)
    face = col(8)
    face_up = jnp.concatenate([face[16:], jnp.zeros((16, 128), f32)], 0)
    K = inva * (
        jnp.where(((ri & 1) == 0) & (ci == ri - 15), face, 0.0)
        + jnp.where(((ri & 1) == 1) & (ci == ri + 15), face_up, 0.0)
    )
    R = corner(0)
    blk = (ri >> 4) + (ri & 1)
    for st in (1, 2, 4):
        link = jnp.where((blk & (2 * st - 1)) == st, K, 0.0)
        d = R * eye
        drow = jnp.sum(d, 1, keepdims=True)
        dcol = jnp.sum(d, 0, keepdims=True)
        off = link / (1.0 - link * link * drow * dcol)
        diag = jnp.sum(off * link * dcol, 1, keepdims=True)
        R = R + hdot(hdot(R, off + eye * diag), R)
    W = eye + hdot(R, K)
    c2_recv()
    CG2[0] = cg2[...].reshape(128, 128)
    B2, B3, B4 = dot3(corner(1), K), dot3(corner(2), K), dot3(corner(3), K)
    V1 = dot3(W, dot3(B2, W))
    V2 = dot3(W, dot3(B3, W) + dot3(B2, V1))
    V3 = dot3(W, dot3(B4, W) + dot3(B3, V1) + dot3(B2, V2))
    VS = [W, V1, V2, V3]

    def lm_of(p):
        l = jnp.where(p < 12, (p >> 2) + 1, jnp.where(p < 14, 0, 4))
        m = jnp.where(p < 12, (p & 3) + 1, (p & 1) + 1)
        return l, m

    def funct(level):
        width = 64 if level == 0 else 256
        rr, rc = iota((128, 128), 0), iota((128, 128), 1)
        p, side = rr & 15, rr >> 4
        if level == 0:
            l, m = jnp.zeros_like(p), p - 11
            live = (rr < 32) & (p >= 12)
        else:
            l, m = lm_of(p)
            live = rr < 32
        target = jnp.where(side == 0, (k - 1) * 16 + l * 2 + 1, (k + 1) * 16 + l * 2)
        pick_rows = jnp.where(live & (rc == target), 1.0, 0.0).astype(f32)
        er, ec = iota((128, width), 0), iota((128, width), 1)
        if level == 0:
            jc, lc, mc, endc = ec >> 3, jnp.zeros_like(ec), ((ec >> 1) & 3) + 1, ec & 1
        else:
            jc, endc = ec >> 5, ec & 1
            lc, mc = lm_of((ec >> 1) & 15)
        expand = jnp.where(er == jc * 16 + lc * 2 + endc, 1.0, 0.0).astype(f32)
        wr = iota((128, width), 0)
        mrow = ((wr & 15) - 11) if level == 0 else lm_of(wr & 15)[1]
        out = jnp.zeros((128, width), f32)
        for n in range(4):
            x = dot3(dot3(pick_rows, VS[n]), expand)
            out = out + jnp.where(mrow - mc == n, x, 0.0)
        return out

    L0 = funct(0)

    side_in, side_out = ri >> 4, ci >> 4
    pi, po = ri & 15, ci & 15
    fl = (ri < 32) & (ci < 32) & (side_in == side_out)
    li, mi = lm_of(pi)
    lo, mo = lm_of(po)
    aout = jnp.zeros((128, 128), f32)
    for l in range(5):
        aout = jnp.where(lo == l, a[l], aout)
    cm = jnp.broadcast_to(zf_ref[0:1, 0:1], (1, 128))
    cp = jnp.broadcast_to(cg[k + 1, 0:1, 8:9], (1, 128))

    def matrices():
        for l in range(5):
            gt = g_ref[l].T
            p1 = pid(l, 1)
            ut = jnp.where(ri == p1, jnp.broadcast_to(cm * gt[0:1], (128, 128)), 0.0)
            ut = jnp.where(ri == 16 + p1, jnp.broadcast_to(cp * gt[127:128], (128, 128)), ut)
            if l == 0:
                q = jnp.where(fl & (pi >= 13) & (pi == po + 1), 1.0, 0.0)
            else:
                den = jnp.where(lo == l, 1.0, a[l] - aout)
                amp = a[l] / den
                nb = -aout / den
                p2 = nb * nb
                p3 = p2 * nb
                dm = mo - mi
                pw = jnp.where(dm == 0, 1.0, jnp.where(dm == 1, nb, jnp.where(dm == 2, p2, p3)))
                pm = jnp.where(mo == 1, nb, jnp.where(mo == 2, p2, jnp.where(mo == 3, p3, p2 * p2)))
                q = jnp.where((li == lo) & (dm >= 0), amp * pw, 0.0)
                q = q + jnp.where((li == l) & (mi == 1), pm, 0.0)
                q = jnp.where(lo == l, jnp.where((li == l) & (mi == mo + 1), 1.0, 0.0), q)
                q = jnp.where(fl, q, 0.0)
            for r, v in ((0, a[l] * gt), (128, ut)):
                vh, vl = split(v)
                th[l, r : r + 128, 0:128] = vh
                tl[l, r : r + 128, 0:128] = vl
            qh, ql = split(q.astype(f32))
            zero = jnp.zeros((128, 128), bf16)
            th[l, 0:128, 128:256] = zero
            tl[l, 0:128, 128:256] = zero
            th[l, 128:256, 128:256] = qh
            tl[l, 128:256, 128:256] = ql

    gt = a[0] * g_ref[0].T
    gh, gl = split(gt)
    ra[0:128, 0:128] = gh
    ra[128:256, 0:128] = gh
    ra[0:128, 128:256] = gl
    ra[128:256, 128:256] = jnp.zeros((128, 128), bf16)
    gt = g_ref[0].T
    for i in range(4):
        row = ri & 31
        u = jnp.where(row == 12 + i, jnp.broadcast_to(cm * gt[0:1], (128, 128)), 0.0)
        u = jnp.where(row == 28 + i, jnp.broadcast_to(cp * gt[127:128], (128, 128)), u)
        uh, ul = split(u)
        u = jnp.where(ri < 64, uh.astype(f32), jnp.where(ri < 96, ul.astype(f32), 0.0))
        ub[:, 128 * i : 128 * i + 128] = u.astype(bf16)

    def apply(l, src, dst, step, n, scale=None):
        y = src.shape[2]

        def body(i, c):
            x = pl.ds(i * step, step)
            v = jnp.concatenate(
                [src[0, x].reshape(step * y, 128), src[1, x].reshape(step * y, 128)], 1
            )
            vh, vl = split(v)
            t = mm(vh, th[l]) + (mm(vh, tl[l]) + mm(vl, th[l]))
            if scale is not None:
                t = scale * t
            dst[0, x] = t[:, 0:128].reshape(step, y, 128)
            dst[1, x] = t[:, 128:256].reshape(step, y, 128)
            return c

        lax.fori_loop(0, n, body, 0)

    def solve_block(src, dst):
        n, y = src.shape[1], src.shape[2]
        v = jnp.concatenate([src[0].reshape(n * y, 128), src[1].reshape(n * y, 128)], 1)
        vh, vl = split(v)
        t = mm(vh, jnp.concatenate([th[0, :, 0:128], tl[0, :, 0:128]], 1))
        t = t[:, 0:128] + (t[:, 128:256] + mm(vl, th[0, :, 0:128]))
        dst[0] = t.reshape(n, y, 128)

    def solves(src, dsts):
        n, y = src.shape[1], src.shape[2]
        v = jnp.concatenate([src[0].reshape(n * y, 128), src[1].reshape(n * y, 128)], 1)
        vh, vl = split(v)
        for dst, i, scale in dsts:
            t = mm(vh, th[i]) + (mm(vh, tl[i]) + mm(vl, th[i]))
            if scale is not None:
                t = scale * t
            dst[0] = t[:, 0:128].reshape(n, y, 128)
            dst[1] = t[:, 128:256].reshape(n, y, 128)

    def product(i, l1, l2):
        t = mm(th[l1], th[l2]) + (mm(th[l1], tl[l2]) + mm(tl[l1], th[l2]))
        h, lo_ = split(t)
        th[i] = h
        tl[i] = lo_

    def square(l):
        product(4 + l, l, l)

    def both(l):
        product(8 + l, l + 1, l)

    def stencil(l, src, dst, grow, post, halves=(0, 1)):
        ox, oy, n, y = OX[l], OY[l], LX[l], SY[l]
        gy0 = iota((y, 128), 0) + (iy * n - oy)
        ym = jnp.where((gy0 >= 0) & (gy0 < ngy * n), 0.25, 0.0).astype(f32)
        total = n + 2 * grow
        step = next(u for u in (4, 3, 2, 1) if total % u == 0)

        def body(i, c):
            x0 = ox - grow + i * step
            outs = []
            for h in halves:
                r = [src[h, x0 - 1 + j] for j in range(step + 2)]
                for j in range(step):
                    gx0 = ix * n + (x0 + j - ox)
                    s = jnp.where((gx0 >= 0) & (gx0 < ngx * n), 1.0, 0.0).astype(f32)
                    t = (r[j] + r[j + 2]) + (
                        pltpu.roll(r[j + 1], 1, 0) + pltpu.roll(r[j + 1], y - 1, 0)
                    )
                    outs.append((h, x0 + j, post(h, x0 + j, (ym * s) * t)))
            for o in outs:
                dst(*o)
            return c

        lax.fori_loop(0, total // step, body, 0)

    def into(ref):
        def put(h, x, v):
            ref[h, x] = v
        return put

    def solve(l, src, dst, matrix=None, scale=None):
        step, n = SX[l], 1
        apply(l if matrix is None else matrix, src, dst, step, n, scale)

    def residual(l, halves=(0, 1)):
        s, ta, tb = S[l], at("TA", l), at("TB", l)
        aa, bb = at("AA", l), at("BB", l)
        solves(s, [(ta, l, None), (tb, 4 + l, None)])
        stencil(l, tb, into(bb), 1, lambda h, x, v: 0.32 * ta[h, x] + 0.64 * v, halves)
        stencil(l, bb, into(aa), 0, lambda h, x, v: 0.04 * s[h, x] + v, halves)

    def smoothed(l):
        w = 0
        s, ta, tb, tc = S[l], at("TA", l), at("TB", l), at("TC", l)
        bb, cc, ma = at("BB", l), at("CC", l), at("MA", l)
        solve(l, tb, tc)
        stencil(l, tc, into(bb), 2 + w, lambda h, x, v: 0.8192 * tb[h, x] + 0.4096 * v)
        stencil(l, bb, into(cc), 1 + w, lambda h, x, v: 0.9728 * ta[h, x] + v)
        stencil(l, cc, into(ma), w, lambda h, x, v: 0.9984 * s[h, x] + v)

    def restrict(l, put, halves=(0, 1)):
        ox, oy, n = OX[l], OY[l], LX[l] // 2
        aa = at("AA", l)

        def body(i, c):
            x = ox + 2 * i
            for h in halves:
                even, off = pl.ds(oy, n, 2), pl.ds(oy + 1, n, 2)
                v = (aa[h, x, even, :] + aa[h, x, off, :]) + (
                    aa[h, x + 1, even, :] + aa[h, x + 1, off, :]
                )
                put(h, i, 0.25 * v)
            return c

        lax.fori_loop(0, n, body, 0)

    def prolong(l, fields, outs, halves):
        c = l + 1
        w = 1 if l == 0 else 0
        n, ox, oc, y = LX[c], OX[l], OX[c], SY[c]
        ys, cnt = [(0, 24), (2, 12), (2, 8), (2, 8)][l]
        gyc = iota((cnt, 128), 0) + (iy * n + ys - OY[c])
        ym = jnp.where((gyc >= 0) & (gyc < ngy * n), 1.0, 0.0).astype(f32)

        def body(j, carry):
            j = j - (1 + w)
            gx = ix * n + j
            s = jnp.where((gx >= 0) & (gx < ngx * n), 1.0, 0.0).astype(f32)
            ms = ym * s
            for h in halves:
                lower, here, upper = (fields(h, oc + j + i) for i in (-1, 0, 1))
                for (o, oh), lo_, he, up_ in zip(outs, lower, here, upper):
                    oh = h if oh is None else oh
                    for i, far in enumerate((lo_, up_)):
                        v = 0.75 * he + 0.25 * far
                        ev = (0.75 * v + 0.25 * pltpu.roll(v, 1, 0))[ys : ys + cnt]
                        od = (0.75 * v + 0.25 * pltpu.roll(v, y - 1, 0))[ys : ys + cnt]
                        o[oh, ox + 2 * j + i, pl.ds(0, cnt, 2), :] = ms * ev
                        o[oh, ox + 2 * j + i, pl.ds(1, cnt, 2), :] = ms * od
            return carry

        lax.fori_loop(0, n + 2 + 2 * w, body, 0)

    def correct(l, store):
        c = l + 1
        m, u, g2 = M[c], at("U", c), at("V", c)
        kap = a[l] / a[c]
        solves(m, [(u, c, kap), (g2, 8 + l, 0.64 * kap)])
        q = 0.04 * (1.0 - a[c] / a[l])
        outs = [at("P0", l), at("P1", l), at("P2", l)]

        def fields(h, x):
            uv = u[h, x]
            return (0.04 * m[h, x] + q * uv, 0.32 * uv, g2[h, x])

        prolong(l, fields, [(o, None) for o in outs], (0, 1))
        cc, ma = at("CC", l), at("MA", l)
        stencil(l, outs[2], into(cc), 1, lambda h, x, v: outs[1][h, x] + v)
        stencil(l, cc, store, 0, lambda h, x, v: (ma[h, x] + outs[0][h, x]) + v)

    def parts(et):
        phi = dot3(L0, et).T
        h, lo_ = split(phi)
        h, lo_ = h.astype(f32), lo_.astype(f32)
        return h + pltpu.roll(lo_, 32, 1) + pltpu.roll(h, 64, 1)

    def powers(first, src, d1, d2):
        for i in range(5):
            x = slice(8 * i, 8 * i + 8)
            w = S0[1, x].reshape(384, 128).astype(bf16)
            c = mm(w, ub[:, 128 * first : 128 * first + 256])
            vh, vl = split(src[0, x].reshape(384, 128))
            t = mm(jnp.concatenate([vh, vl], 1), ra[...])
            t = (t[:, 0:128] + t[:, 128:256]) + c[:, 0:128]
            d1[0, x] = t.reshape(8, 48, 128)
            vh, vl = split(t)
            t = mm(jnp.concatenate([vh, vl], 1), ra[...])
            t = (t[:, 0:128] + t[:, 128:256]) + c[:, 128:256]
            d2[0, x] = t.reshape(8, 48, 128)

    g0_recv()
    for i in range(4):
        w = parts(e0[:, :, 256 * i : 256 * i + 256].reshape(64, 256))
        S0[1, 4 + 8 * i : 12 + 8 * i, 8:40, :] = w.reshape(8, 32, 128)
    gh_recv()
    w = parts(eh[:, :, 0:384].reshape(64, 384))
    S0[1, 0:4] = w[0:192].reshape(4, 48, 128)
    S0[1, 36:40] = w[192:384].reshape(4, 48, 128)
    w = parts(eh[:, :, 384:640].reshape(64, 256)).reshape(32, 8, 128)
    S0[1, 4:36, 4:8, :] = w[:, 0:4]
    S0[1, 4:36, 40:44, :] = w[:, 4:8]

    t1, t2, t3, t4 = at("TA", 0), at("TB", 0), at("TC", 0), at("P0", 0)
    aa0, bb0, cc0, ma0 = at("AA", 0), at("BB", 0), at("CC", 0), at("MA", 0)
    powers(0, S0, t1, t2)
    stencil(0, t2, into(bb0), 1, lambda h, x, v: 0.32 * t1[h, x] + 0.64 * v, (0,))
    stencil(0, bb0, into(aa0), 0, lambda h, x, v: 0.04 * S0[h, x] + v, (0,))

    def put1(h, i, v):
        S1[h, 3 + i, 4:20, :] = v
    restrict(0, put1, (0,))
    el1[...] = dot3(re1[...], S1[0, 3:19, 4:20, :].reshape(256, 128), True)
    e1[k] = el1[...]
    g1_start, g1_recv, g1_send = gather(2, el1, e1)
    g1_start()
    x1_start, x1_finish, x1_send = packed(1, 1, "g1", S1, True, False)
    x1_start()

    L1 = funct(1)
    matrices()
    powers(2, t2, t3, t4)
    for l in (1, 2, 3):
        square(l)
    clear(r_["in_s2"])

    def both0(h, x, v):
        bb0[0, x] = 0.8192 * t3[0, x] + 0.4096 * v
        bb0[1, x] = 0.4096 * (t3[0, x] + v)

    g1_recv()
    phi = dot3(L1, e1[...].reshape(256, 256))
    S1[1, 3:19, 4:20, :] = phi.T.reshape(16, 16, 128)
    y1_start, y1_finish, y1_send = packed(2, 1, "f1", S1, False, True)
    y1_start()
    stencil(0, t4, both0, 3, lambda h, x, v: v, (0,))
    stencil(0, bb0, into(cc0), 2, lambda h, x, v: (0.1536 if h else 0.9728) * t2[0, x] + v)
    for r in (S3, S4, M3, M4):
        clear2(r)
    for name in ("s3", "s4", "m3", "m2", "m1"):
        clear(r_["in_" + name])
    x1_finish()
    y1_finish()
    residual(1)

    def put2(h, i, v):
        S2[h, 3 + i, 4:12, :] = v
    restrict(1, put2)
    x2_start, x2_finish, x2_send = packed(3, 2, "s2", S2)
    x2_start()
    smoothed(1)
    stencil(0, cc0, into(aa0), 1, lambda h, x, v: (0.0256 if h else 0.9984) * t1[0, x] + v)

    x2_finish()
    residual(2)

    def put3(h, i, v):
        S3[h, 4 + i, 4:8, :] = v
    restrict(2, put3)
    x3_start, x3_finish, x3_send = packed_block(4, 3, "s3", S3)
    x3_start()
    smoothed(2)
    stencil(0, aa0, into(ma0), 0, lambda h, x, v: 0.0016 * S0[0, x] + v, (1,))

    x3_finish()
    residual(3)

    def put4(h, i, v):
        S4[h, 4 + i, 4:6, :] = v
    restrict(3, put4)
    x4_start, x4_finish, x4_send = packed_block(5, 4, "s4", S4, FAR)
    x4_start()
    smoothed(3)
    for l in (3, 2, 1, 0):
        both(l)

    x4_finish()
    ta4 = at("TA", 4)
    solve(4, S4, ta4)

    stencil(4, ta4, into(M4), 2, lambda h, x, v: 0.96 * S4[h, x] + 0.64 * v)

    def putm3(h, x, v):
        M3[h, x, 4:8, :] = v[4:8]
    correct(3, putm3)
    z3_start, z3_finish, z3_send = packed_block(7, 3, "m3", M3)
    z3_start()
    z3_finish()

    def putm2(h, x, v):
        M2[h, x, 4:12, :] = v[4:12]
    correct(2, putm2)
    z2_start, z2_finish, z2_send = packed(8, 2, "m2", M2)
    z2_start()
    z2_finish()

    def putm1(h, x, v):
        M1[h, x, 4:20, :] = v[4:20]
    correct(1, putm1)
    z1_start, z1_finish, z1_send = packed(9, 1, "m1", M1)
    z1_start()
    z1_finish()

    u, g2 = at("U", 1), at("V", 1)
    kap = a[0] / a[1]
    solves(M1, [(u, 1, kap), (g2, 8, 0.64 * kap)])
    solve_block(M1, HM)
    solve_block(g2, H2)
    q = 0.04 * (1.0 - a[1] / a[0])

    def fields0(h, x):
        uv, gv = u[0, x], g2[0, x]
        h0 = 0.04 * HM[0, x] + (q / 0.64) * gv
        return (0.04 * M1[0, x] + q * uv, h0 - 0.32 * uv, 0.5 * gv, H2[0, x], h0)

    P0, P1, P2 = at("P0", 0), at("P1", 0), at("P2", 0)
    prolong(0, fields0, [(P0, 0), (P0, 1), (P1, 0), (P1, 1), (P2, 0)], (0,))

    def pair(h, x, v):
        bb0[0, x] = v - P1[0, x]
        bb0[1, x] = v + P1[0, x]
    stencil(0, P1, pair, 2, lambda h, x, v: v, (1,))
    stencil(0, bb0, into(cc0), 1, lambda h, x, v: P0[1, x] + v, (0,))
    inv0 = 1.0 / a[0]

    def put_sol(h, x, v):
        sol_ref[x - 4] = v[8:40]

    def put_res(h, x, v):
        res_ref[x - 4] = v[8:40]
    stencil(0, bb0, put_sol, 0, lambda h, x, v: inv0 * ((aa0[0, x] + P2[0, x]) + v), (1,))
    stencil(0, cc0, put_res, 0, lambda h, x, v: (ma0[1, x] - P0[0, x]) + v, (0,))

    for wait in sends + [
        x1_send, g1_send, y1_send, x2_send, x3_send, x4_send, z3_send, z2_send, z1_send
    ]:
        wait()


def body(sizes, right_side, z_faces, xy_coupling, block_inverse):
    n = right_side.shape
    vmem = pl.BlockSpec(memory_space=pltpu.VMEM)
    hbm = pl.BlockSpec(memory_space=pl.ANY)
    scratch = [pltpu.VMEM(s, f32) for s in scratch_shapes().values()]
    scratch += [pltpu.VMEM((5, 128, 128), f32)]
    scratch += [pltpu.VMEM((12, 256, 256), bf16), pltpu.VMEM((12, 256, 256), bf16)]
    scratch += [pltpu.VMEM((256, 256), bf16), pltpu.VMEM((128, 512), bf16)]
    scratch += [pltpu.SemaphoreType.DMA((10, 20)), pltpu.SemaphoreType.DMA((10, 20))]
    scratch += [pltpu.SemaphoreType.DMA((5, 8)), pltpu.SemaphoreType.DMA((5, 8))]
    scratch += [pltpu.SemaphoreType.DMA((4,)), pltpu.VMEM((1, 128), f32), pltpu.SMEM((5,), f32)]
    return pl.pallas_call(
        lambda *r: kernel(sizes, *r),
        out_shape=(pltpu.VMEM(n, f32), pltpu.VMEM(n, f32)),
        in_specs=[hbm, hbm, hbm, hbm],
        out_specs=(vmem, vmem),
        scratch_shapes=scratch,
        compiler_params=pltpu.CompilerParams(
            collective_id=0, has_side_effects=True, vmem_limit_bytes=60 * 2**20
        ),
        name="vcycle",
    )(right_side, z_faces.reshape(1, -1), block_inverse, xy_coupling)


def solution(mesh):
    sizes = tuple(mesh.shape[n] for n in ("gx", "gy", "gz"))
    return jax.shard_map(
        lambda *args: body(sizes, *args),
        mesh=mesh,
        in_specs=(P("gx", "gy", "gz"), P("gz"), P(), P(None, "gz", None)),
        out_specs=(P("gx", "gy", "gz"), P("gx", "gy", "gz")),
        check_vma=False,
    )
```

```python
import jax
import jax.numpy as jnp
from jax import lax
from jax.experimental import pallas as pl
from jax.experimental.pallas import tpu as pltpu
from jax.sharding import PartitionSpec as P

f32 = jnp.float32
bf16 = jnp.bfloat16
HI = lax.Precision.HIGHEST
MESH = pl.DeviceIdType.MESH
FAR = [(dx, dy) for dx in (-2, -1, 0, 1, 2) for dy in (-2, -1, 0, 1, 2) if 0 < abs(dx) + abs(dy) < 4]
DIRS = [(dx, dy) for dx in (-1, 0, 1) for dy in (-1, 0, 1) if (dx, dy) != (0, 0)]

LX = [32, 16, 8, 4, 2]
OX = [4, 3, 3, 4, 4]
OY = [8, 4, 4, 4, 4]
SX = [40, 22, 14, 12, 10]
SY = [48, 24, 16, 16, 16]


def pair_of(p):
    if p < 12:
        return p // 4 + 1, p % 4 + 1
    return (0 if p < 14 else 4), p % 2 + 1


def pid(l, m):
    if l == 0:
        return 11 + m
    if l == 4:
        return 13 + m
    return (l - 1) * 4 + m - 1


def split(x):
    h = x.astype(bf16)
    return h, (x - h.astype(f32)).astype(bf16)


def mm(a, b, trans_b=False):
    dims = (((1,), (1 if trans_b else 0,)), ((), ()))
    return lax.dot_general(a, b, dims, preferred_element_type=f32)


def dot3(a, b, trans_b=False):
    ah, al = split(a)
    bh, bl = split(b)
    return mm(ah, bh, trans_b) + (mm(ah, bl, trans_b) + mm(al, bh, trans_b))


def hdot(a, b):
    return jnp.dot(a, b, precision=HI, preferred_element_type=f32)


def iota(shape, dim):
    return lax.broadcasted_iota(jnp.int32, shape, dim)


MESSAGES = {"f0": 16, "g1": 8, "f1": 2, "s2": 5, "s3": 3, "s4": 1, "m3": 3, "m2": 5, "m1": 10}


def scratch_shapes():
    out = {}
    for l in range(5):
        out[f"S{l}"] = (2, SX[l], SY[l], 128)
        for t in ("TA", "TB", "TC", "AA", "BB", "CC", "MA", "P0", "P1", "P2"):
            out[f"{t}{l}"] = (2, SX[l], SY[l], 128)
        if l:
            for t in ("M", "U", "V"):
                out[f"{t}{l}"] = (2, SX[l], SY[l], 128)
    out["HM"] = out["H2"] = (2, SX[1], SY[1], 128)
    for name, tiles in MESSAGES.items():
        out["out_" + name] = out["in_" + name] = (len(FAR) if name == "s4" else 8, tiles, 8, 128)
    out["rows"] = (4, 16, 128)
    out["re0"] = (8, 128)
    out["re1"] = (32, 128)
    out["cg"] = (9, 16, 128)
    out["cgl"] = out["cgl2"] = (16, 128)
    out["cg2"] = (8, 16, 128)
    out["e0"] = (8, 8, 1024)
    out["eh"] = (8, 8, 640)
    out["e1"] = (8, 32, 256)
    out["el0"] = (8, 1024)
    out["elh"] = (8, 640)
    out["el1"] = (32, 256)
    return out


def kernel(sizes, f_ref, zf_in, ginv_ref, e_in, sol_ref, res_ref, *refs):
    names = list(scratch_shapes())
    r_ = dict(zip(names, refs))
    g_ref, th, tl, ra, ub, hs, hr, gs, gr, ls, zf_ref, e_ref = refs[len(names):]
    S0, S1, S2, S3, S4 = [r_[f"S{l}"] for l in range(5)]
    M1, M2, M3, M4 = [r_[f"M{l}"] for l in range(1, 5)]
    rows, re0, re1, cg, cgl = r_["rows"], r_["re0"], r_["re1"], r_["cg"], r_["cgl"]
    e0, e1, el0, el1 = r_["e0"], r_["e1"], r_["el0"], r_["el1"]
    eh, elh, HM, H2 = r_["eh"], r_["elh"], r_["HM"], r_["H2"]
    cg2, cgl2 = r_["cg2"], r_["cgl2"]

    ngx, ngy, ngz = sizes
    ix, iy, k = lax.axis_index("gx"), lax.axis_index("gy"), lax.axis_index("gz")
    S = [S0, S1, S2, S3, S4]
    M = [None, M1, M2, M3, M4]

    def at(name, l):
        return r_[f"{name}{l}"]


    def peer(o):
        return jnp.where(k + o >= ngz, k + o - ngz, k + o)

    def exists(dx, dy):
        x, y = ix + dx, iy + dy
        return (x >= 0) & (x < ngx) & (y >= 0) & (y < ngy)

    def clear(ref):
        def step(i, c):
            ref[i] = jnp.zeros(ref.shape[1:], f32)
            return c
        lax.fori_loop(0, ref.shape[0], step, 0)

    def clear2(ref):
        def step(i, c):
            for h in range(2):
                ref[h, i] = jnp.zeros(ref.shape[2:], f32)
            return c
        lax.fori_loop(0, ref.shape[1], step, 0)

    load_f = pltpu.make_async_copy(f_ref, S0.at[0, 4:36, 8:40, :], ls.at[0])
    load_g = pltpu.make_async_copy(ginv_ref, g_ref, ls.at[1])
    load_z = pltpu.make_async_copy(zf_in, zf_ref, ls.at[2])
    load_e = pltpu.make_async_copy(e_in, e_ref, ls.at[3])
    for load in (load_e, load_z, load_g, load_f):
        load.start()

    barrier = pltpu.get_barrier_semaphore()
    count = jnp.int32(ngz - 1)
    for dx, dy in FAR:
        ok = exists(dx, dy)

        @pl.when(ok)
        def _():
            pl.semaphore_signal(
                barrier, inc=1, device_id=(ix + dx, iy + dy, k), device_id_type=MESH
            )

        count = count + jnp.where(ok, 1, 0)
    for o in range(1, ngz):
        pl.semaphore_signal(
            barrier, inc=1, device_id=(ix, iy, peer(o)), device_id_type=MESH
        )

    for d, (dx, dy) in enumerate(DIRS):
        @pl.when(jnp.logical_not(exists(-dx, -dy)))
        def _():
            for name in ("f0", "g1", "f1"):
                r = r_["in_" + name]
                for t in range(MESSAGES[name]):
                    r[d, t] = jnp.zeros((8, 128), f32)
            if dy == 0:
                for i in range(4):
                    S0[0, (0 if dx == 1 else 36) + i, 8:40, :] = jnp.zeros((32, 128), f32)

    def sides(i, c):
        S0[0, i, 0:8, :] = jnp.zeros((8, 128), f32)
        S0[0, i, 40:48, :] = jnp.zeros((8, 128), f32)
        return c
    lax.fori_loop(0, 40, sides, 0)
    clear(rows)
    if ngz < 8:
        for r in (e0, eh, e1, cg2):
            clear(r)
    cg[8] = jnp.zeros((16, 128), f32)

    def exchange(phase, pick, dirs=DIRS):
        def copy(d, dx, dy):
            src, dst = pick(dx, dy)
            return pltpu.make_async_remote_copy(
                src_ref=src, dst_ref=dst, send_sem=hs.at[phase, d], recv_sem=hr.at[phase, d],
                device_id=(ix + dx, iy + dy, k), device_id_type=MESH,
            )

        def start():
            for d, (dx, dy) in sorted(enumerate(dirs), key=lambda i: -abs(i[1][0]) - abs(i[1][1])):
                @pl.when(exists(dx, dy))
                def _():
                    copy(d, dx, dy).start()

        def wait_recv():
            for d, (dx, dy) in enumerate(dirs):
                @pl.when(exists(-dx, -dy))
                def _():
                    copy(d, dx, dy).wait_recv()

        def wait_send():
            for d, (dx, dy) in enumerate(dirs):
                @pl.when(exists(dx, dy))
                def _():
                    copy(d, dx, dy).wait_send()

        return start, wait_recv, wait_send

    def span(d, off, n, h):
        if d == 0:
            return pl.ds(off, n), pl.ds(off, n)
        if d == 1:
            return pl.ds(off + n - h, h), pl.ds(off - h, h)
        return pl.ds(off, h), pl.ds(off + n, h)

    def lanes_of(planes):
        out = planes[0]
        for i, v in enumerate(planes[1:]):
            out = out + pltpu.roll(v, 32 * (i + 1), 1)
        return out

    low_lanes = {r: iota((r, 128), 1) < 32 for r in (8,)}

    def lanes_back(tile, i):
        v = tile if i == 0 else pltpu.roll(tile, 128 - 32 * i, 1)
        return jnp.where(low_lanes[8], v, 0.0)

    def tiles_of(l, dx, dy, wf, wp):
        n = LX[l]
        if dx == 0:
            return (n // 2 if wf else 0) + ((n + 7) // 8 if wp else 0)
        if dy == 0:
            return (3 * n // 8 if wf else 0) + (n // 8 if wp else 0)
        return 2 if wf else 1

    def packed(phase, l, name, buf, wf=True, wp=True):
        n, ox, oy = LX[l], OX[l], OY[l]
        ob, ib = r_["out_" + name], r_["in_" + name]

        def pick(dx, dy):
            d, t = DIRS.index((dx, dy)), tiles_of(l, dx, dy, wf, wp)
            return ob.at[d, 0:t], ib.at[d, 0:t]

        start0, wait_recv, wait_send = exchange(phase, pick)

        def start():
            for d, (dx, dy) in enumerate(DIRS):
                xs = ox + n - 3 if dx == 1 else ox
                ys = oy + n - 4 if dy == 1 else oy
                yt = ys // 8 * 8
                part = slice(ys - yt, ys - yt + 4)
                if dx == 0:
                    base = n // 2 if wf else 0
                    if wf:
                        for t in range(n // 2):
                            ob[d, t, 0:4, :] = buf[0, ox + t, ys : ys + 4, :]
                            ob[d, t, 4:8, :] = buf[0, ox + t + n // 2, ys : ys + 4, :]
                    if wp:
                        for b in range(n // 4):
                            v = lanes_of([buf[1, ox + 4 * b + i, yt : yt + 8, :] for i in range(4)])
                            r = 4 * (b % 2)
                            ob[d, base + b // 2, r : r + 4, :] = v[part]
                elif dy == 0:
                    m = n // 8
                    base = 3 * m if wf else 0
                    for r in range(m):
                        y = slice(oy + 8 * r, oy + 8 * r + 8)
                        if wf:
                            for i in range(3):
                                ob[d, i * m + r] = buf[0, xs + i, y, :]
                        if wp:
                            ob[d, base + r] = lanes_of([buf[1, xs + i, y, :] for i in range(3)])
                else:
                    if wf:
                        ob[d, 0, 0:4, :] = buf[0, xs, ys : ys + 4, :]
                        ob[d, 0, 4:8, :] = buf[0, xs + 1, ys : ys + 4, :]
                        ob[d, 1, 0:4, :] = buf[0, xs + 2, ys : ys + 4, :]
                    if wp:
                        v = lanes_of([buf[1, xs + i, yt : yt + 8, :] for i in range(3)])
                        ob[d, 1 if wf else 0, 4:8, :] = v[part]
            start0()

        def finish():
            wait_recv()
            for d, (dx, dy) in enumerate(DIRS):
                xd = ox - 3 if dx == 1 else ox + n
                yd = oy - 4 if dy == 1 else oy + n
                if dx == 0:
                    base = n // 2 if wf else 0
                    if wf:
                        for t in range(n // 2):
                            buf[0, ox + t, yd : yd + 4, :] = ib[d, t, 0:4, :]
                            buf[0, ox + t + n // 2, yd : yd + 4, :] = ib[d, t, 4:8, :]
                    if wp:
                        for b in range(n // 4):
                            tile, r = ib[d, base + b // 2], 4 * (b % 2)
                            for i in range(4):
                                v = lanes_back(tile, i)
                                buf[1, ox + 4 * b + i, yd : yd + 4, :] = v[r : r + 4]
                elif dy == 0:
                    m = n // 8
                    base = 3 * m if wf else 0
                    for r in range(m):
                        y = slice(oy + 8 * r, oy + 8 * r + 8)
                        for i in range(3):
                            if wf:
                                buf[0, xd + i, y, :] = ib[d, i * m + r]
                            if wp:
                                buf[1, xd + i, y, :] = lanes_back(ib[d, base + r], i)
                else:
                    if wf:
                        buf[0, xd, yd : yd + 4, :] = ib[d, 0, 0:4, :]
                        buf[0, xd + 1, yd : yd + 4, :] = ib[d, 0, 4:8, :]
                        buf[0, xd + 2, yd : yd + 4, :] = ib[d, 1, 0:4, :]
                    if wp:
                        tile = ib[d, 1 if wf else 0]
                        for i in range(3):
                            buf[1, xd + i, yd : yd + 4, :] = lanes_back(tile, i)[4:8]

        return start, finish, wait_send

    def packed_block(phase, l, name, buf, dirs=DIRS):
        n = LX[l]
        ob, ib = r_["out_" + name], r_["in_" + name]

        def pick(dx, dy):
            return ob.at[0], ib.at[dirs.index((dx, dy))]

        start0, wait_recv, wait_send = exchange(phase, pick, dirs)

        def start():
            phi = lanes_of([buf[1, 4 + i, 0:8, :] for i in range(n)])
            if n == 4:
                for i in range(4):
                    r = 4 * (i // 2)
                    ob[0, i % 2, r : r + 4, :] = buf[0, 4 + i, 4:8, :]
                ob[0, 2] = phi
            else:
                ob[0, 0, 0:2, :] = buf[0, 4, 4:6, :]
                ob[0, 0, 2:4, :] = buf[0, 5, 4:6, :]
                ob[0, 0, 4:8, :] = phi[4:8]
            start0()

        def finish():
            wait_recv()
            for d, (dx, dy) in enumerate(dirs):
                xd, yd = 4 - n * dx, 4 - n * dy
                tile = ib[d, 2 if n == 4 else 0]
                for i in range(n):
                    v = lanes_back(tile, i)
                    buf[1, xd + i, yd : yd + n, :] = v[4 : 4 + n]
                    if n == 4:
                        r = 4 * (i // 2)
                        buf[0, xd + i, yd : yd + 4, :] = ib[d, i % 2, r : r + 4, :]
                    else:
                        buf[0, xd + i, yd : yd + 2, :] = tile[2 * i : 2 * i + 2]

        return start, finish, wait_send

    def gather(phase, src, buf):
        def copy(o):
            return pltpu.make_async_remote_copy(
                src_ref=src, dst_ref=buf.at[k], send_sem=gs.at[phase, o],
                recv_sem=gr.at[phase, o], device_id=(ix, iy, peer(o)),
                device_id_type=MESH,
            )

        def start():
            for o in range(1, ngz):
                copy(o).start()

        def wait_recv():
            for o in range(1, ngz):
                copy(o).wait_recv()

        def wait_send():
            for o in range(1, ngz):
                copy(o).wait_send()

        return start, wait_recv, wait_send

    sends = []
    ob0, ib0 = r_["out_f0"], r_["in_f0"]

    def pick0(dx, dy):
        d = DIRS.index((dx, dy))
        if dy == 0:
            sx, tx = span(dx, 4, 32, 4)
            return S0.at[0, sx, 8:40, :], S0.at[0, tx, 8:40, :]
        t = 16 if dx == 0 else 2
        return ob0.at[d, 0:t], ib0.at[d, 0:t]

    def ends0(dx):
        return 32 if dx == 1 else 4

    load_e.wait()
    a = [4.0 * e_ref[l] for l in range(5)]
    lane16 = iota((16, 128), 1)

    def corner_tile(first, last, tile):
        for n in range(first, last):
            rn = rows[n]
            tile = jnp.where(lane16 == 2 * n, jnp.broadcast_to(rn[:, 0:1], (16, 128)), tile)
            tile = jnp.where(lane16 == 2 * n + 1, jnp.broadcast_to(rn[:, 127:128], (16, 128)), tile)
        return tile

    load_z.wait()
    load_g.wait()
    for l in range(5):
        rows[0, 2 * l : 2 * l + 1, :] = a[l] * g_ref[l, 0:1, :]
        rows[0, 2 * l + 1 : 2 * l + 2, :] = a[l] * g_ref[l, 127:128, :]
    tile = corner_tile(
        0, 1, jnp.where(lane16 == 8, jnp.broadcast_to(zf_ref[0:1, 0:1], (16, 128)), 0.0)
    )
    cgl[...] = tile
    cg[k] = tile
    load_f.wait()
    for d, (dx, dy) in enumerate(DIRS):
        ys = 36 if dy == 1 else 8
        if dy != 0 and dx == 0:
            for t in range(16):
                ob0[d, t, 0:4, :] = S0[0, 4 + t, ys : ys + 4, :]
                ob0[d, t, 4:8, :] = S0[0, 20 + t, ys : ys + 4, :]
        elif dy != 0:
            for t in range(4):
                r = 4 * (t % 2)
                ob0[d, t // 2, r : r + 4, :] = S0[0, ends0(dx) + t, ys : ys + 4, :]

    pl.semaphore_wait(barrier, count)
    h_start, h_recv, h_send = exchange(0, pick0)
    h_start()
    c_start, c_recv, c_send = gather(0, cgl, cg)
    c_start()

    for m in range(4):
        if m > 0:
            prev = rows[m - 1]
            for l in range(5):
                nxt = a[l] * hdot(prev, g_ref[l])
                rows[m, 2 * l : 2 * l + 2, :] = nxt[2 * l : 2 * l + 2]
        re0[2 * m : 2 * m + 2, :] = rows[m, 0:2, :]
    tile = corner_tile(1, 4, jnp.zeros((16, 128), f32))
    cgl2[...] = tile
    cg2[k] = tile
    c2_start, c2_recv, c2_send = gather(4, cgl2, cg2)
    c2_start()

    r0 = re0[...]
    for i in range(4):
        fx = S0[0, 4 + 8 * i : 12 + 8 * i, 8:40, :].reshape(256, 128)
        el0[:, 256 * i : 256 * i + 256] = dot3(r0, fx, True)
    e0[k] = el0[...]
    g0_start, g0_recv, g0_send = gather(1, el0, e0)
    g0_start()
    for p in range(16):
        l, m = pair_of(p)
        re1[2 * p : 2 * p + 2, :] = rows[m - 1, 2 * l : 2 * l + 2, :]
    def side_phi(i, c):
        S0[1, 4 + i, 0:8, :] = jnp.zeros((8, 128), f32)
        S0[1, 4 + i, 40:48, :] = jnp.zeros((8, 128), f32)
        return c
    lax.fori_loop(0, 32, side_phi, 0)

    h_recv()
    for d, (dx, dy) in enumerate(DIRS):
        yd = 4 if dy == 1 else 40
        if dy != 0 and dx == 0:
            for t in range(16):
                S0[0, 4 + t, yd : yd + 4, :] = ib0[d, t, 0:4, :]
                S0[0, 20 + t, yd : yd + 4, :] = ib0[d, t, 4:8, :]
        elif dy != 0:
            for t in range(4):
                r = 4 * (t % 2)
                S0[0, (0 if dx == 1 else 36) + t, yd : yd + 4, :] = ib0[d, t // 2, r : r + 4, :]
    elh[:, 0:384] = dot3(
        r0, jnp.concatenate([S0[0, 0:4].reshape(192, 128), S0[0, 36:40].reshape(192, 128)], 0), True
    )
    fx = jnp.concatenate([S0[0, 4:36, 4:8, :], S0[0, 4:36, 40:44, :]], 1).reshape(256, 128)
    elh[:, 384:640] = dot3(r0, fx, True)
    eh[k] = elh[...]
    gh_start, gh_recv, gh_send = gather(3, elh, eh)
    gh_start()
    sends += [h_send, c_send, c2_send, g0_send, gh_send]

    c_recv()
    CG = cg[0:8].reshape(128, 128)
    CG2 = [None]
    ri, ci = iota((128, 128), 0), iota((128, 128), 1)
    same = (ri >> 1) == (ci >> 1)
    odd = (ci & 1) == 1
    eye = jnp.where(ri == ci, 1.0, 0.0).astype(f32)

    def col(c):
        src = CG2[0] if 2 <= c < 8 else CG
        return jnp.broadcast_to(src[:, c : c + 1], (128, 128))

    def corner(n):
        return jnp.where(same, jnp.where(odd, col(2 * n + 1), col(2 * n)), 0.0)

    lrow = (ri >> 1) & 7
    inva = jnp.zeros((128, 128), f32)
    for l in range(5):
        inva = jnp.where(lrow == l, 1.0 / a[l], inva)
    face = col(8)
    face_up = jnp.concatenate([face[16:], jnp.zeros((16, 128), f32)], 0)
    K = inva * (
        jnp.where(((ri & 1) == 0) & (ci == ri - 15), face, 0.0)
        + jnp.where(((ri & 1) == 1) & (ci == ri + 15), face_up, 0.0)
    )
    R = corner(0)
    blk = (ri >> 4) + (ri & 1)
    for st in (1, 2, 4):
        link = jnp.where((blk & (2 * st - 1)) == st, K, 0.0)
        d = R * eye
        drow = jnp.sum(d, 1, keepdims=True)
        dcol = jnp.sum(d, 0, keepdims=True)
        off = link / (1.0 - link * link * drow * dcol)
        diag = jnp.sum(off * link * dcol, 1, keepdims=True)
        R = R + hdot(hdot(R, off + eye * diag), R)
    W = eye + hdot(R, K)
    c2_recv()
    CG2[0] = cg2[...].reshape(128, 128)
    B2, B3, B4 = dot3(corner(1), K), dot3(corner(2), K), dot3(corner(3), K)
    V1 = dot3(W, dot3(B2, W))
    V2 = dot3(W, dot3(B3, W) + dot3(B2, V1))
    V3 = dot3(W, dot3(B4, W) + dot3(B3, V1) + dot3(B2, V2))
    VS = [W, V1, V2, V3]

    def lm_of(p):
        l = jnp.where(p < 12, (p >> 2) + 1, jnp.where(p < 14, 0, 4))
        m = jnp.where(p < 12, (p & 3) + 1, (p & 1) + 1)
        return l, m

    def funct(level):
        width = 64 if level == 0 else 256
        rr, rc = iota((128, 128), 0), iota((128, 128), 1)
        p, side = rr & 15, rr >> 4
        if level == 0:
            l, m = jnp.zeros_like(p), p - 11
            live = (rr < 32) & (p >= 12)
        else:
            l, m = lm_of(p)
            live = rr < 32
        target = jnp.where(side == 0, (k - 1) * 16 + l * 2 + 1, (k + 1) * 16 + l * 2)
        pick_rows = jnp.where(live & (rc == target), 1.0, 0.0).astype(f32)
        er, ec = iota((128, width), 0), iota((128, width), 1)
        if level == 0:
            jc, lc, mc, endc = ec >> 3, jnp.zeros_like(ec), ((ec >> 1) & 3) + 1, ec & 1
        else:
            jc, endc = ec >> 5, ec & 1
            lc, mc = lm_of((ec >> 1) & 15)
        expand = jnp.where(er == jc * 16 + lc * 2 + endc, 1.0, 0.0).astype(f32)
        wr = iota((128, width), 0)
        mrow = ((wr & 15) - 11) if level == 0 else lm_of(wr & 15)[1]
        out = jnp.zeros((128, width), f32)
        pb, eb = pick_rows.astype(bf16), expand.astype(bf16)
        vh, vl = split(jnp.concatenate(VS, 1))
        y = mm(pb, vh) + mm(pb, vl)
        yh, yl = split(jnp.concatenate([y[:, 128 * n : 128 * n + 128] for n in range(4)], 0))
        x = mm(yh, eb) + mm(yl, eb)
        for n in range(4):
            out = out + jnp.where(mrow - mc == n, x[128 * n : 128 * n + 128], 0.0)
        return out

    L0 = funct(0)

    side_in, side_out = ri >> 4, ci >> 4
    pi, po = ri & 15, ci & 15
    fl = (ri < 32) & (ci < 32) & (side_in == side_out)
    li, mi = lm_of(pi)
    lo, mo = lm_of(po)
    aout = jnp.zeros((128, 128), f32)
    for l in range(5):
        aout = jnp.where(lo == l, a[l], aout)
    cm = jnp.broadcast_to(zf_ref[0:1, 0:1], (1, 128))
    cp = jnp.broadcast_to(cg[k + 1, 0:1, 8:9], (1, 128))

    def matrices():
        for l in range(5):
            gt = g_ref[l].T
            p1 = pid(l, 1)
            ut = jnp.where(ri == p1, jnp.broadcast_to(cm * gt[0:1], (128, 128)), 0.0)
            ut = jnp.where(ri == 16 + p1, jnp.broadcast_to(cp * gt[127:128], (128, 128)), ut)
            if l == 0:
                q = jnp.where(fl & (pi >= 13) & (pi == po + 1), 1.0, 0.0)
            else:
                den = jnp.where(lo == l, 1.0, a[l] - aout)
                amp = a[l] / den
                nb = -aout / den
                p2 = nb * nb
                p3 = p2 * nb
                dm = mo - mi
                pw = jnp.where(dm == 0, 1.0, jnp.where(dm == 1, nb, jnp.where(dm == 2, p2, p3)))
                pm = jnp.where(mo == 1, nb, jnp.where(mo == 2, p2, jnp.where(mo == 3, p3, p2 * p2)))
                q = jnp.where((li == lo) & (dm >= 0), amp * pw, 0.0)
                q = q + jnp.where((li == l) & (mi == 1), pm, 0.0)
                q = jnp.where(lo == l, jnp.where((li == l) & (mi == mo + 1), 1.0, 0.0), q)
                q = jnp.where(fl, q, 0.0)
            for r, v in ((0, a[l] * gt), (128, ut)):
                vh, vl = split(v)
                th[l, r : r + 128, 0:128] = vh
                tl[l, r : r + 128, 0:128] = vl
            qh, ql = split(q.astype(f32))
            zero = jnp.zeros((128, 128), bf16)
            th[l, 0:128, 128:256] = zero
            tl[l, 0:128, 128:256] = zero
            th[l, 128:256, 128:256] = qh
            tl[l, 128:256, 128:256] = ql

    gt = a[0] * g_ref[0].T
    gh, gl = split(gt)
    ra[0:128, 0:128] = gh
    ra[128:256, 0:128] = gh
    ra[0:128, 128:256] = gl
    ra[128:256, 128:256] = jnp.zeros((128, 128), bf16)
    gt = g_ref[0].T
    for i in range(4):
        row = ri & 31
        u = jnp.where(row == 12 + i, jnp.broadcast_to(cm * gt[0:1], (128, 128)), 0.0)
        u = jnp.where(row == 28 + i, jnp.broadcast_to(cp * gt[127:128], (128, 128)), u)
        uh, ul = split(u)
        u = jnp.where(ri < 64, uh.astype(f32), jnp.where(ri < 96, ul.astype(f32), 0.0))
        ub[:, 128 * i : 128 * i + 128] = u.astype(bf16)

    def apply(l, src, dst, step, n, scale=None):
        y = src.shape[2]

        def body(i, c):
            x = pl.ds(i * step, step)
            v = jnp.concatenate(
                [src[0, x].reshape(step * y, 128), src[1, x].reshape(step * y, 128)], 1
            )
            vh, vl = split(v)
            t = mm(vh, th[l]) + (mm(vh, tl[l]) + mm(vl, th[l]))
            if scale is not None:
                t = scale * t
            dst[0, x] = t[:, 0:128].reshape(step, y, 128)
            dst[1, x] = t[:, 128:256].reshape(step, y, 128)
            return c

        lax.fori_loop(0, n, body, 0)

    def solve_block(src, dst):
        n, y = src.shape[1], src.shape[2]
        v = jnp.concatenate([src[0].reshape(n * y, 128), src[1].reshape(n * y, 128)], 1)
        vh, vl = split(v)
        t = mm(vh, jnp.concatenate([th[0, :, 0:128], tl[0, :, 0:128]], 1))
        t = t[:, 0:128] + (t[:, 128:256] + mm(vl, th[0, :, 0:128]))
        dst[0] = t.reshape(n, y, 128)

    def solves(src, dsts):
        n, y = src.shape[1], src.shape[2]
        v = jnp.concatenate([src[0].reshape(n * y, 128), src[1].reshape(n * y, 128)], 1)
        vh, vl = split(v)
        for dst, i, scale in dsts:
            t = mm(vh, th[i]) + (mm(vh, tl[i]) + mm(vl, th[i]))
            if scale is not None:
                t = scale * t
            dst[0] = t[:, 0:128].reshape(n, y, 128)
            dst[1] = t[:, 128:256].reshape(n, y, 128)

    def product(i, l1, l2):
        t = mm(th[l1], th[l2]) + (mm(th[l1], tl[l2]) + mm(tl[l1], th[l2]))
        h, lo_ = split(t)
        th[i] = h
        tl[i] = lo_

    def square(l):
        product(4 + l, l, l)

    def both(l):
        product(8 + l, l + 1, l)

    def stencil(l, src, dst, grow, post, halves=(0, 1)):
        ox, oy, n, y = OX[l], OY[l], LX[l], SY[l]
        gy0 = iota((y, 128), 0) + (iy * n - oy)
        ym = jnp.where((gy0 >= 0) & (gy0 < ngy * n), 0.25, 0.0).astype(f32)
        total = n + 2 * grow
        step = next(u for u in (4, 3, 2, 1) if total % u == 0)

        def body(i, c):
            x0 = ox - grow + i * step
            outs = []
            for h in halves:
                r = [src[h, x0 - 1 + j] for j in range(step + 2)]
                for j in range(step):
                    gx0 = ix * n + (x0 + j - ox)
                    s = jnp.where((gx0 >= 0) & (gx0 < ngx * n), 1.0, 0.0).astype(f32)
                    t = (r[j] + r[j + 2]) + (
                        pltpu.roll(r[j + 1], 1, 0) + pltpu.roll(r[j + 1], y - 1, 0)
                    )
                    outs.append((h, x0 + j, post(h, x0 + j, (ym * s) * t)))
            for o in outs:
                dst(*o)
            return c

        lax.fori_loop(0, total // step, body, 0)

    def into(ref):
        def put(h, x, v):
            ref[h, x] = v
        return put

    def solve(l, src, dst, matrix=None, scale=None):
        step, n = SX[l], 1
        apply(l if matrix is None else matrix, src, dst, step, n, scale)

    def residual(l, halves=(0, 1)):
        s, ta, tb = S[l], at("TA", l), at("TB", l)
        aa, bb = at("AA", l), at("BB", l)
        solves(s, [(ta, l, None), (tb, 4 + l, None)])
        stencil(l, tb, into(bb), 1, lambda h, x, v: 0.32 * ta[h, x] + 0.64 * v, halves)
        stencil(l, bb, into(aa), 0, lambda h, x, v: 0.04 * s[h, x] + v, halves)

    def smoothed(l):
        w = 0
        s, ta, tb, tc = S[l], at("TA", l), at("TB", l), at("TC", l)
        bb, cc, ma = at("BB", l), at("CC", l), at("MA", l)
        solve(l, tb, tc)
        stencil(l, tc, into(bb), 2 + w, lambda h, x, v: 0.8192 * tb[h, x] + 0.4096 * v)
        stencil(l, bb, into(cc), 1 + w, lambda h, x, v: 0.9728 * ta[h, x] + v)
        stencil(l, cc, into(ma), w, lambda h, x, v: 0.9984 * s[h, x] + v)

    def restrict(l, put, halves=(0, 1)):
        ox, oy, n = OX[l], OY[l], LX[l] // 2
        aa = at("AA", l)

        def body(i, c):
            x = ox + 2 * i
            for h in halves:
                even, off = pl.ds(oy, n, 2), pl.ds(oy + 1, n, 2)
                v = (aa[h, x, even, :] + aa[h, x, off, :]) + (
                    aa[h, x + 1, even, :] + aa[h, x + 1, off, :]
                )
                put(h, i, 0.25 * v)
            return c

        lax.fori_loop(0, n, body, 0)

    def prolong(l, fields, outs, halves):
        c = l + 1
        w = 1 if l == 0 else 0
        n, ox, oc, y = LX[c], OX[l], OX[c], SY[c]
        ys, cnt = [(0, 24), (2, 12), (2, 8), (2, 8)][l]
        gyc = iota((cnt, 128), 0) + (iy * n + ys - OY[c])
        ym = jnp.where((gyc >= 0) & (gyc < ngy * n), 1.0, 0.0).astype(f32)

        def body(j, carry):
            j = j - (1 + w)
            gx = ix * n + j
            s = jnp.where((gx >= 0) & (gx < ngx * n), 1.0, 0.0).astype(f32)
            ms = ym * s
            for h in halves:
                lower, here, upper = (fields(h, oc + j + i) for i in (-1, 0, 1))
                for (o, oh), lo_, he, up_ in zip(outs, lower, here, upper):
                    oh = h if oh is None else oh
                    for i, far in enumerate((lo_, up_)):
                        v = 0.75 * he + 0.25 * far
                        ev = (0.75 * v + 0.25 * pltpu.roll(v, 1, 0))[ys : ys + cnt]
                        od = (0.75 * v + 0.25 * pltpu.roll(v, y - 1, 0))[ys : ys + cnt]
                        o[oh, ox + 2 * j + i, pl.ds(0, cnt, 2), :] = ms * ev
                        o[oh, ox + 2 * j + i, pl.ds(1, cnt, 2), :] = ms * od
            return carry

        lax.fori_loop(0, n + 2 + 2 * w, body, 0)

    def correct(l, store):
        c = l + 1
        m, u, g2 = M[c], at("U", c), at("V", c)
        kap = a[l] / a[c]
        solves(m, [(u, c, kap), (g2, 8 + l, 0.64 * kap)])
        q = 0.04 * (1.0 - a[c] / a[l])
        outs = [at("P0", l), at("P1", l), at("P2", l)]

        def fields(h, x):
            uv = u[h, x]
            return (0.04 * m[h, x] + q * uv, 0.32 * uv, g2[h, x])

        prolong(l, fields, [(o, None) for o in outs], (0, 1))
        cc, ma = at("CC", l), at("MA", l)
        stencil(l, outs[2], into(cc), 1, lambda h, x, v: outs[1][h, x] + v)
        stencil(l, cc, store, 0, lambda h, x, v: (ma[h, x] + outs[0][h, x]) + v)

    def parts(et):
        phi = dot3(L0, et).T
        h, lo_ = split(phi)
        h, lo_ = h.astype(f32), lo_.astype(f32)
        return h + pltpu.roll(lo_, 32, 1) + pltpu.roll(h, 64, 1)

    def powers(first, src, d1, d2):
        for i in range(5):
            x = slice(8 * i, 8 * i + 8)
            w = S0[1, x].reshape(384, 128).astype(bf16)
            c = mm(w, ub[:, 128 * first : 128 * first + 256])
            vh, vl = split(src[0, x].reshape(384, 128))
            t = mm(jnp.concatenate([vh, vl], 1), ra[...])
            t = (t[:, 0:128] + t[:, 128:256]) + c[:, 0:128]
            d1[0, x] = t.reshape(8, 48, 128)
            vh, vl = split(t)
            t = mm(jnp.concatenate([vh, vl], 1), ra[...])
            t = (t[:, 0:128] + t[:, 128:256]) + c[:, 128:256]
            d2[0, x] = t.reshape(8, 48, 128)

    g0_recv()
    for i in range(4):
        w = parts(e0[:, :, 256 * i : 256 * i + 256].reshape(64, 256))
        S0[1, 4 + 8 * i : 12 + 8 * i, 8:40, :] = w.reshape(8, 32, 128)
    gh_recv()
    w = parts(eh[:, :, 0:384].reshape(64, 384))
    S0[1, 0:4] = w[0:192].reshape(4, 48, 128)
    S0[1, 36:40] = w[192:384].reshape(4, 48, 128)
    w = parts(eh[:, :, 384:640].reshape(64, 256)).reshape(32, 8, 128)
    S0[1, 4:36, 4:8, :] = w[:, 0:4]
    S0[1, 4:36, 40:44, :] = w[:, 4:8]

    t1, t2, t3, t4 = at("TA", 0), at("TB", 0), at("TC", 0), at("P0", 0)
    aa0, bb0, cc0, ma0 = at("AA", 0), at("BB", 0), at("CC", 0), at("MA", 0)
    powers(0, S0, t1, t2)
    stencil(0, t2, into(bb0), 1, lambda h, x, v: 0.32 * t1[h, x] + 0.64 * v, (0,))
    stencil(0, bb0, into(aa0), 0, lambda h, x, v: 0.04 * S0[h, x] + v, (0,))

    def put1(h, i, v):
        S1[h, 3 + i, 4:20, :] = v
    restrict(0, put1, (0,))
    el1[...] = dot3(re1[...], S1[0, 3:19, 4:20, :].reshape(256, 128), True)
    e1[k] = el1[...]
    g1_start, g1_recv, g1_send = gather(2, el1, e1)
    g1_start()
    x1_start, x1_finish, x1_send = packed(1, 1, "g1", S1, True, False)
    x1_start()

    L1 = funct(1)
    matrices()
    powers(2, t2, t3, t4)
    for l in (1, 2, 3):
        square(l)
    clear(r_["in_s2"])

    def both0(h, x, v):
        bb0[0, x] = 0.8192 * t3[0, x] + 0.4096 * v
        bb0[1, x] = 0.4096 * (t3[0, x] + v)

    g1_recv()
    phi = dot3(L1, e1[...].reshape(256, 256))
    S1[1, 3:19, 4:20, :] = phi.T.reshape(16, 16, 128)
    y1_start, y1_finish, y1_send = packed(2, 1, "f1", S1, False, True)
    y1_start()
    stencil(0, t4, both0, 3, lambda h, x, v: v, (0,))
    stencil(0, bb0, into(cc0), 2, lambda h, x, v: (0.1536 if h else 0.9728) * t2[0, x] + v)
    for r in (S3, S4, M3, M4):
        clear2(r)
    for name in ("s3", "s4", "m3", "m2", "m1"):
        clear(r_["in_" + name])
    x1_finish()
    y1_finish()
    residual(1)

    def put2(h, i, v):
        S2[h, 3 + i, 4:12, :] = v
    restrict(1, put2)
    x2_start, x2_finish, x2_send = packed(3, 2, "s2", S2)
    x2_start()
    smoothed(1)
    stencil(0, cc0, into(aa0), 1, lambda h, x, v: (0.0256 if h else 0.9984) * t1[0, x] + v)

    x2_finish()
    residual(2)

    def put3(h, i, v):
        S3[h, 4 + i, 4:8, :] = v
    restrict(2, put3)
    x3_start, x3_finish, x3_send = packed_block(4, 3, "s3", S3)
    x3_start()
    smoothed(2)
    stencil(0, aa0, into(ma0), 0, lambda h, x, v: 0.0016 * S0[0, x] + v, (1,))

    x3_finish()
    residual(3)

    def put4(h, i, v):
        S4[h, 4 + i, 4:6, :] = v
    restrict(3, put4)
    x4_start, x4_finish, x4_send = packed_block(5, 4, "s4", S4, FAR)
    x4_start()
    smoothed(3)
    for l in (3, 2, 1, 0):
        both(l)

    x4_finish()
    ta4 = at("TA", 4)
    solve(4, S4, ta4)

    stencil(4, ta4, into(M4), 2, lambda h, x, v: 0.96 * S4[h, x] + 0.64 * v)

    def putm3(h, x, v):
        M3[h, x, 4:8, :] = v[4:8]
    correct(3, putm3)
    z3_start, z3_finish, z3_send = packed_block(7, 3, "m3", M3)
    z3_start()
    z3_finish()

    def putm2(h, x, v):
        M2[h, x, 4:12, :] = v[4:12]
    correct(2, putm2)
    z2_start, z2_finish, z2_send = packed(8, 2, "m2", M2)
    z2_start()
    z2_finish()

    def putm1(h, x, v):
        M1[h, x, 4:20, :] = v[4:20]
    correct(1, putm1)
    z1_start, z1_finish, z1_send = packed(9, 1, "m1", M1)
    z1_start()
    z1_finish()

    u, g2 = at("U", 1), at("V", 1)
    kap = a[0] / a[1]
    solves(M1, [(u, 1, kap), (g2, 8, 0.64 * kap)])
    solve_block(M1, HM)
    solve_block(g2, H2)
    q = 0.04 * (1.0 - a[1] / a[0])

    def fields0(h, x):
        uv, gv = u[0, x], g2[0, x]
        h0 = 0.04 * HM[0, x] + (q / 0.64) * gv
        return (0.04 * M1[0, x] + q * uv, h0 - 0.32 * uv, 0.5 * gv, H2[0, x], h0)

    P0, P1, P2 = at("P0", 0), at("P1", 0), at("P2", 0)
    prolong(0, fields0, [(P0, 0), (P0, 1), (P1, 0), (P1, 1), (P2, 0)], (0,))

    def pair(h, x, v):
        bb0[0, x] = v - P1[0, x]
        bb0[1, x] = v + P1[0, x]
    stencil(0, P1, pair, 2, lambda h, x, v: v, (1,))
    stencil(0, bb0, into(cc0), 1, lambda h, x, v: P0[1, x] + v, (0,))
    inv0 = 1.0 / a[0]

    def put_sol(h, x, v):
        sol_ref[x - 4] = v[8:40]

    def put_res(h, x, v):
        res_ref[x - 4] = v[8:40]
    stencil(0, bb0, put_sol, 0, lambda h, x, v: inv0 * ((aa0[0, x] + P2[0, x]) + v), (1,))
    stencil(0, cc0, put_res, 0, lambda h, x, v: (ma0[1, x] - P0[0, x]) + v, (0,))

    for wait in sends + [
        x1_send, g1_send, y1_send, x2_send, x3_send, x4_send, z3_send, z2_send, z1_send
    ]:
        wait()


def body(sizes, right_side, z_faces, xy_coupling, block_inverse):
    n = right_side.shape
    vmem = pl.BlockSpec(memory_space=pltpu.VMEM)
    hbm = pl.BlockSpec(memory_space=pl.ANY)
    scratch = [pltpu.VMEM(s, f32) for s in scratch_shapes().values()]
    scratch += [pltpu.VMEM((5, 128, 128), f32)]
    scratch += [pltpu.VMEM((12, 256, 256), bf16), pltpu.VMEM((12, 256, 256), bf16)]
    scratch += [pltpu.VMEM((256, 256), bf16), pltpu.VMEM((128, 512), bf16)]
    scratch += [pltpu.SemaphoreType.DMA((10, 20)), pltpu.SemaphoreType.DMA((10, 20))]
    scratch += [pltpu.SemaphoreType.DMA((5, 8)), pltpu.SemaphoreType.DMA((5, 8))]
    scratch += [pltpu.SemaphoreType.DMA((4,)), pltpu.VMEM((1, 128), f32), pltpu.SMEM((5,), f32)]
    return pl.pallas_call(
        lambda *r: kernel(sizes, *r),
        out_shape=(pltpu.VMEM(n, f32), pltpu.VMEM(n, f32)),
        in_specs=[hbm, hbm, hbm, hbm],
        out_specs=(vmem, vmem),
        scratch_shapes=scratch,
        compiler_params=pltpu.CompilerParams(
            collective_id=0, has_side_effects=True, vmem_limit_bytes=60 * 2**20
        ),
        name="vcycle",
    )(right_side, z_faces.reshape(1, -1), block_inverse, xy_coupling)


def solution(mesh):
    sizes = tuple(mesh.shape[n] for n in ("gx", "gy", "gz"))
    return jax.shard_map(
        lambda *args: body(sizes, *args),
        mesh=mesh,
        in_specs=(P("gx", "gy", "gz"), P("gz"), P(), P(None, "gz", None)),
        out_specs=(P("gx", "gy", "gz"), P("gx", "gy", "gz")),
        check_vma=False,
    )
```
